128 devices in a mesh: gy: 2 (over core), gx: 64 (over z, y, x).
Axes of the slice: x: 4, y: 4, z: 4, core: 2. Of those that a mesh axis runs over, the one named last changes fastest.
Arguments:
- basis_vectors: float32 [36, 256, 128, 256], P(None, 'gx', 'gy'), may hold values from -30 to 30, as said below
- reaction: float32 [256, 128, 256], P('gx', 'gy'), may hold values from 0.5 to 3
Outputs:
- new_vectors: float32 [4, 256, 128, 256], P(None, 'gx', 'gy')
- hessenberg: float32 [40, 4], replicated
The draws below stay inside these ranges and needn't reach their ends.
Inputs may be any that keep to these rules, and one draw needn't show every extreme that they name: `basis_vectors`: under the inner product the basis vectors are nearly orthonormal.
All inputs are finite; a program needn't handle non-finite values.
Results may differ from the reference program's by a relative error of at most 0.0003.
Values sent between devices are 32-bit elements; how exact they have to be, the bound alone decides.
No kernel may reach another device: no remote copies, remote signals or barrier semaphores. Data moves between devices by JAX's collectives and lax.ppermute only.
A program may use at most 128 MiB of HBM per device.

```python
import math
import jax
import jax.numpy as jnp
from jax import lax

KEEP = 36
STEPS = 4
BASIS = 40
NX = 256
NY = 128
NZ = 256


WIND_SPEEDS = (0.9, 0.6, 0.4)


TILT_SHARE = 0.01


MIXING_SHARE = 0.003


RAMP_FACTOR = 3.0


def stencil_drawn(values, x_ext, y_ext, z_ext, reaction):
    summed = -reaction * values
    for position, extended in enumerate((x_ext, y_ext, z_ext)):
        count = values.shape[position]
        higher = lax.slice_in_dim(extended, 3, count + 3, axis=position)
        lower_one = lax.slice_in_dim(extended, 1, count + 1, axis=position)
        lower_two = lax.slice_in_dim(extended, 0, count, axis=position)
        wind_speed = WIND_SPEEDS[position]
        summed = summed + higher + lower_one - 2.0 * values - wind_speed * (3.0 * values - 4.0 * lower_one + lower_two) * 0.5
    return summed


def apply_operator_drawn(values, reaction):
    padded = jnp.pad(values, ((2, 1), (2, 1), (2, 1)))
    return stencil_drawn(values, padded[:, 2:-1, 2:-1], padded[2:-1, :, 2:-1], padded[2:-1, 2:-1, :], reaction)


def reaction_field(key):
    key_field = jax.random.fold_in(key, 7)
    shape = (NX, NY, NZ)
    return jax.random.uniform(key_field, shape, jnp.float32, 0.5, 3.0)


def draw_reaction(key, part):
    return reaction_field(key)


def rough_fields(key, count, plane_scale):
    shape = (count, NX, NY, NZ)
    values = jax.random.normal(key, shape, jnp.float32)
    return values * plane_scale


def draw_basis_vectors(key, part):
    key_list = jax.random.split(jax.random.fold_in(key, 11), 4)
    plane_index = jnp.arange(NX, dtype=jnp.float32).reshape(NX, 1, 1)
    plane_scale = jnp.exp(math.log(RAMP_FACTOR) * plane_index / float(NX - 1))
    plane_scale = plane_scale / jnp.sqrt(jnp.mean(plane_scale * plane_scale))
    seed_fields = rough_fields(key_list[0], 2, plane_scale)
    start_field = seed_fields[0] / jnp.sqrt(jnp.mean(seed_fields[0] * seed_fields[0]))
    image_field = apply_operator_drawn(start_field, reaction_field(key))
    tilted = image_field + TILT_SHARE * jnp.sqrt(jnp.mean(image_field * image_field)) * seed_fields[1]
    tilted = tilted - jnp.sum(tilted * start_field) / jnp.sum(start_field * start_field) * start_field
    tilted = tilted / jnp.sqrt(jnp.mean(tilted * tilted))
    row_fields = jnp.concatenate([start_field[None], tilted[None], rough_fields(key_list[1], KEEP - 2, plane_scale)], axis=0)
    gram_matrix = jnp.einsum('axyz,bxyz->ab', row_fields, row_fields, precision=lax.Precision.HIGHEST) / float(NX * NY * NZ)
    inverse = jnp.linalg.inv(jnp.linalg.cholesky(gram_matrix))
    moved_order = jnp.concatenate([jnp.arange(1, KEEP, dtype=jnp.int32), jnp.zeros((1,), jnp.int32)])
    shuffle = jnp.eye(KEEP, dtype=jnp.float32)[moved_order]
    mixing = jnp.eye(KEEP, dtype=jnp.float32) + MIXING_SHARE * jax.random.normal(key_list[2], (KEEP, KEEP), jnp.float32)
    matrix = jnp.dot(mixing, jnp.dot(shuffle, inverse, precision=lax.Precision.HIGHEST), precision=lax.Precision.HIGHEST)
    return jnp.einsum('ab,bxyz->axyz', matrix, row_fields, precision=lax.Precision.HIGHEST)


def setup_inputs(seed: int = 0) -> dict:
    splits = jax.random.split(jax.random.key(seed), 3)
    basis_vectors = draw_basis_vectors(jax.random.fold_in(splits[2], 71), 0)
    reaction = draw_reaction(jax.random.fold_in(splits[2], 71), 0)
    return {"basis_vectors": basis_vectors, "reaction": reaction}


WIND_SPEEDS = (0.9, 0.6, 0.4)
EPSILON = 1e-06

def stencil(values, x_ext, y_ext, z_ext, reaction):
    summed = -reaction * values
    for position, extended in enumerate((x_ext, y_ext, z_ext)):
        count = values.shape[position]
        higher = lax.slice_in_dim(extended, 3, count + 3, axis=position)
        lower_one = lax.slice_in_dim(extended, 1, count + 1, axis=position)
        lower_two = lax.slice_in_dim(extended, 0, count, axis=position)
        wind_speed = WIND_SPEEDS[position]
        summed = summed + higher + lower_one - 2.0 * values - wind_speed * (3.0 * values - 4.0 * lower_one + lower_two) * 0.5
    return summed

def apply_operator(values, reaction):
    padded = jnp.pad(values, ((2, 1), (2, 1), (2, 1)))
    return stencil(values, padded[:, 2:-1, 2:-1], padded[2:-1, :, 2:-1], padded[2:-1, 2:-1, :], reaction)

def project(basis_vectors, created, image):
    local = jnp.einsum('kxyz,xyz->k', basis_vectors, image, precision=lax.Precision.HIGHEST)
    extra = [jnp.sum(vector * image)[None] for vector in created]
    return jnp.concatenate([local] + extra)

def combine(basis_vectors, created, weights):
    keep_count = basis_vectors.shape[0]
    summed = jnp.einsum('k,kxyz->xyz', weights[:keep_count], basis_vectors, precision=lax.Precision.HIGHEST)
    for index, vector in enumerate(created):
        summed = summed + weights[keep_count + index] * vector
    return summed

def reference(basis_vectors, reaction):
    cell_count = float(NX * NY * NZ)
    created = []
    columns = []
    for section in range(STEPS):
        current = KEEP + section
        vector_now = basis_vectors[KEEP - 1] if section == 0 else created[-1]
        image = apply_operator(vector_now, reaction)
        first_terms = project(basis_vectors, created, image) / cell_count
        first_rest = image - combine(basis_vectors, created, first_terms)
        second_terms = project(basis_vectors, created, first_rest) / cell_count
        second_rest = first_rest - combine(basis_vectors, created, second_terms)
        length_now = jnp.sqrt(jnp.sum(second_rest * second_rest) / cell_count + EPSILON)
        columns.append(jnp.concatenate([first_terms + second_terms, length_now[None], jnp.zeros((BASIS - current - 1,), jnp.float32)]))
        created.append(second_rest / length_now)
    return (jnp.stack(created), jnp.stack(columns, axis=1))
```

```python
import functools

import jax
import jax.numpy as jnp
from jax import lax
from jax.experimental import pallas as pl
from jax.experimental.pallas import tpu as pltpu
from jax.sharding import PartitionSpec as P

KEEP = 36
STEPS = 4
BASIS = KEEP + STEPS
WIND_SPEEDS = (0.9, 0.6, 0.4)
EPSILON = 1e-06
F32 = jnp.float32

XS, YS, ZS = 4, 64, 256
ROWS = XS * YS
GROUP = 6
PACK = 12
PACK_LANES = 40
CHUNK = 32

PARAMS = pltpu.CompilerParams(vmem_limit_bytes=16 * 2**20)
VMEM_SPEC = pl.BlockSpec(memory_space=pltpu.VMEM)


def iota(shape, axis):
    return lax.broadcasted_iota(jnp.int32, shape, axis)


def to_column(row):
    pick = iota((BASIS, 128), 0) == iota((BASIS, 128), 1)
    return jnp.sum(jnp.where(pick, row, 0.0), axis=1, keepdims=True)


def to_row(column):
    pick = iota((BASIS, 128), 0) == iota((BASIS, 128), 1)
    return jnp.sum(jnp.where(pick, column, 0.0), axis=0, keepdims=True)


def fold_tiles(block):
    return jnp.sum(block.reshape(-1, 8, ZS), axis=0)


def fold_row(acc):
    return jnp.sum(acc[:, :128] + acc[:, 128:], axis=0, keepdims=True)


def gram_kernel(v_hbm, v_ref, out_ref, sums_ref, matrix_ref, sems):
    groups = KEEP // GROUP
    copies = [
        pltpu.make_async_copy(
            v_hbm.at[pl.ds(g * GROUP, GROUP)], v_ref.at[pl.ds(g * GROUP, GROUP)], sems.at[g]
        )
        for g in range(groups)
    ]
    for c in copies:
        c.start()

    def block(ga, gb):
        pairs = [
            (a, b)
            for a in range(GROUP)
            for b in range(GROUP)
            if ga != gb or a <= b
        ]

        def step(t, accs):
            rows = pl.ds(pl.multiple_of(t * 8, 8), 8)
            accs = list(accs)
            for half in range(2):
                lanes = pl.ds(half * 128, 128)
                left = [v_ref[ga * GROUP + a, rows, lanes] for a in range(GROUP)]
                right = left if ga == gb else [v_ref[gb * GROUP + b, rows, lanes] for b in range(GROUP)]
                for n, (a, b) in enumerate(pairs):
                    accs[n] = accs[n] + left[a] * right[b]
            return tuple(accs)

        zero = jnp.zeros((8, 128), F32)
        accs = lax.fori_loop(0, ROWS // 8, step, tuple(zero for _ in pairs))
        for (a, b), acc in zip(pairs, accs):
            row = jnp.sum(acc, axis=0, keepdims=True)
            i, j = ga * GROUP + a, gb * GROUP + b
            sums_ref[i, pl.ds(j, 1), :] = row
            if i != j:
                sums_ref[j, pl.ds(i, 1), :] = row

    for gb in range(groups):
        copies[gb].wait()
        for ga in range(gb + 1):
            block(ga, gb)
    lane = iota((KEEP, 128), 1)
    matrix = jnp.zeros((KEEP, 128), F32)
    for i in range(KEEP):
        column = jnp.sum(sums_ref[i], axis=1, keepdims=True)
        matrix = jnp.where(lane == i, column, matrix)
    matrix_ref[...] = matrix
    packed = matrix_ref[pl.ds(0, PACK), :]
    for p in range(1, KEEP // PACK):
        packed = packed + pltpu.roll(matrix_ref[pl.ds(p * PACK, PACK), :], p * PACK_LANES, 1)
    out_ref[pl.ds(0, PACK), :] = packed
    out_ref[pl.ds(PACK, 16 - PACK), :] = jnp.zeros((16 - PACK, 128), F32)


def gram_call(basis):
    return pl.pallas_call(
        gram_kernel,
        in_specs=[pl.BlockSpec(memory_space=pl.ANY)],
        out_specs=(VMEM_SPEC, VMEM_SPEC),
        out_shape=(
            pltpu.VMEM((KEEP, ROWS, ZS), F32),
            jax.ShapeDtypeStruct((16, 128), F32),
        ),
        scratch_shapes=[
            pltpu.VMEM((KEEP, KEEP, 128), F32),
            pltpu.VMEM((KEEP, 128), F32),
            pltpu.SemaphoreType.DMA((KEEP // GROUP,)),
        ],
        compiler_params=PARAMS,
        name="gram",
    )(basis)


def dot_all(v_ref, others, x_ref, dots_ref):
    dots_ref[...] = jnp.zeros((BASIS, 128), F32)
    batch = 12

    def run(reads, base):
        def step(c, accs):
            rows = pl.ds(pl.multiple_of(c * CHUNK, CHUNK), CHUNK)
            x = x_ref[rows, :]
            return tuple(acc + fold_tiles(read(rows) * x) for acc, read in zip(accs, reads))

        zero = jnp.zeros((8, ZS), F32)
        accs = lax.fori_loop(0, ROWS // CHUNK, step, tuple(zero for _ in reads))
        for n, acc in enumerate(accs):
            dots_ref[pl.ds(base + n, 1), :] = fold_row(acc)

    for first in range(0, KEEP, batch):
        run([lambda rows, i=i: v_ref[i, rows, :] for i in range(first, first + batch)], first)
    if others:
        run([lambda rows, r=r: r[rows, :] for r in others], KEEP)
    return to_row(jnp.sum(dots_ref[...], axis=1, keepdims=True))


def self_dots_kernel(count, *refs):
    v_ref, *others = refs[: 1 + count]
    out_ref, dots_ref = refs[1 + count :]
    out_ref[...] = dot_all(v_ref, others, others[-1], dots_ref)


def self_dots_call(v, created):
    count = len(created)
    return pl.pallas_call(
        functools.partial(self_dots_kernel, count),
        in_specs=[VMEM_SPEC] * (1 + count),
        out_specs=VMEM_SPEC,
        out_shape=jax.ShapeDtypeStruct((1, 128), F32),
        scratch_shapes=[pltpu.VMEM((BASIS, 128), F32)],
        compiler_params=PARAMS,
        name="self_dots_%d" % count,
    )(v, *created)


def image_kernel(count, *refs):
    core_ref, v_ref, *others = refs[: 2 + count]
    up_ref, down_ref, swap_ref, reaction_ref, extra_ref = refs[2 + count : 7 + count]
    w_ref, out_ref, dots_ref, pad_ref = refs[7 + count :]
    core = core_ref[0]
    upper = core.astype(F32)
    lower = 1.0 - upper
    source = others[-1] if others else v_ref.at[KEEP - 1]
    lane = iota((YS, ZS), 1)
    center = -6.0 - 1.5 * sum(WIND_SPEEDS)
    near = [1.0 + 2.0 * s for s in WIND_SPEEDS]
    far = [-0.5 * s for s in WIND_SPEEDS]

    def plane(x):
        if x < 0:
            return up_ref[pl.ds((x + 2) * YS, YS), :]
        if x >= XS:
            return down_ref[...]
        return source[pl.ds(x * YS, YS), :]

    for x in range(XS):
        mine = plane(x)
        pad_ref[x, pl.ds(8, YS), :] = mine
        edge = swap_ref[pl.ds(2 * x, 2), :]
        pad_ref[x, pl.ds(6, 2), :] = edge * upper
        pad_ref[x, pl.ds(72, 1), :] = edge[0:1] * lower
        image = (center - reaction_ref[pl.ds(x * YS, YS), :]) * mine
        image = image + plane(x + 1) + near[0] * plane(x - 1) + far[0] * plane(x - 2)
        image = (
            image
            + pad_ref[x, pl.ds(9, YS), :]
            + near[1] * pad_ref[x, pl.ds(7, YS), :]
            + far[1] * pad_ref[x, pl.ds(6, YS), :]
        )
        image = (
            image
            + jnp.where(lane < ZS - 1, pltpu.roll(mine, ZS - 1, 1), 0.0)
            + near[2] * jnp.where(lane >= 1, pltpu.roll(mine, 1, 1), 0.0)
            + far[2] * jnp.where(lane >= 2, pltpu.roll(mine, 2, 1), 0.0)
        )
        w_ref[pl.ds(x * YS, YS), :] = image
    row = dot_all(v_ref, others, w_ref, dots_ref)
    if others:
        out_ref[pl.ds(0, 1), :] = row
        out_ref[pl.ds(1, 1), :] = extra_ref[...]
    else:
        out_ref[...] = extra_ref[...]
        out_ref[pl.ds(PACK, 1), :] = row


def image_call(core, v, created, halo, reaction, extra):
    count = len(created)
    payload = 2 if created else 16
    return pl.pallas_call(
        functools.partial(image_kernel, count),
        in_specs=[pl.BlockSpec(memory_space=pltpu.SMEM)] + [VMEM_SPEC] * (6 + count),
        out_specs=(VMEM_SPEC, VMEM_SPEC),
        out_shape=(
            pltpu.VMEM((ROWS, ZS), F32),
            jax.ShapeDtypeStruct((payload, 128), F32),
        ),
        scratch_shapes=[
            pltpu.VMEM((BASIS, 128), F32),
            pltpu.VMEM((XS, YS + 16, ZS), F32),
        ],
        compiler_params=PARAMS,
        name="image_%d" % count,
    )(core, v, *created, *halo, reaction, extra)


STATE_G, STATE_H, STATE_D, STATE_ROWS = 0, BASIS, 2 * BASIS, 2 * BASIS + 8


def summed_rows(recv_ref, count):
    if count >= 8:
        return jnp.sum(recv_ref[...].reshape(-1, count, 128), axis=0)
    total = jnp.sum(recv_ref[...].reshape(-1, 8, 128), axis=0)
    shift = count
    while shift < 8:
        total = total + pltpu.roll(total, 8 - shift, 0)
        shift *= 2
    return total


def combine_kernel(count, cells, *refs):
    core_ref, recv_ref, w_ref, v_ref, *others = refs[: 4 + count]
    pos = 4 + count
    if count:
        state_in = refs[pos]
        pos += 1
    u_ref, up_ref, down_ref, swap_ref, state_ref, square_ref, weight_ref = refs[pos:]
    lane = iota((1, 128), 1)
    lanes = iota((BASIS, 128), 1)
    subs = iota((BASIS, 128), 0)
    scale = 1.0 / cells
    if count == 0:
        total = summed_rows(recv_ref, 16) * scale
        state_ref[...] = jnp.zeros((STATE_ROWS, 128), F32)
        for p in range(KEEP // PACK):
            part = total[:PACK]
            if p:
                part = pltpu.roll(part, 128 - p * PACK_LANES, 1)
            part = jnp.where(iota((PACK, 128), 1) < KEEP, part, 0.0)
            state_ref[pl.ds(STATE_G + p * PACK, PACK), :] = part
        gram = state_ref[pl.ds(STATE_G, BASIS), :]
        hess = jnp.zeros((BASIS, 128), F32)
        inverse_row = jnp.where(lane < KEEP, 1.0, 0.0)
        first_row = total[PACK : PACK + 1]
        inverse = jnp.ones((1, 1), F32)
    else:
        total = summed_rows(recv_ref, 2) * scale
        newest = KEEP + count - 1
        raw_first, raw_gram = total[0:1], total[1:2]
        square = jnp.sum(jnp.where(lane == newest, raw_gram, 0.0), axis=1, keepdims=True)
        norm = jnp.sqrt(square + EPSILON)
        inverse = 1.0 / norm
        inverse_row = jnp.where(lane == newest, inverse, state_in[pl.ds(STATE_D, 1), :])
        gram_row = raw_gram * inverse_row * inverse
        first_row = raw_first * inverse_row * inverse
        gram = state_in[pl.ds(STATE_G, BASIS), :]
        gram = jnp.where(lanes == newest, to_column(gram_row), gram)
        gram = jnp.where(subs == newest, gram_row, gram)
        hess = state_in[pl.ds(STATE_H, BASIS), :]
        hess = jnp.where((subs == newest) & (lanes == count - 1), norm, hess)
    first = to_column(first_row)
    folded = jnp.sum(gram * first_row, axis=1, keepdims=True)
    weights = first + (first - folded)
    hess = jnp.where((lanes == count) & (subs < KEEP + count), weights, hess)
    state_ref[pl.ds(STATE_G, BASIS), :] = gram
    state_ref[pl.ds(STATE_H, BASIS), :] = hess
    state_ref[pl.ds(STATE_D, 8), :] = jnp.broadcast_to(inverse_row, (8, 128))
    weight_ref[...] = jnp.broadcast_to(weights * to_column(inverse_row), (BASIS, ZS))

    def step(c, acc):
        rows = pl.ds(pl.multiple_of(c * CHUNK, CHUNK), CHUNK)
        value = w_ref[rows, :] * inverse
        for i in range(KEEP):
            value = value - weight_ref[pl.ds(i, 1), :] * v_ref[i, rows, :]
        for i, other in enumerate(others):
            value = value - weight_ref[pl.ds(KEEP + i, 1), :] * other[rows, :]
        u_ref[rows, :] = value
        return acc + fold_tiles(value * value)

    acc = lax.fori_loop(0, ROWS // CHUNK, step, jnp.zeros((8, ZS), F32))
    square_ref[...] = fold_row(acc)
    up_ref[...] = u_ref[pl.ds((XS - 2) * YS, 2 * YS), :]
    down_ref[...] = u_ref[pl.ds(0, YS), :]
    upper = core_ref[0] == 1
    for x in range(XS):
        low = u_ref[pl.ds(x * YS, 2), :]
        high = u_ref[pl.ds(x * YS + YS - 2, 2), :]
        swap_ref[pl.ds(2 * x, 2), :] = jnp.where(upper, low, high)


def combine_call(core, recv, w, v, created, state, cells):
    count = len(created)
    states = [state] if created else []
    return pl.pallas_call(
        functools.partial(combine_kernel, count, cells),
        in_specs=[pl.BlockSpec(memory_space=pltpu.SMEM)] + [VMEM_SPEC] * (3 + count + len(states)),
        out_specs=(VMEM_SPEC,) * 6,
        out_shape=(
            pltpu.VMEM((ROWS, ZS), F32),
            jax.ShapeDtypeStruct((2 * YS, ZS), F32),
            jax.ShapeDtypeStruct((YS, ZS), F32),
            jax.ShapeDtypeStruct((2 * XS, ZS), F32),
            jax.ShapeDtypeStruct((STATE_ROWS, 128), F32),
            jax.ShapeDtypeStruct((1, 128), F32),
        ),
        scratch_shapes=[pltpu.VMEM((BASIS, ZS), F32)],
        compiler_params=PARAMS,
        name="combine_%d" % count,
    )(core, recv, w, v, *created, *states)


def finish_kernel(cells, *refs):
    recv_ref, state_ref, *created = refs[: 2 + STEPS]
    new_ref, hess_ref = refs[2 + STEPS :]
    lane = iota((1, 128), 1)
    total = summed_rows(recv_ref, 1)[0:1] * (1.0 / cells)
    norm = jnp.sqrt(jnp.sum(total, axis=1, keepdims=True) + EPSILON)
    lanes = iota((BASIS, 128), 1)
    subs = iota((BASIS, 128), 0)
    hess = state_ref[pl.ds(STATE_H, BASIS), :]
    hess = jnp.where((subs == BASIS - 1) & (lanes == STEPS - 1), norm, hess)
    hess_ref[...] = hess[:, :STEPS]
    inverse_row = state_ref[pl.ds(STATE_D, 1), :]
    for j, u_ref in enumerate(created):
        if j == STEPS - 1:
            inverse = 1.0 / norm
        else:
            inverse = jnp.sum(jnp.where(lane == KEEP + j, inverse_row, 0.0), axis=1, keepdims=True)
        for c in range(ROWS // CHUNK):
            rows = pl.ds(c * CHUNK, CHUNK)
            new_ref[j, rows, :] = u_ref[rows, :] * inverse


def finish_call(recv, state, created, cells):
    return pl.pallas_call(
        functools.partial(finish_kernel, cells),
        in_specs=[VMEM_SPEC] * (2 + STEPS),
        out_specs=(VMEM_SPEC, VMEM_SPEC),
        out_shape=(
            jax.ShapeDtypeStruct((STEPS, ROWS, ZS), F32),
            jax.ShapeDtypeStruct((BASIS, STEPS), F32),
        ),
        compiler_params=PARAMS,
        name="finish",
    )(recv, state, *created)


def exchange(up, down, swap):
    count = lax.axis_size("gx")
    up = lax.ppermute(up, "gx", [(i, i + 1) for i in range(count - 1)])
    down = lax.ppermute(down, "gx", [(i + 1, i) for i in range(count - 1)])
    swap = lax.ppermute(swap, "gy", [(0, 1), (1, 0)])
    return up, down, swap


def from_all(payload):
    axes = ("gy", "gx")
    devices = lax.axis_size(axes)
    copies = jnp.broadcast_to(payload, (devices, *payload.shape))
    got = lax.all_to_all(copies, axes, split_axis=0, concat_axis=0, tiled=True)
    return got.reshape(-1, 128)


def body(basis_vectors, reaction):
    cells = float(ROWS * ZS * lax.axis_size("gx") * lax.axis_size("gy"))
    core_index = lax.axis_index("gy")
    core = core_index.astype(jnp.int32).reshape(1)
    last = basis_vectors[KEEP - 1]
    edge = jnp.where(core_index == 1, last[:, :2], last[:, YS - 2 :])
    halo = exchange(
        last[XS - 2 :].reshape(2 * YS, ZS), last[:1].reshape(YS, ZS), edge.reshape(2 * XS, ZS)
    )
    reaction = reaction.reshape(ROWS, ZS)
    v, extra = gram_call(basis_vectors.reshape(KEEP, ROWS, ZS))
    created = []
    state = None
    for j in range(STEPS):
        if j:
            extra = self_dots_call(v, created)
        w, payload = image_call(core, v, created, halo, reaction, extra)
        recv = from_all(payload)
        u, up, down, swap, state, square = combine_call(core, recv, w, v, created, state, cells)
        created.append(u)
        if j + 1 < STEPS:
            halo = exchange(up, down, swap)
    new, hessenberg = finish_call(from_all(square), state, created, cells)
    return new.reshape(STEPS, XS, YS, ZS), hessenberg


def solution(mesh):
    return jax.shard_map(
        body,
        mesh=mesh,
        in_specs=(P(None, "gx", "gy", None), P("gx", "gy", None)),
        out_specs=(P(None, "gx", "gy", None), P()),
        check_vma=False,
    )
```

```python
import functools

import jax
import jax.numpy as jnp
from jax import lax
from jax.experimental import pallas as pl
from jax.experimental.pallas import tpu as pltpu
from jax.sharding import PartitionSpec as P

KEEP = 36
STEPS = 4
BASIS = KEEP + STEPS
WIND_SPEEDS = (0.9, 0.6, 0.4)
EPSILON = 1e-06
F32 = jnp.float32

XS, YS, ZS = 4, 64, 256
ROWS = XS * YS
GROUP = 4
GRAM_ROWS = 32
HALF = KEEP // 2
PACK = 6
PACK_LANES = 40
CHUNK = 32
SOUND_SHARE = 0.05

PARAMS = pltpu.CompilerParams(vmem_limit_bytes=16 * 2**20)
SMEM_SPEC = pl.BlockSpec(memory_space=pltpu.SMEM)
VMEM_SPEC = pl.BlockSpec(memory_space=pltpu.VMEM)


def iota(shape, axis):
    return lax.broadcasted_iota(jnp.int32, shape, axis)


def to_column(row):
    pick = iota((BASIS, 128), 0) == iota((BASIS, 128), 1)
    return jnp.sum(jnp.where(pick, row, 0.0), axis=1, keepdims=True)


def to_row(column):
    pick = iota((BASIS, 128), 0) == iota((BASIS, 128), 1)
    return jnp.sum(jnp.where(pick, column, 0.0), axis=0, keepdims=True)


def fold_tiles(block):
    return jnp.sum(block.reshape(-1, 8, ZS), axis=0)


def fold_row(acc):
    return jnp.sum(acc[:, :128] + acc[:, 128:], axis=0, keepdims=True)


def gram_kernel(v_hbm, v_ref, out_ref, sums_ref, matrix_ref, sems):
    groups = KEEP // GROUP
    copies = [
        pltpu.make_async_copy(
            v_hbm.at[pl.ds(g * GROUP, GROUP)], v_ref.at[pl.ds(g * GROUP, GROUP)], sems.at[g]
        )
        for g in range(groups)
    ]
    for c in copies:
        c.start()

    def block(ga, gb):
        pairs = [(a, b) for a in range(GROUP) for b in range(GROUP) if ga != gb or a <= b]

        def step(t, accs):
            accs = list(accs)
            for part in range(GRAM_ROWS // 8):
                rows = pl.ds(pl.multiple_of(t * GRAM_ROWS, GRAM_ROWS) + 8 * part, 8)
                for half in range(2):
                    lanes = pl.ds(half * 128, 128)
                    left = [v_ref[ga * GROUP + a, rows, lanes] for a in range(GROUP)]
                    right = left
                    if ga != gb:
                        right = [v_ref[gb * GROUP + b, rows, lanes] for b in range(GROUP)]
                    for n, (a, b) in enumerate(pairs):
                        accs[n] = accs[n] + left[a] * right[b]
            return tuple(accs)

        zero = jnp.zeros((8, 128), F32)
        accs = lax.fori_loop(0, ROWS // GRAM_ROWS, step, tuple(zero for _ in pairs))
        for (a, b), acc in zip(pairs, accs):
            row = jnp.sum(acc, axis=0, keepdims=True)
            i, j = ga * GROUP + a, gb * GROUP + b
            sums_ref[i, pl.ds(j, 1), :] = row
            if i != j:
                sums_ref[j, pl.ds(i, 1), :] = row

    for gb in range(groups):
        copies[gb].wait()
        for ga in range(gb + 1):
            block(ga, gb)
    lane = iota((KEEP, 128), 1)
    matrix = jnp.zeros((KEEP, 128), F32)
    for i in range(KEEP):
        column = jnp.sum(sums_ref[i], axis=1, keepdims=True)
        matrix = jnp.where(lane == i, column, matrix)
    matrix_ref[pl.ds(0, KEEP), :] = matrix
    top = matrix_ref[pl.ds(0, HALF), :]
    bottom = pltpu.roll(matrix_ref[pl.ds(HALF, HALF), :], 128 - HALF, 1)
    lane = iota((HALF, 128), 1)
    sub = iota((HALF, 128), 0)
    diagonal = jnp.sum(jnp.where(lane == sub, top, 0.0), axis=1, keepdims=True)
    packed = jnp.where((lane > sub) | (lane >= HALF), top, bottom)
    packed = jnp.where(lane < KEEP, packed, jnp.where(lane == KEEP, diagonal, 0.0))
    matrix_ref[pl.ds(0, HALF), :] = packed
    packed = matrix_ref[pl.ds(0, PACK), :]
    for p in range(1, HALF // PACK):
        packed = packed + pltpu.roll(matrix_ref[pl.ds(p * PACK, PACK), :], p * PACK_LANES, 1)
    for r in range(PACK):
        out_ref[:, pl.ds(r * 128, 128)] = packed[r : r + 1]


def gram_call(basis):
    return pl.pallas_call(
        gram_kernel,
        in_specs=[pl.BlockSpec(memory_space=pltpu.HBM)],
        out_specs=(VMEM_SPEC, VMEM_SPEC),
        out_shape=(
            pltpu.VMEM((KEEP, ROWS, ZS), F32),
            jax.ShapeDtypeStruct((1, PACK * 128), F32),
        ),
        scratch_shapes=[
            pltpu.VMEM((KEEP, KEEP, 128), F32),
            pltpu.VMEM((BASIS, 128), F32),
            pltpu.SemaphoreType.DMA((KEEP // GROUP,)),
        ],
        compiler_params=PARAMS,
        name="gram",
    )(pltpu.with_memory_space_constraint(basis, pltpu.HBM))


def dot_all(v_ref, others, x_ref, dots_ref):
    dots_ref[...] = jnp.zeros((BASIS, 128), F32)
    batch = 12

    def run(reads, base):
        def step(c, accs):
            rows = pl.ds(pl.multiple_of(c * CHUNK, CHUNK), CHUNK)
            x = x_ref[rows, :]
            return tuple(acc + fold_tiles(read(rows) * x) for acc, read in zip(accs, reads))

        zero = jnp.zeros((8, ZS), F32)
        accs = lax.fori_loop(0, ROWS // CHUNK, step, tuple(zero for _ in reads))
        for n, acc in enumerate(accs):
            dots_ref[pl.ds(base + n, 1), :] = fold_row(acc)

    for first in range(0, KEEP, batch):
        run([lambda rows, i=i: v_ref[i, rows, :] for i in range(first, first + batch)], first)
    if others:
        run([lambda rows, r=r: r[rows, :] for r in others], KEEP)
    return to_row(jnp.sum(dots_ref[...], axis=1, keepdims=True))


def self_dots_kernel(count, *refs):
    v_ref, *others = refs[: 1 + count]
    out_ref, dots_ref = refs[1 + count :]
    out_ref[...] = dot_all(v_ref, others, others[-1], dots_ref)


def self_dots_call(v, created):
    count = len(created)
    return pl.pallas_call(
        functools.partial(self_dots_kernel, count),
        in_specs=[VMEM_SPEC] * (1 + count),
        out_specs=VMEM_SPEC,
        out_shape=jax.ShapeDtypeStruct((1, 128), F32),
        scratch_shapes=[pltpu.VMEM((BASIS, 128), F32)],
        compiler_params=PARAMS,
        name="self_dots_%d" % count,
    )(v, *created)


def write_edges(place_ref, u_ref, first_ref, second_ref, swap_ref):
    odd = place_ref[1] == 1
    upper = place_ref[0] == 1
    for x in range(2):
        low = u_ref[pl.ds(x * YS, YS), :]
        high = u_ref[pl.ds((XS - 2 + x) * YS, YS), :]
        first_ref[pl.ds(x * YS, YS), :] = jnp.where(odd, low, high)
        second_ref[pl.ds(x * YS, YS), :] = jnp.where(odd, high, low)
    for x in range(XS):
        low = u_ref[pl.ds(x * YS, 2), :]
        high = u_ref[pl.ds(x * YS + YS - 2, 2), :]
        swap_ref[pl.ds(2 * x, 2), :] = jnp.where(upper, low, high)


EDGE_SHAPES = (
    jax.ShapeDtypeStruct((2 * YS, ZS), F32),
    jax.ShapeDtypeStruct((2 * YS, ZS), F32),
    jax.ShapeDtypeStruct((2 * XS, ZS), F32),
)


LAST_SHAPES = (
    jax.ShapeDtypeStruct((1, 128), F32),
    jax.ShapeDtypeStruct((1, 128), F32),
    jax.ShapeDtypeStruct((1,), jnp.int32),
)


def edges_kernel(place_ref, v_hbm, first_ref, second_ref, swap_ref, u_ref, sem):
    copy = pltpu.make_async_copy(v_hbm.at[KEEP - 1], u_ref, sem)
    copy.start()
    copy.wait()
    write_edges(place_ref, u_ref, first_ref, second_ref, swap_ref)


def edges_call(place, basis):
    return pl.pallas_call(
        edges_kernel,
        in_specs=[SMEM_SPEC, pl.BlockSpec(memory_space=pltpu.HBM)],
        out_specs=(VMEM_SPEC,) * 3,
        out_shape=EDGE_SHAPES,
        scratch_shapes=[pltpu.VMEM((ROWS, ZS), F32), pltpu.SemaphoreType.DMA],
        compiler_params=PARAMS,
        name="edges",
    )(place, pltpu.with_memory_space_constraint(basis, pltpu.HBM))


def write_for_all(out_ref, rows):
    count = len(rows)
    period = count
    while period % 8:
        period += count
    for tile in range(period // 8):
        sub = iota((8, 128), 0)
        block = jnp.zeros((8, 128), F32)
        for r in range(8):
            block = jnp.where(sub == r, rows[(8 * tile + r) % count], block)
        for p in range(out_ref.shape[0] // period):
            out_ref[pl.ds(p * period + 8 * tile, 8), :] = block


def payload_rows(count):
    return 2 if count else 1 + PACK


def image_kernel(count, *refs):
    place_ref, v_ref, *others = refs[: 2 + count]
    first_ref, second_ref, swap_ref, reaction_ref, extra_ref = refs[2 + count : 7 + count]
    w_ref, out_ref, dots_ref, pad_ref = refs[7 + count :]
    odd = place_ref[1] == 1
    upper = place_ref[0].astype(F32)
    lower = 1.0 - upper
    source = others[-1] if others else v_ref.at[KEEP - 1]
    lane = iota((YS, ZS), 1)
    center = -6.0 - 1.5 * sum(WIND_SPEEDS)
    near = [1.0 + 2.0 * s for s in WIND_SPEEDS]
    far = [-0.5 * s for s in WIND_SPEEDS]

    def plane(x):
        if x < 0:
            rows = pl.ds((x + 2) * YS, YS)
            return jnp.where(odd, first_ref[rows, :], second_ref[rows, :])
        if x >= XS:
            rows = pl.ds(0, YS)
            return jnp.where(odd, second_ref[rows, :], first_ref[rows, :])
        return source[pl.ds(x * YS, YS), :]

    for x in range(XS):
        mine = plane(x)
        pad_ref[x, pl.ds(8, YS), :] = mine
        edge = swap_ref[pl.ds(2 * x, 2), :]
        pad_ref[x, pl.ds(6, 2), :] = edge * upper
        pad_ref[x, pl.ds(72, 1), :] = edge[0:1] * lower
        image = (center - reaction_ref[pl.ds(x * YS, YS), :]) * mine
        image = image + plane(x + 1) + near[0] * plane(x - 1) + far[0] * plane(x - 2)
        image = (
            image
            + pad_ref[x, pl.ds(9, YS), :]
            + near[1] * pad_ref[x, pl.ds(7, YS), :]
            + far[1] * pad_ref[x, pl.ds(6, YS), :]
        )
        image = (
            image
            + jnp.where(lane < ZS - 1, pltpu.roll(mine, ZS - 1, 1), 0.0)
            + near[2] * jnp.where(lane >= 1, pltpu.roll(mine, 1, 1), 0.0)
            + far[2] * jnp.where(lane >= 2, pltpu.roll(mine, 2, 1), 0.0)
        )
        w_ref[pl.ds(x * YS, YS), :] = image
    more = [w_ref] if count == STEPS - 1 else []
    rows = [dot_all(v_ref, others + more, w_ref, dots_ref)]
    rows += [extra_ref[:, pl.ds(128 * r, 128)] for r in range(payload_rows(count) - 1)]
    write_for_all(out_ref, rows)


def image_call(place, v, created, halo, reaction, extra, devices):
    count = len(created)
    return pl.pallas_call(
        functools.partial(image_kernel, count),
        in_specs=[SMEM_SPEC] + [VMEM_SPEC] * (6 + count),
        out_specs=(VMEM_SPEC, VMEM_SPEC),
        out_shape=(
            pltpu.VMEM((ROWS, ZS), F32),
            jax.ShapeDtypeStruct((devices * payload_rows(count), 128), F32),
        ),
        scratch_shapes=[
            pltpu.VMEM((BASIS, 128), F32),
            pltpu.VMEM((XS, YS + 16, ZS), F32),
        ],
        compiler_params=PARAMS,
        name="image_%d" % count,
    )(place, v, *created, *halo, reaction, extra)


STATE_G, STATE_H, STATE_D, STATE_ROWS = 0, BASIS, 2 * BASIS, 2 * BASIS + 8


def summed_rows(recv_ref, count):
    period = count
    while period % 8:
        period += count
    total = jnp.sum(recv_ref[...].reshape(-1, period, 128), axis=0)
    if count in (1, 2):
        while count < 8:
            total = total + pltpu.roll(total, 8 - count, 0)
            count *= 2
        return total
    return sum(total[p : p + count] for p in range(0, period, count))


def unpacked_gram(packed, pack_ref):
    pack_ref[...] = jnp.zeros((128, 128), F32)
    for p in range(HALF // PACK):
        part = packed
        if p:
            part = pltpu.roll(part, 128 - p * PACK_LANES, 1)
        pack_ref[pl.ds(p * PACK, PACK), :] = part
    turned = jnp.transpose(pack_ref[...])
    plain = pack_ref[pl.ds(0, HALF), :]
    lane = iota((HALF, 128), 1)
    sub = iota((HALF, 128), 0)
    diagonal = jnp.sum(jnp.where(lane == KEEP, plain, 0.0), axis=1, keepdims=True)
    top = jnp.where((lane > sub) | (lane >= HALF), plain, turned[:HALF])
    top = jnp.where(lane == sub, diagonal, top)
    last = jnp.where(lane <= sub, plain, turned[:HALF])
    pack_ref[...] = turned
    bottom = jnp.where(lane < HALF, pack_ref[pl.ds(HALF, HALF), :], pltpu.roll(last, HALF, 1))
    pack_ref[pl.ds(0, HALF), :] = jnp.where(lane < KEEP, top, 0.0)
    pack_ref[pl.ds(HALF, HALF), :] = jnp.where(lane < KEEP, bottom, 0.0)
    pack_ref[pl.ds(KEEP, STEPS), :] = jnp.zeros((STEPS, 128), F32)


def combine_kernel(count, cells, *refs):
    place_ref, recv_ref, w_ref, v_ref, *others = refs[: 4 + count]
    pos = 4 + count
    if count:
        state_in = refs[pos]
        pos += 1
    u_ref, state_ref, *outs, weight_ref, pack_ref = refs[pos:]
    final = count == STEPS - 1
    if final:
        square_ref, guess_ref, sound_ref = outs
    lane = iota((1, 128), 1)
    lanes = iota((BASIS, 128), 1)
    subs = iota((BASIS, 128), 0)
    scale = 1.0 / cells
    if count == 0:
        total = summed_rows(recv_ref, 1 + PACK) * scale
        unpacked_gram(total[1 : 1 + PACK], pack_ref)
        gram = pack_ref[pl.ds(0, BASIS), :]
        hess = jnp.zeros((BASIS, 128), F32)
        inverse_row = jnp.where(lane < KEEP, 1.0, 0.0)
        first_row = total[0:1]
        inverse = jnp.ones((1, 1), F32)
    else:
        total = summed_rows(recv_ref, 2) * scale
        newest = KEEP + count - 1
        raw_first, raw_gram = total[0:1], total[1:2]
        square = jnp.sum(jnp.where(lane == newest, raw_gram, 0.0), axis=1, keepdims=True)
        norm = jnp.sqrt(square + EPSILON)
        inverse = 1.0 / norm
        inverse_row = jnp.where(lane == newest, inverse, state_in[pl.ds(STATE_D, 1), :])
        gram_row = raw_gram * inverse_row * inverse
        first_row = raw_first * inverse_row * inverse
        gram = state_in[pl.ds(STATE_G, BASIS), :]
        gram = jnp.where(lanes == newest, to_column(gram_row), gram)
        gram = jnp.where(subs == newest, gram_row, gram)
        hess = state_in[pl.ds(STATE_H, BASIS), :]
        hess = jnp.where((subs == newest) & (lanes == count - 1), norm, hess)
    first = to_column(first_row)
    folded = jnp.sum(gram * first_row, axis=1, keepdims=True)
    weights = first + (first - folded)
    hess = jnp.where((lanes == count) & (subs < KEEP + count), weights, hess)
    if final:
        image_square = jnp.sum(jnp.where(lane == BASIS - 1, raw_first, 0.0), axis=1, keepdims=True)
        image_square = image_square * inverse * inverse
        again = jnp.sum(gram * to_row(weights), axis=1, keepdims=True)
        guess = image_square - jnp.sum(weights * (2.0 * first - again), axis=0, keepdims=True)
        guess_ref[...] = jnp.where(lane == 0, guess, 0.0)
        sound = jnp.where(guess > SOUND_SHARE * image_square, 1, 0)
        sound_ref[0] = sound[0, 0]
    state_ref[pl.ds(STATE_G, BASIS), :] = gram
    state_ref[pl.ds(STATE_H, BASIS), :] = hess
    state_ref[pl.ds(STATE_D, 8), :] = jnp.broadcast_to(inverse_row, (8, 128))
    weight_ref[...] = jnp.broadcast_to(weights * to_column(inverse_row), (BASIS, ZS))

    def step(c, acc):
        rows = pl.ds(pl.multiple_of(c * CHUNK, CHUNK), CHUNK)
        value = w_ref[rows, :] * inverse
        for i in range(KEEP):
            value = value - weight_ref[pl.ds(i, 1), :] * v_ref[i, rows, :]
        for i, other in enumerate(others):
            value = value - weight_ref[pl.ds(KEEP + i, 1), :] * other[rows, :]
        u_ref[rows, :] = value
        return acc + fold_tiles(value * value)

    acc = lax.fori_loop(0, ROWS // CHUNK, step, jnp.zeros((8, ZS), F32))
    if final:
        square_ref[...] = fold_row(acc)
    else:
        write_edges(place_ref, u_ref, *outs)


def combine_call(place, recv, w, v, created, state, cells):
    count = len(created)
    states = [state] if created else []
    final = count == STEPS - 1
    return pl.pallas_call(
        functools.partial(combine_kernel, count, cells),
        in_specs=[SMEM_SPEC] + [VMEM_SPEC] * (3 + count + len(states)),
        out_specs=(VMEM_SPEC,) * 4 + (SMEM_SPEC if final else VMEM_SPEC,),
        out_shape=(
            pltpu.VMEM((ROWS, ZS), F32),
            jax.ShapeDtypeStruct((STATE_ROWS, 128), F32),
            *(LAST_SHAPES if final else EDGE_SHAPES),
        ),
        scratch_shapes=[pltpu.VMEM((BASIS, ZS), F32), pltpu.VMEM((128, 128), F32)],
        compiler_params=PARAMS,
        name="combine_%d" % count,
    )(place, recv, w, v, *created, *states)


def finish_kernel(*refs):
    square_ref, state_ref, *created = refs[: 2 + STEPS]
    new_ref, hess_ref = refs[2 + STEPS :]
    lane = iota((1, 128), 1)
    norm = jnp.sqrt(jnp.sum(square_ref[...], axis=1, keepdims=True) + EPSILON)
    lanes = iota((BASIS, 128), 1)
    subs = iota((BASIS, 128), 0)
    hess = state_ref[pl.ds(STATE_H, BASIS), :]
    hess = jnp.where((subs == BASIS - 1) & (lanes == STEPS - 1), norm, hess)
    hess_ref[...] = jnp.transpose(jnp.concatenate([hess, jnp.zeros((128 - BASIS, 128), F32)], axis=0))[:STEPS, :BASIS]
    inverse_row = state_ref[pl.ds(STATE_D, 1), :]
    for j, u_ref in enumerate(created):
        if j == STEPS - 1:
            inverse = 1.0 / norm
        else:
            inverse = jnp.sum(jnp.where(lane == KEEP + j, inverse_row, 0.0), axis=1, keepdims=True)
        for c in range(ROWS // CHUNK):
            rows = pl.ds(c * CHUNK, CHUNK)
            new_ref[j, rows, :] = u_ref[rows, :] * inverse


def finish_call(square, state, created):
    return pl.pallas_call(
        finish_kernel,
        in_specs=[VMEM_SPEC] * (2 + STEPS),
        out_specs=(VMEM_SPEC, VMEM_SPEC),
        out_shape=(
            jax.ShapeDtypeStruct((STEPS, ROWS, ZS), F32),
            jax.ShapeDtypeStruct((STEPS, BASIS), F32),
        ),
        compiler_params=PARAMS,
        name="finish",
    )(square, state, *created)


def exchange(first, second, swap):
    count = lax.axis_size("gx")

    def pairs(start):
        lower = range(start, count - 1, 2)
        return [(i, i + 1) for i in lower] + [(i + 1, i) for i in lower]

    second = lax.ppermute(second, "gx", pairs(1))
    first = lax.ppermute(first, "gx", pairs(0))
    swap = lax.ppermute(swap, "gy", [(0, 1), (1, 0)])
    return first, second, swap


def from_all(payload):
    axes = ("gy", "gx")
    devices = lax.axis_size(axes)
    copies = payload.reshape(devices, 1, -1)
    got = lax.all_to_all(copies, axes, split_axis=0, concat_axis=0, tiled=True)
    return got.reshape(-1, 128)


def body(basis_vectors, reaction):
    devices = lax.axis_size(("gy", "gx"))
    cells = float(ROWS * ZS * devices)
    place = jnp.stack([lax.axis_index("gy"), lax.axis_index("gx") % 2]).astype(jnp.int32)
    basis = basis_vectors.reshape(KEEP, ROWS, ZS)
    halo = exchange(*edges_call(place, basis))
    reaction = reaction.reshape(ROWS, ZS)
    v, extra = gram_call(basis)
    created = []
    state = None
    for j in range(STEPS):
        if j:
            extra = self_dots_call(v, created)
        w, payload = image_call(place, v, created, halo, reaction, extra, devices)
        recv = from_all(payload)
        u, state, *edges = combine_call(place, recv, w, v, created, state, cells)
        created.append(u)
        if j + 1 < STEPS:
            halo = exchange(*edges)
    square, guess, sound = edges
    square = lax.cond(
        sound[0] == 1,
        lambda guess, square: guess,
        lambda guess, square: jnp.sum(from_all(square), axis=0, keepdims=True) * (1.0 / cells),
        guess,
        jnp.broadcast_to(square, (devices, 128)),
    )
    new, hessenberg = finish_call(square, state, created)
    return new.reshape(STEPS, XS, YS, ZS), hessenberg.T


def solution(mesh):
    return jax.shard_map(
        body,
        mesh=mesh,
        in_specs=(P(None, "gx", "gy", None), P("gx", "gy", None)),
        out_specs=(P(None, "gx", "gy", None), P()),
        check_vma=False,
    )
```

```python
import functools

import jax
import jax.numpy as jnp
from jax import lax
from jax.experimental import pallas as pl
from jax.experimental.pallas import tpu as pltpu
from jax.sharding import PartitionSpec as P


KEEP = 36
STEPS = 4
BASIS = KEEP + STEPS
WIND_SPEEDS = (0.9, 0.6, 0.4)
EPSILON = 1e-06
F32 = jnp.float32

XS, YS, ZS = 4, 64, 256
ROWS = XS * YS
GROUP = 4
GRAM_ROWS = 32
HALF = KEEP // 2
PACK = 6
PACK_LANES = 40
CHUNK = 32
SOUND_SHARE = 0.05

PARAMS = pltpu.CompilerParams(vmem_limit_bytes=16 * 2**20)
SMEM_SPEC = pl.BlockSpec(memory_space=pltpu.SMEM)
VMEM_SPEC = pl.BlockSpec(memory_space=pltpu.VMEM)


def iota(shape, axis):
    return lax.broadcasted_iota(jnp.int32, shape, axis)


def to_column(row):
    pick = iota((BASIS, 128), 0) == iota((BASIS, 128), 1)
    return jnp.sum(jnp.where(pick, row, 0.0), axis=1, keepdims=True)


def to_row(column):
    pick = iota((BASIS, 128), 0) == iota((BASIS, 128), 1)
    return jnp.sum(jnp.where(pick, column, 0.0), axis=0, keepdims=True)


def fold_tiles(block):
    return jnp.sum(block.reshape(-1, 8, ZS), axis=0)


def fold_row(acc):
    return jnp.sum(acc[:, :128] + acc[:, 128:], axis=0, keepdims=True)


def gram_kernel(v_hbm, v_ref, out_ref, sums_ref, matrix_ref, sems):
    groups = KEEP // GROUP
    copies = [
        pltpu.make_async_copy(
            v_hbm.at[pl.ds(g * GROUP, GROUP)], v_ref.at[pl.ds(g * GROUP, GROUP)], sems.at[g]
        )
        for g in range(groups)
    ]
    for c in copies:
        c.start()

    def block(ga, gb):
        pairs = [(a, b) for a in range(GROUP) for b in range(GROUP) if ga != gb or a <= b]

        def step(t, accs):
            accs = list(accs)
            for part in range(GRAM_ROWS // 8):
                rows = pl.ds(pl.multiple_of(t * GRAM_ROWS, GRAM_ROWS) + 8 * part, 8)
                for half in range(2):
                    lanes = pl.ds(half * 128, 128)
                    left = [v_ref[ga * GROUP + a, rows, lanes] for a in range(GROUP)]
                    right = left
                    if ga != gb:
                        right = [v_ref[gb * GROUP + b, rows, lanes] for b in range(GROUP)]
                    for n, (a, b) in enumerate(pairs):
                        accs[n] = accs[n] + left[a] * right[b]
            return tuple(accs)

        zero = jnp.zeros((8, 128), F32)
        accs = lax.fori_loop(0, ROWS // GRAM_ROWS, step, tuple(zero for _ in pairs))
        for (a, b), acc in zip(pairs, accs):
            row = jnp.sum(acc, axis=0, keepdims=True)
            i, j = ga * GROUP + a, gb * GROUP + b
            sums_ref[i, pl.ds(j, 1), :] = row
            if i != j:
                sums_ref[j, pl.ds(i, 1), :] = row

    for gb in range(groups):
        copies[gb].wait()
        for ga in range(gb + 1):
            block(ga, gb)
    lane = iota((KEEP, 128), 1)
    matrix = jnp.zeros((KEEP, 128), F32)
    for i in range(KEEP):
        column = jnp.sum(sums_ref[i], axis=1, keepdims=True)
        matrix = jnp.where(lane == i, column, matrix)
    matrix_ref[pl.ds(0, KEEP), :] = matrix
    top = matrix_ref[pl.ds(0, HALF), :]
    bottom = pltpu.roll(matrix_ref[pl.ds(HALF, HALF), :], 128 - HALF, 1)
    lane = iota((HALF, 128), 1)
    sub = iota((HALF, 128), 0)
    diagonal = jnp.sum(jnp.where(lane == sub, top, 0.0), axis=1, keepdims=True)
    packed = jnp.where((lane > sub) | (lane >= HALF), top, bottom)
    packed = jnp.where(lane < KEEP, packed, jnp.where(lane == KEEP, diagonal, 0.0))
    matrix_ref[pl.ds(0, HALF), :] = packed
    packed = matrix_ref[pl.ds(0, PACK), :]
    for p in range(1, HALF // PACK):
        packed = packed + pltpu.roll(matrix_ref[pl.ds(p * PACK, PACK), :], p * PACK_LANES, 1)
    for r in range(PACK):
        out_ref[:, pl.ds(r * 128, 128)] = packed[r : r + 1]


def gram_call(basis):
    return pl.pallas_call(
        gram_kernel,
        in_specs=[pl.BlockSpec(memory_space=pltpu.HBM)],
        out_specs=(VMEM_SPEC, VMEM_SPEC),
        out_shape=(
            pltpu.VMEM((KEEP, ROWS, ZS), F32),
            jax.ShapeDtypeStruct((1, PACK * 128), F32),
        ),
        scratch_shapes=[
            pltpu.VMEM((KEEP, KEEP, 128), F32),
            pltpu.VMEM((BASIS, 128), F32),
            pltpu.SemaphoreType.DMA((KEEP // GROUP,)),
        ],
        compiler_params=PARAMS,
        name="gram",
    )(pltpu.with_memory_space_constraint(basis, pltpu.HBM))


def dot_all(v_ref, others, x_ref, dots_ref):
    dots_ref[...] = jnp.zeros((BASIS, 128), F32)
    batch = 12

    def run(reads, base):
        def step(c, accs):
            rows = pl.ds(pl.multiple_of(c * CHUNK, CHUNK), CHUNK)
            x = x_ref[rows, :]
            return tuple(acc + fold_tiles(read(rows) * x) for acc, read in zip(accs, reads))

        zero = jnp.zeros((8, ZS), F32)
        accs = lax.fori_loop(0, ROWS // CHUNK, step, tuple(zero for _ in reads))
        for n, acc in enumerate(accs):
            dots_ref[pl.ds(base + n, 1), :] = fold_row(acc)

    for first in range(0, KEEP, batch):
        run([lambda rows, i=i: v_ref[i, rows, :] for i in range(first, first + batch)], first)
    if others:
        run([lambda rows, r=r: r[rows, :] for r in others], KEEP)
    return to_row(jnp.sum(dots_ref[...], axis=1, keepdims=True))


def self_dots_kernel(count, *refs):
    v_ref, *others = refs[: 1 + count]
    out_ref, dots_ref = refs[1 + count :]
    out_ref[...] = dot_all(v_ref, others, others[-1], dots_ref)


def self_dots_call(v, created):
    count = len(created)
    return pl.pallas_call(
        functools.partial(self_dots_kernel, count),
        in_specs=[VMEM_SPEC] * (1 + count),
        out_specs=VMEM_SPEC,
        out_shape=jax.ShapeDtypeStruct((1, 128), F32),
        scratch_shapes=[pltpu.VMEM((BASIS, 128), F32)],
        compiler_params=PARAMS,
    )(v, *created)


def write_edges(u_ref, first_ref, second_ref, swap_ref):
    odd = lax.axis_index("gx") % 2 == 1
    upper = lax.axis_index("gy") == 1
    for x in range(2):
        low = u_ref[pl.ds(x * YS, YS), :]
        high = u_ref[pl.ds((XS - 2 + x) * YS, YS), :]
        first_ref[pl.ds(x * YS, YS), :] = jnp.where(odd, low, high)
        second_ref[pl.ds(x * YS, YS), :] = jnp.where(odd, high, low)
    for x in range(XS):
        low = u_ref[pl.ds(x * YS, 2), :]
        high = u_ref[pl.ds(x * YS + YS - 2, 2), :]
        swap_ref[pl.ds(2 * x, 2), :] = jnp.where(upper, low, high)


EDGE_SHAPES = (
    jax.ShapeDtypeStruct((2 * YS, ZS), F32),
    jax.ShapeDtypeStruct((2 * YS, ZS), F32),
    jax.ShapeDtypeStruct((2 * XS, ZS), F32),
)


LAST_SHAPES = (
    jax.ShapeDtypeStruct((1, 128), F32),
    jax.ShapeDtypeStruct((1, 128), F32),
    jax.ShapeDtypeStruct((1,), jnp.int32),
)


def edges_kernel(v_hbm, first_ref, second_ref, swap_ref, u_ref, sem):
    copy = pltpu.make_async_copy(v_hbm.at[KEEP - 1], u_ref, sem)
    copy.start()
    copy.wait()
    write_edges(u_ref, first_ref, second_ref, swap_ref)


def edges_call(basis):
    return pl.pallas_call(
        edges_kernel,
        in_specs=[pl.BlockSpec(memory_space=pltpu.HBM)],
        out_specs=(VMEM_SPEC,) * 3,
        out_shape=EDGE_SHAPES,
        scratch_shapes=[pltpu.VMEM((ROWS, ZS), F32), pltpu.SemaphoreType.DMA],
        compiler_params=PARAMS,
        name="edges",
    )(pltpu.with_memory_space_constraint(basis, pltpu.HBM))


def write_for_all(out_ref, rows):
    count = len(rows)
    period = count
    while period % 8:
        period += count
    for tile in range(period // 8):
        sub = iota((8, 128), 0)
        block = jnp.zeros((8, 128), F32)
        for r in range(8):
            block = jnp.where(sub == r, rows[(8 * tile + r) % count], block)
        for p in range(out_ref.shape[0] // period):
            out_ref[pl.ds(p * period + 8 * tile, 8), :] = block


def payload_rows(count):
    return 2 if count else 1 + PACK


def image_kernel(count, *refs):
    v_ref, *others = refs[: 1 + count]
    first_ref, second_ref, swap_ref, reaction_ref, extra_ref = refs[1 + count : 6 + count]
    w_ref, out_ref, dots_ref, pad_ref = refs[6 + count :]
    odd = lax.axis_index("gx") % 2 == 1
    upper = lax.axis_index("gy").astype(F32)
    lower = 1.0 - upper
    source = others[-1] if others else v_ref.at[KEEP - 1]
    lane = iota((YS, ZS), 1)
    center = -6.0 - 1.5 * sum(WIND_SPEEDS)
    near = [1.0 + 2.0 * s for s in WIND_SPEEDS]
    far = [-0.5 * s for s in WIND_SPEEDS]

    def plane(x):
        if x < 0:
            rows = pl.ds((x + 2) * YS, YS)
            return jnp.where(odd, first_ref[rows, :], second_ref[rows, :])
        if x >= XS:
            rows = pl.ds(0, YS)
            return jnp.where(odd, second_ref[rows, :], first_ref[rows, :])
        return source[pl.ds(x * YS, YS), :]

    for x in range(XS):
        mine = plane(x)
        pad_ref[x, pl.ds(8, YS), :] = mine
        edge = swap_ref[pl.ds(2 * x, 2), :]
        pad_ref[x, pl.ds(6, 2), :] = edge * upper
        pad_ref[x, pl.ds(72, 1), :] = edge[0:1] * lower
        image = (center - reaction_ref[pl.ds(x * YS, YS), :]) * mine
        image = image + plane(x + 1) + near[0] * plane(x - 1) + far[0] * plane(x - 2)
        image = (
            image
            + pad_ref[x, pl.ds(9, YS), :]
            + near[1] * pad_ref[x, pl.ds(7, YS), :]
            + far[1] * pad_ref[x, pl.ds(6, YS), :]
        )
        image = (
            image
            + jnp.where(lane < ZS - 1, pltpu.roll(mine, ZS - 1, 1), 0.0)
            + near[2] * jnp.where(lane >= 1, pltpu.roll(mine, 1, 1), 0.0)
            + far[2] * jnp.where(lane >= 2, pltpu.roll(mine, 2, 1), 0.0)
        )
        w_ref[pl.ds(x * YS, YS), :] = image
    more = [w_ref] if count == STEPS - 1 else []
    rows = [dot_all(v_ref, others + more, w_ref, dots_ref)]
    rows += [extra_ref[:, pl.ds(128 * r, 128)] for r in range(payload_rows(count) - 1)]
    write_for_all(out_ref, rows)


def image_call(v, created, halo, reaction, extra, devices):
    count = len(created)
    return pl.pallas_call(
        functools.partial(image_kernel, count),
        in_specs=[VMEM_SPEC] * (6 + count),
        out_specs=(VMEM_SPEC, VMEM_SPEC),
        out_shape=(
            pltpu.VMEM((ROWS, ZS), F32),
            jax.ShapeDtypeStruct((devices * payload_rows(count), 128), F32),
        ),
        scratch_shapes=[
            pltpu.VMEM((BASIS, 128), F32),
            pltpu.VMEM((XS, YS + 16, ZS), F32),
        ],
        compiler_params=PARAMS,
    )(v, *created, *halo, reaction, extra)


STATE_G, STATE_H, STATE_D, STATE_ROWS = 0, BASIS, 2 * BASIS, 2 * BASIS + 8


def summed_rows(recv_ref, count):
    period = count
    while period % 8:
        period += count
    total = jnp.sum(recv_ref[...].reshape(-1, period, 128), axis=0)
    if count in (1, 2):
        while count < 8:
            total = total + pltpu.roll(total, 8 - count, 0)
            count *= 2
        return total
    return sum(total[p : p + count] for p in range(0, period, count))


def unpacked_gram(packed, pack_ref):
    pack_ref[...] = jnp.zeros((128, 128), F32)
    for p in range(HALF // PACK):
        part = packed
        if p:
            part = pltpu.roll(part, 128 - p * PACK_LANES, 1)
        pack_ref[pl.ds(p * PACK, PACK), :] = part
    turned = jnp.transpose(pack_ref[...])
    plain = pack_ref[pl.ds(0, HALF), :]
    lane = iota((HALF, 128), 1)
    sub = iota((HALF, 128), 0)
    diagonal = jnp.sum(jnp.where(lane == KEEP, plain, 0.0), axis=1, keepdims=True)
    top = jnp.where((lane > sub) | (lane >= HALF), plain, turned[:HALF])
    top = jnp.where(lane == sub, diagonal, top)
    last = jnp.where(lane <= sub, plain, turned[:HALF])
    pack_ref[...] = turned
    bottom = jnp.where(lane < HALF, pack_ref[pl.ds(HALF, HALF), :], pltpu.roll(last, HALF, 1))
    pack_ref[pl.ds(0, HALF), :] = jnp.where(lane < KEEP, top, 0.0)
    pack_ref[pl.ds(HALF, HALF), :] = jnp.where(lane < KEEP, bottom, 0.0)
    pack_ref[pl.ds(KEEP, STEPS), :] = jnp.zeros((STEPS, 128), F32)


def combine_kernel(count, cells, *refs):
    recv_ref, w_ref, v_ref, *others = refs[: 3 + count]
    pos = 3 + count
    if count:
        state_in = refs[pos]
        pos += 1
    u_ref, state_ref, *outs, weight_ref, pack_ref = refs[pos:]
    final = count == STEPS - 1
    if final:
        square_ref, guess_ref, sound_ref = outs
    lane = iota((1, 128), 1)
    lanes = iota((BASIS, 128), 1)
    subs = iota((BASIS, 128), 0)
    scale = 1.0 / cells
    if count == 0:
        total = summed_rows(recv_ref, 1 + PACK) * scale
        unpacked_gram(total[1 : 1 + PACK], pack_ref)
        gram = pack_ref[pl.ds(0, BASIS), :]
        hess = jnp.zeros((BASIS, 128), F32)
        inverse_row = jnp.where(lane < KEEP, 1.0, 0.0)
        first_row = total[0:1]
        inverse = jnp.ones((1, 1), F32)
    else:
        total = summed_rows(recv_ref, 2) * scale
        newest = KEEP + count - 1
        raw_first, raw_gram = total[0:1], total[1:2]
        square = jnp.sum(jnp.where(lane == newest, raw_gram, 0.0), axis=1, keepdims=True)
        norm = jnp.sqrt(square + EPSILON)
        inverse = 1.0 / norm
        inverse_row = jnp.where(lane == newest, inverse, state_in[pl.ds(STATE_D, 1), :])
        gram_row = raw_gram * inverse_row * inverse
        first_row = raw_first * inverse_row * inverse
        gram = state_in[pl.ds(STATE_G, BASIS), :]
        gram = jnp.where(lanes == newest, to_column(gram_row), gram)
        gram = jnp.where(subs == newest, gram_row, gram)
        hess = state_in[pl.ds(STATE_H, BASIS), :]
        hess = jnp.where((subs == newest) & (lanes == count - 1), norm, hess)
    first = to_column(first_row)
    folded = jnp.sum(gram * first_row, axis=1, keepdims=True)
    weights = first + (first - folded)
    hess = jnp.where((lanes == count) & (subs < KEEP + count), weights, hess)
    if final:
        image_square = jnp.sum(jnp.where(lane == BASIS - 1, raw_first, 0.0), axis=1, keepdims=True)
        image_square = image_square * inverse * inverse
        again = jnp.sum(gram * to_row(weights), axis=1, keepdims=True)
        guess = image_square - jnp.sum(weights * (2.0 * first - again), axis=0, keepdims=True)
        guess_ref[...] = jnp.where(lane == 0, guess, 0.0)
        sound = jnp.where(guess > SOUND_SHARE * image_square, 1, 0)
        sound_ref[0] = sound[0, 0]
    state_ref[pl.ds(STATE_G, BASIS), :] = gram
    state_ref[pl.ds(STATE_H, BASIS), :] = hess
    state_ref[pl.ds(STATE_D, 8), :] = jnp.broadcast_to(inverse_row, (8, 128))
    weight_ref[...] = jnp.broadcast_to(weights * to_column(inverse_row), (BASIS, ZS))

    def step(c, acc):
        rows = pl.ds(pl.multiple_of(c * CHUNK, CHUNK), CHUNK)
        value = w_ref[rows, :] * inverse
        for i in range(KEEP):
            value = value - weight_ref[pl.ds(i, 1), :] * v_ref[i, rows, :]
        for i, other in enumerate(others):
            value = value - weight_ref[pl.ds(KEEP + i, 1), :] * other[rows, :]
        u_ref[rows, :] = value
        return acc + fold_tiles(value * value)

    acc = lax.fori_loop(0, ROWS // CHUNK, step, jnp.zeros((8, ZS), F32))
    if final:
        square_ref[...] = fold_row(acc)
    else:
        write_edges(u_ref, *outs)


def combine_call(recv, w, v, created, state, cells):
    count = len(created)
    states = [state] if created else []
    final = count == STEPS - 1
    return pl.pallas_call(
        functools.partial(combine_kernel, count, cells),
        in_specs=[VMEM_SPEC] * (3 + count + len(states)),
        out_specs=(VMEM_SPEC,) * 4 + (SMEM_SPEC if final else VMEM_SPEC,),
        out_shape=(
            pltpu.VMEM((ROWS, ZS), F32),
            jax.ShapeDtypeStruct((STATE_ROWS, 128), F32),
            *(LAST_SHAPES if final else EDGE_SHAPES),
        ),
        scratch_shapes=[pltpu.VMEM((BASIS, ZS), F32), pltpu.VMEM((128, 128), F32)],
        compiler_params=PARAMS,
    )(recv, w, v, *created, *states)


def finish_kernel(*refs):
    square_ref, state_ref, *created = refs[: 2 + STEPS]
    new_ref, hess_ref = refs[2 + STEPS :]
    lane = iota((1, 128), 1)
    norm = jnp.sqrt(jnp.sum(square_ref[...], axis=1, keepdims=True) + EPSILON)
    lanes = iota((BASIS, 128), 1)
    subs = iota((BASIS, 128), 0)
    hess = state_ref[pl.ds(STATE_H, BASIS), :]
    hess = jnp.where((subs == BASIS - 1) & (lanes == STEPS - 1), norm, hess)
    hess_ref[...] = jnp.transpose(jnp.concatenate([hess, jnp.zeros((128 - BASIS, 128), F32)], axis=0))[:STEPS, :BASIS]
    inverse_row = state_ref[pl.ds(STATE_D, 1), :]
    for j, u_ref in enumerate(created):
        if j == STEPS - 1:
            inverse = 1.0 / norm
        else:
            inverse = jnp.sum(jnp.where(lane == KEEP + j, inverse_row, 0.0), axis=1, keepdims=True)
        for c in range(ROWS // CHUNK):
            rows = pl.ds(c * CHUNK, CHUNK)
            new_ref[j, rows, :] = u_ref[rows, :] * inverse


def finish_call(square, state, created):
    return pl.pallas_call(
        finish_kernel,
        in_specs=[VMEM_SPEC] * (2 + STEPS),
        out_specs=(VMEM_SPEC, VMEM_SPEC),
        out_shape=(
            jax.ShapeDtypeStruct((STEPS, ROWS, ZS), F32),
            jax.ShapeDtypeStruct((STEPS, BASIS), F32),
        ),
        compiler_params=PARAMS,
        name="finish",
    )(square, state, *created)


def exchange(first, second, swap):
    count = lax.axis_size("gx")

    def pairs(start):
        lower = range(start, count - 1, 2)
        return [(i, i + 1) for i in lower] + [(i + 1, i) for i in lower]

    second = lax.ppermute(second, "gx", pairs(1))
    first = lax.ppermute(first, "gx", pairs(0))
    swap = lax.ppermute(swap, "gy", [(0, 1), (1, 0)])
    return first, second, swap


def from_all(payload):
    axes = ("gy", "gx")
    devices = lax.axis_size(axes)
    copies = payload.reshape(devices, 1, -1)
    got = lax.all_to_all(copies, axes, split_axis=0, concat_axis=0, tiled=True)
    return got.reshape(-1, 128)


def body(basis_vectors, reaction):
    devices = lax.axis_size(("gy", "gx"))
    cells = float(ROWS * ZS * devices)
    basis = basis_vectors.reshape(KEEP, ROWS, ZS)
    halo = exchange(*edges_call(basis))
    reaction = reaction.reshape(ROWS, ZS)
    v, extra = gram_call(basis)
    created = []
    state = None
    for j in range(STEPS):
        if j:
            extra = self_dots_call(v, created)
        w, payload = image_call(v, created, halo, reaction, extra, devices)
        recv = from_all(payload)
        u, state, *edges = combine_call(recv, w, v, created, state, cells)
        created.append(u)
        if j + 1 < STEPS:
            halo = exchange(*edges)
    square, guess, sound = edges
    square = lax.cond(
        sound[0] == 1,
        lambda guess, square: guess,
        lambda guess, square: jnp.sum(from_all(square), axis=0, keepdims=True) * (1.0 / cells),
        guess,
        jnp.broadcast_to(square, (devices, 128)),
    )
    new, hessenberg = finish_call(square, state, created)
    return new.reshape(STEPS, XS, YS, ZS), hessenberg.T


def solution(mesh):
    return jax.shard_map(
        body,
        mesh=mesh,
        in_specs=(P(None, "gx", "gy", None), P("gx", "gy", None)),
        out_specs=(P(None, "gx", "gy", None), P()),
        check_vma=False,
    )
```

```python
import functools

import jax
import jax.numpy as jnp
from jax import lax
from jax.experimental import pallas as pl
from jax.experimental.pallas import tpu as pltpu
from jax.sharding import PartitionSpec as P


KEEP = 36
STEPS = 4
BASIS = KEEP + STEPS
WIND_SPEEDS = (0.9, 0.6, 0.4)
EPSILON = 1e-06
F32 = jnp.float32

XS, YS, ZS = 4, 64, 256
ROWS = XS * YS
GROUP = 4
GRAM_ROWS = 32
HALF = KEEP // 2
PACK = 6
PACK_LANES = 40
CHUNK = 32
SOUND_SHARE = 0.05

PARAMS = pltpu.CompilerParams(vmem_limit_bytes=16 * 2**20)
SMEM_SPEC = pl.BlockSpec(memory_space=pltpu.SMEM)
VMEM_SPEC = pl.BlockSpec(memory_space=pltpu.VMEM)


def iota(shape, axis):
    return lax.broadcasted_iota(jnp.int32, shape, axis)


def to_column(row):
    pick = iota((BASIS, 128), 0) == iota((BASIS, 128), 1)
    return jnp.sum(jnp.where(pick, row, 0.0), axis=1, keepdims=True)


def to_row(column):
    pick = iota((BASIS, 128), 0) == iota((BASIS, 128), 1)
    return jnp.sum(jnp.where(pick, column, 0.0), axis=0, keepdims=True)


def fold_tiles(block):
    return jnp.sum(block.reshape(-1, 8, ZS), axis=0)


def fold_row(acc):
    return jnp.sum(acc[:, :128] + acc[:, 128:], axis=0, keepdims=True)


def gram_block(v_ref, sums_ref, ga, gb):
    pairs = [(a, b) for a in range(GROUP) for b in range(GROUP) if ga != gb or a <= b]

    def step(t, accs):
        accs = list(accs)
        for part in range(GRAM_ROWS // 8):
            rows = pl.ds(pl.multiple_of(t * GRAM_ROWS, GRAM_ROWS) + 8 * part, 8)
            for half in range(2):
                lanes = pl.ds(half * 128, 128)
                left = [v_ref[ga * GROUP + a, rows, lanes] for a in range(GROUP)]
                right = left
                if ga != gb:
                    right = [v_ref[gb * GROUP + b, rows, lanes] for b in range(GROUP)]
                for n, (a, b) in enumerate(pairs):
                    accs[n] = accs[n] + left[a] * right[b]
        return tuple(accs)

    zero = jnp.zeros((8, 128), F32)
    accs = lax.fori_loop(0, ROWS // GRAM_ROWS, step, tuple(zero for _ in pairs))
    for (a, b), acc in zip(pairs, accs):
        row = jnp.sum(acc, axis=0, keepdims=True)
        i, j = ga * GROUP + a, gb * GROUP + b
        sums_ref[i, pl.ds(j, 1), :] = row
        if i != j:
            sums_ref[j, pl.ds(i, 1), :] = row


def write_edges(u_ref, first_ref, second_ref, swap_ref):
    odd = lax.axis_index("gx") % 2 == 1
    upper = lax.axis_index("gy") == 1
    for x in range(2):
        low = u_ref[pl.ds(x * YS, YS), :]
        high = u_ref[pl.ds((XS - 2 + x) * YS, YS), :]
        first_ref[pl.ds(x * YS, YS), :] = jnp.where(odd, low, high)
        second_ref[pl.ds(x * YS, YS), :] = jnp.where(odd, high, low)
    for x in range(XS):
        low = u_ref[pl.ds(x * YS, 2), :]
        high = u_ref[pl.ds(x * YS + YS - 2, 2), :]
        swap_ref[pl.ds(2 * x, 2), :] = jnp.where(upper, low, high)


EDGE_SHAPES = (
    jax.ShapeDtypeStruct((2 * YS, ZS), F32),
    jax.ShapeDtypeStruct((2 * YS, ZS), F32),
    jax.ShapeDtypeStruct((2 * XS, ZS), F32),
)


ARRIVAL = [KEEP // GROUP - 1, *range(KEEP // GROUP - 1)]
EARLY = 4
LATE_PAIRS = [
    (ARRIVAL[m], ARRIVAL[n]) for n in range(EARLY, len(ARRIVAL)) for m in range(n + 1)
]


def start_kernel(v_hbm, v_ref, first_ref, second_ref, swap_ref, sums_ref, sems):
    copies = {}
    for g in ARRIVAL:
        part = pl.ds(g * GROUP, GROUP)
        copies[g] = pltpu.make_async_copy(v_hbm.at[part], v_ref.at[part], sems.at[g])
        copies[g].start()
    for n, g in enumerate(ARRIVAL[:EARLY]):
        copies[g].wait()
        if n == 0:
            write_edges(v_ref.at[KEEP - 1], first_ref, second_ref, swap_ref)
        for m in range(n + 1):
            gram_block(v_ref, sums_ref, ARRIVAL[m], g)
    for g in ARRIVAL[EARLY:]:
        copies[g].wait()


def start_call(basis):
    return pl.pallas_call(
        start_kernel,
        in_specs=[pl.BlockSpec(memory_space=pltpu.HBM)],
        out_specs=(VMEM_SPEC,) * 5,
        out_shape=(
            pltpu.VMEM((KEEP, ROWS, ZS), F32),
            *EDGE_SHAPES,
            pltpu.VMEM((KEEP, KEEP, 128), F32),
        ),
        scratch_shapes=[pltpu.SemaphoreType.DMA((KEEP // GROUP,))],
        compiler_params=PARAMS,
        name="start",
    )(pltpu.with_memory_space_constraint(basis, pltpu.HBM))


def gram_kernel(v_ref, early_ref, out_ref, sums_ref, matrix_ref):
    for ga, gb in LATE_PAIRS:
        gram_block(v_ref, sums_ref, ga, gb)
    early = sorted(g * GROUP + a for g in ARRIVAL[:EARLY] for a in range(GROUP))
    sub = iota((KEEP, 128), 0)
    in_early = (sub < (EARLY - 1) * GROUP) | (sub >= KEEP - GROUP)
    lane = iota((KEEP, 128), 1)
    matrix = jnp.zeros((KEEP, 128), F32)
    for i in range(KEEP):
        part = sums_ref[i]
        if i in early:
            part = jnp.where(in_early, early_ref[i], part)
        column = jnp.sum(part, axis=1, keepdims=True)
        matrix = jnp.where(lane == i, column, matrix)
    matrix_ref[pl.ds(0, KEEP), :] = matrix
    top = matrix_ref[pl.ds(0, HALF), :]
    bottom = pltpu.roll(matrix_ref[pl.ds(HALF, HALF), :], 128 - HALF, 1)
    lane = iota((HALF, 128), 1)
    sub = iota((HALF, 128), 0)
    diagonal = jnp.sum(jnp.where(lane == sub, top, 0.0), axis=1, keepdims=True)
    packed = jnp.where((lane > sub) | (lane >= HALF), top, bottom)
    packed = jnp.where(lane < KEEP, packed, jnp.where(lane == KEEP, diagonal, 0.0))
    matrix_ref[pl.ds(0, HALF), :] = packed
    packed = matrix_ref[pl.ds(0, PACK), :]
    for p in range(1, HALF // PACK):
        packed = packed + pltpu.roll(matrix_ref[pl.ds(p * PACK, PACK), :], p * PACK_LANES, 1)
    for r in range(PACK):
        out_ref[:, pl.ds(r * 128, 128)] = packed[r : r + 1]


def gram_call(v, early):
    return pl.pallas_call(
        gram_kernel,
        in_specs=[VMEM_SPEC, VMEM_SPEC],
        out_specs=VMEM_SPEC,
        out_shape=jax.ShapeDtypeStruct((1, PACK * 128), F32),
        scratch_shapes=[pltpu.VMEM((KEEP, KEEP, 128), F32), pltpu.VMEM((BASIS, 128), F32)],
        compiler_params=PARAMS,
        name="gram",
    )(v, early)


def dot_all(v_ref, others, x_ref, dots_ref):
    dots_ref[...] = jnp.zeros((BASIS, 128), F32)
    batch = 12

    def run(reads, base):
        def step(c, accs):
            rows = pl.ds(pl.multiple_of(c * CHUNK, CHUNK), CHUNK)
            x = x_ref[rows, :]
            return tuple(acc + fold_tiles(read(rows) * x) for acc, read in zip(accs, reads))

        zero = jnp.zeros((8, ZS), F32)
        accs = lax.fori_loop(0, ROWS // CHUNK, step, tuple(zero for _ in reads))
        for n, acc in enumerate(accs):
            dots_ref[pl.ds(base + n, 1), :] = fold_row(acc)

    for first in range(0, KEEP, batch):
        run([lambda rows, i=i: v_ref[i, rows, :] for i in range(first, first + batch)], first)
    if others:
        run([lambda rows, r=r: r[rows, :] for r in others], KEEP)
    return to_row(jnp.sum(dots_ref[...], axis=1, keepdims=True))


def self_dots_kernel(count, *refs):
    v_ref, *others = refs[: 1 + count]
    out_ref, dots_ref = refs[1 + count :]
    out_ref[...] = dot_all(v_ref, others, others[-1], dots_ref)


def self_dots_call(v, created):
    count = len(created)
    return pl.pallas_call(
        functools.partial(self_dots_kernel, count),
        in_specs=[VMEM_SPEC] * (1 + count),
        out_specs=VMEM_SPEC,
        out_shape=jax.ShapeDtypeStruct((1, 128), F32),
        scratch_shapes=[pltpu.VMEM((BASIS, 128), F32)],
        compiler_params=PARAMS,
    )(v, *created)


LAST_SHAPES = (
    jax.ShapeDtypeStruct((1, 128), F32),
    jax.ShapeDtypeStruct((1, 128), F32),
    jax.ShapeDtypeStruct((1,), jnp.int32),
)


def write_for_all(out_ref, rows):
    count = len(rows)
    period = count
    while period % 8:
        period += count
    for tile in range(period // 8):
        sub = iota((8, 128), 0)
        block = jnp.zeros((8, 128), F32)
        for r in range(8):
            block = jnp.where(sub == r, rows[(8 * tile + r) % count], block)
        for p in range(out_ref.shape[0] // period):
            out_ref[pl.ds(p * period + 8 * tile, 8), :] = block


def payload_rows(count):
    return 2 if count else 1 + PACK


def image_kernel(count, *refs):
    v_ref, *others = refs[: 1 + count]
    first_ref, second_ref, swap_ref, reaction_ref, extra_ref = refs[1 + count : 6 + count]
    w_ref, out_ref, dots_ref, pad_ref = refs[6 + count :]
    odd = lax.axis_index("gx") % 2 == 1
    upper = lax.axis_index("gy").astype(F32)
    lower = 1.0 - upper
    source = others[-1] if others else v_ref.at[KEEP - 1]
    lane = iota((YS, ZS), 1)
    center = -6.0 - 1.5 * sum(WIND_SPEEDS)
    near = [1.0 + 2.0 * s for s in WIND_SPEEDS]
    far = [-0.5 * s for s in WIND_SPEEDS]

    def plane(x):
        if x < 0:
            rows = pl.ds((x + 2) * YS, YS)
            return jnp.where(odd, first_ref[rows, :], second_ref[rows, :])
        if x >= XS:
            rows = pl.ds(0, YS)
            return jnp.where(odd, second_ref[rows, :], first_ref[rows, :])
        return source[pl.ds(x * YS, YS), :]

    for x in range(XS):
        mine = plane(x)
        pad_ref[x, pl.ds(8, YS), :] = mine
        edge = swap_ref[pl.ds(2 * x, 2), :]
        pad_ref[x, pl.ds(6, 2), :] = edge * upper
        pad_ref[x, pl.ds(72, 1), :] = edge[0:1] * lower
        image = (center - reaction_ref[pl.ds(x * YS, YS), :]) * mine
        image = image + plane(x + 1) + near[0] * plane(x - 1) + far[0] * plane(x - 2)
        image = (
            image
            + pad_ref[x, pl.ds(9, YS), :]
            + near[1] * pad_ref[x, pl.ds(7, YS), :]
            + far[1] * pad_ref[x, pl.ds(6, YS), :]
        )
        image = (
            image
            + jnp.where(lane < ZS - 1, pltpu.roll(mine, ZS - 1, 1), 0.0)
            + near[2] * jnp.where(lane >= 1, pltpu.roll(mine, 1, 1), 0.0)
            + far[2] * jnp.where(lane >= 2, pltpu.roll(mine, 2, 1), 0.0)
        )
        w_ref[pl.ds(x * YS, YS), :] = image
    more = [w_ref] if count == STEPS - 1 else []
    rows = [dot_all(v_ref, others + more, w_ref, dots_ref)]
    rows += [extra_ref[:, pl.ds(128 * r, 128)] for r in range(payload_rows(count) - 1)]
    write_for_all(out_ref, rows)


def image_call(v, created, halo, reaction, extra, devices):
    count = len(created)
    return pl.pallas_call(
        functools.partial(image_kernel, count),
        in_specs=[VMEM_SPEC] * (6 + count),
        out_specs=(VMEM_SPEC, VMEM_SPEC),
        out_shape=(
            pltpu.VMEM((ROWS, ZS), F32),
            jax.ShapeDtypeStruct((devices * payload_rows(count), 128), F32),
        ),
        scratch_shapes=[
            pltpu.VMEM((BASIS, 128), F32),
            pltpu.VMEM((XS, YS + 16, ZS), F32),
        ],
        compiler_params=PARAMS,
    )(v, *created, *halo, reaction, extra)


STATE_G, STATE_H, STATE_D, STATE_ROWS = 0, BASIS, 2 * BASIS, 2 * BASIS + 8


def summed_rows(recv_ref, count):
    period = count
    while period % 8:
        period += count
    total = jnp.sum(recv_ref[...].reshape(-1, period, 128), axis=0)
    if count in (1, 2):
        while count < 8:
            total = total + pltpu.roll(total, 8 - count, 0)
            count *= 2
        return total
    return sum(total[p : p + count] for p in range(0, period, count))


def unpacked_gram(packed, pack_ref):
    pack_ref[...] = jnp.zeros((128, 128), F32)
    for p in range(HALF // PACK):
        part = packed
        if p:
            part = pltpu.roll(part, 128 - p * PACK_LANES, 1)
        pack_ref[pl.ds(p * PACK, PACK), :] = part
    turned = jnp.transpose(pack_ref[...])
    plain = pack_ref[pl.ds(0, HALF), :]
    lane = iota((HALF, 128), 1)
    sub = iota((HALF, 128), 0)
    diagonal = jnp.sum(jnp.where(lane == KEEP, plain, 0.0), axis=1, keepdims=True)
    top = jnp.where((lane > sub) | (lane >= HALF), plain, turned[:HALF])
    top = jnp.where(lane == sub, diagonal, top)
    last = jnp.where(lane <= sub, plain, turned[:HALF])
    pack_ref[...] = turned
    bottom = jnp.where(lane < HALF, pack_ref[pl.ds(HALF, HALF), :], pltpu.roll(last, HALF, 1))
    pack_ref[pl.ds(0, HALF), :] = jnp.where(lane < KEEP, top, 0.0)
    pack_ref[pl.ds(HALF, HALF), :] = jnp.where(lane < KEEP, bottom, 0.0)
    pack_ref[pl.ds(KEEP, STEPS), :] = jnp.zeros((STEPS, 128), F32)


def combine_kernel(count, cells, *refs):
    recv_ref, w_ref, v_ref, *others = refs[: 3 + count]
    pos = 3 + count
    if count:
        state_in = refs[pos]
        pos += 1
    u_ref, state_ref, *outs, weight_ref, pack_ref = refs[pos:]
    final = count == STEPS - 1
    if final:
        square_ref, guess_ref, sound_ref = outs
    lane = iota((1, 128), 1)
    lanes = iota((BASIS, 128), 1)
    subs = iota((BASIS, 128), 0)
    scale = 1.0 / cells
    if count == 0:
        total = summed_rows(recv_ref, 1 + PACK) * scale
        unpacked_gram(total[1 : 1 + PACK], pack_ref)
        gram = pack_ref[pl.ds(0, BASIS), :]
        hess = jnp.zeros((BASIS, 128), F32)
        inverse_row = jnp.where(lane < KEEP, 1.0, 0.0)
        first_row = total[0:1]
        inverse = jnp.ones((1, 1), F32)
    else:
        total = summed_rows(recv_ref, 2) * scale
        newest = KEEP + count - 1
        raw_first, raw_gram = total[0:1], total[1:2]
        square = jnp.sum(jnp.where(lane == newest, raw_gram, 0.0), axis=1, keepdims=True)
        norm = jnp.sqrt(square + EPSILON)
        inverse = 1.0 / norm
        inverse_row = jnp.where(lane == newest, inverse, state_in[pl.ds(STATE_D, 1), :])
        gram_row = raw_gram * inverse_row * inverse
        first_row = raw_first * inverse_row * inverse
        gram = state_in[pl.ds(STATE_G, BASIS), :]
        gram = jnp.where(lanes == newest, to_column(gram_row), gram)
        gram = jnp.where(subs == newest, gram_row, gram)
        hess = state_in[pl.ds(STATE_H, BASIS), :]
        hess = jnp.where((subs == newest) & (lanes == count - 1), norm, hess)
    first = to_column(first_row)
    folded = jnp.sum(gram * first_row, axis=1, keepdims=True)
    weights = first + (first - folded)
    hess = jnp.where((lanes == count) & (subs < KEEP + count), weights, hess)
    if final:
        image_square = jnp.sum(jnp.where(lane == BASIS - 1, raw_first, 0.0), axis=1, keepdims=True)
        image_square = image_square * inverse * inverse
        again = jnp.sum(gram * to_row(weights), axis=1, keepdims=True)
        guess = image_square - jnp.sum(weights * (2.0 * first - again), axis=0, keepdims=True)
        guess_ref[...] = jnp.where(lane == 0, guess, 0.0)
        sound = jnp.where(guess > SOUND_SHARE * image_square, 1, 0)
        sound_ref[0] = sound[0, 0]
    state_ref[pl.ds(STATE_G, BASIS), :] = gram
    state_ref[pl.ds(STATE_H, BASIS), :] = hess
    state_ref[pl.ds(STATE_D, 8), :] = jnp.broadcast_to(inverse_row, (8, 128))
    weight_ref[...] = jnp.broadcast_to(weights * to_column(inverse_row), (BASIS, ZS))

    def step(c, acc):
        rows = pl.ds(pl.multiple_of(c * CHUNK, CHUNK), CHUNK)
        value = w_ref[rows, :] * inverse
        for i in range(KEEP):
            value = value - weight_ref[pl.ds(i, 1), :] * v_ref[i, rows, :]
        for i, other in enumerate(others):
            value = value - weight_ref[pl.ds(KEEP + i, 1), :] * other[rows, :]
        u_ref[rows, :] = value
        return acc + fold_tiles(value * value)

    acc = lax.fori_loop(0, ROWS // CHUNK, step, jnp.zeros((8, ZS), F32))
    if final:
        square_ref[...] = fold_row(acc)
    else:
        write_edges(u_ref, *outs)


def combine_call(recv, w, v, created, state, cells):
    count = len(created)
    states = [state] if created else []
    final = count == STEPS - 1
    return pl.pallas_call(
        functools.partial(combine_kernel, count, cells),
        in_specs=[VMEM_SPEC] * (3 + count + len(states)),
        out_specs=(VMEM_SPEC,) * 4 + (SMEM_SPEC if final else VMEM_SPEC,),
        out_shape=(
            pltpu.VMEM((ROWS, ZS), F32),
            jax.ShapeDtypeStruct((STATE_ROWS, 128), F32),
            *(LAST_SHAPES if final else EDGE_SHAPES),
        ),
        scratch_shapes=[pltpu.VMEM((BASIS, ZS), F32), pltpu.VMEM((128, 128), F32)],
        compiler_params=PARAMS,
    )(recv, w, v, *created, *states)


def finish_kernel(*refs):
    square_ref, state_ref, *created = refs[: 2 + STEPS]
    new_ref, hess_ref = refs[2 + STEPS :]
    lane = iota((1, 128), 1)
    norm = jnp.sqrt(jnp.sum(square_ref[...], axis=1, keepdims=True) + EPSILON)
    lanes = iota((BASIS, 128), 1)
    subs = iota((BASIS, 128), 0)
    hess = state_ref[pl.ds(STATE_H, BASIS), :]
    hess = jnp.where((subs == BASIS - 1) & (lanes == STEPS - 1), norm, hess)
    hess_ref[...] = jnp.transpose(jnp.concatenate([hess, jnp.zeros((128 - BASIS, 128), F32)], axis=0))[:STEPS, :BASIS]
    inverse_row = state_ref[pl.ds(STATE_D, 1), :]
    for j, u_ref in enumerate(created):
        if j == STEPS - 1:
            inverse = 1.0 / norm
        else:
            inverse = jnp.sum(jnp.where(lane == KEEP + j, inverse_row, 0.0), axis=1, keepdims=True)
        for c in range(ROWS // CHUNK):
            rows = pl.ds(c * CHUNK, CHUNK)
            new_ref[j, rows, :] = u_ref[rows, :] * inverse


def finish_call(square, state, created):
    return pl.pallas_call(
        finish_kernel,
        in_specs=[VMEM_SPEC] * (2 + STEPS),
        out_specs=(VMEM_SPEC, VMEM_SPEC),
        out_shape=(
            jax.ShapeDtypeStruct((STEPS, ROWS, ZS), F32),
            jax.ShapeDtypeStruct((STEPS, BASIS), F32),
        ),
        compiler_params=PARAMS,
        name="finish",
    )(square, state, *created)


def exchange(first, second, swap):
    count = lax.axis_size("gx")

    def pairs(start):
        lower = range(start, count - 1, 2)
        return [(i, i + 1) for i in lower] + [(i + 1, i) for i in lower]

    second = lax.ppermute(second, "gx", pairs(1))
    first = lax.ppermute(first, "gx", pairs(0))
    swap = lax.ppermute(swap, "gy", [(0, 1), (1, 0)])
    return first, second, swap


def from_all(payload):
    axes = ("gy", "gx")
    devices = lax.axis_size(axes)
    copies = payload.reshape(devices, 1, -1)
    got = lax.all_to_all(copies, axes, split_axis=0, concat_axis=0, tiled=True)
    return got.reshape(-1, 128)


def body(basis_vectors, reaction):
    devices = lax.axis_size(("gy", "gx"))
    cells = float(ROWS * ZS * devices)
    basis = basis_vectors.reshape(KEEP, ROWS, ZS)
    v, *edges, early = start_call(basis)
    halo = exchange(*edges)
    reaction = reaction.reshape(ROWS, ZS)
    extra = gram_call(v, early)
    created = []
    state = None
    for j in range(STEPS):
        if j:
            extra = self_dots_call(v, created)
        w, payload = image_call(v, created, halo, reaction, extra, devices)
        recv = from_all(payload)
        u, state, *edges = combine_call(recv, w, v, created, state, cells)
        created.append(u)
        if j + 1 < STEPS:
            halo = exchange(*edges)
    square, guess, sound = edges
    square = lax.cond(
        sound[0] == 1,
        lambda guess, square: guess,
        lambda guess, square: jnp.sum(from_all(square), axis=0, keepdims=True) * (1.0 / cells),
        guess,
        jnp.broadcast_to(square, (devices, 128)),
    )
    new, hessenberg = finish_call(square, state, created)
    return new.reshape(STEPS, XS, YS, ZS), hessenberg.T


def solution(mesh):
    return jax.shard_map(
        body,
        mesh=mesh,
        in_specs=(P(None, "gx", "gy", None), P("gx", "gy", None)),
        out_specs=(P(None, "gx", "gy", None), P()),
        check_vma=False,
    )
```

```python
import functools

import jax
import jax.numpy as jnp
from jax import lax
from jax.experimental import pallas as pl
from jax.experimental.pallas import tpu as pltpu
from jax.sharding import PartitionSpec as P


KEEP = 36
STEPS = 4
BASIS = KEEP + STEPS
WIND_SPEEDS = (0.9, 0.6, 0.4)
EPSILON = 1e-06
F32 = jnp.float32

XS, YS, ZS = 4, 64, 256
ROWS = XS * YS
GROUP = 4
GRAM_ROWS = 64
HALF = KEEP // 2
PACK = 6
PACK_LANES = 40
CHUNK = 32
SOUND_SHARE = 0.05

PARAMS = pltpu.CompilerParams(vmem_limit_bytes=16 * 2**20)
SMEM_SPEC = pl.BlockSpec(memory_space=pltpu.SMEM)
VMEM_SPEC = pl.BlockSpec(memory_space=pltpu.VMEM)


def iota(shape, axis):
    return lax.broadcasted_iota(jnp.int32, shape, axis)


def to_column(row):
    pick = iota((BASIS, 128), 0) == iota((BASIS, 128), 1)
    return jnp.sum(jnp.where(pick, row, 0.0), axis=1, keepdims=True)


def to_row(column):
    pick = iota((BASIS, 128), 0) == iota((BASIS, 128), 1)
    return jnp.sum(jnp.where(pick, column, 0.0), axis=0, keepdims=True)


def fold_tiles(block):
    return jnp.sum(block.reshape(-1, 8, ZS), axis=0)


def fold_row(acc):
    return jnp.sum(acc[:, :128] + acc[:, 128:], axis=0, keepdims=True)


def gram_block(v_ref, sums_ref, ga, gb):
    pairs = [(a, b) for a in range(GROUP) for b in range(GROUP) if ga != gb or a <= b]

    def step(t, accs):
        accs = list(accs)
        for part in range(GRAM_ROWS // 8):
            rows = pl.ds(pl.multiple_of(t * GRAM_ROWS, GRAM_ROWS) + 8 * part, 8)
            for half in range(2):
                lanes = pl.ds(half * 128, 128)
                left = [v_ref[ga * GROUP + a, rows, lanes] for a in range(GROUP)]
                right = left
                if ga != gb:
                    right = [v_ref[gb * GROUP + b, rows, lanes] for b in range(GROUP)]
                for n, (a, b) in enumerate(pairs):
                    accs[n] = accs[n] + left[a] * right[b]
        return tuple(accs)

    zero = jnp.zeros((8, 128), F32)
    accs = lax.fori_loop(0, ROWS // GRAM_ROWS, step, tuple(zero for _ in pairs))
    for (a, b), acc in zip(pairs, accs):
        row = jnp.sum(acc, axis=0, keepdims=True)
        i, j = ga * GROUP + a, gb * GROUP + b
        sums_ref[i, pl.ds(j, 1), :] = row
        if i != j:
            sums_ref[j, pl.ds(i, 1), :] = row


def write_edges(u_ref, first_ref, second_ref, swap_ref):
    odd = lax.axis_index("gx") % 2 == 1
    upper = lax.axis_index("gy") == 1
    for x in range(2):
        low = u_ref[pl.ds(x * YS, YS), :]
        high = u_ref[pl.ds((XS - 2 + x) * YS, YS), :]
        first_ref[pl.ds(x * YS, YS), :] = jnp.where(odd, low, high)
        second_ref[pl.ds(x * YS, YS), :] = jnp.where(odd, high, low)
    for x in range(XS):
        low = u_ref[pl.ds(x * YS, 2), :]
        high = u_ref[pl.ds(x * YS + YS - 2, 2), :]
        swap_ref[pl.ds(2 * x, 2), :] = jnp.where(upper, low, high)


EDGE_SHAPES = (
    jax.ShapeDtypeStruct((2 * YS, ZS), F32),
    jax.ShapeDtypeStruct((2 * YS, ZS), F32),
    jax.ShapeDtypeStruct((2 * XS, ZS), F32),
)


ARRIVAL = [KEEP // GROUP - 1, *range(KEEP // GROUP - 1)]
EARLY = 4
LATE_PAIRS = [
    (ARRIVAL[m], ARRIVAL[n]) for n in range(EARLY, len(ARRIVAL)) for m in range(n + 1)
]


def start_kernel(v_hbm, v_ref, first_ref, second_ref, swap_ref, sums_ref, sems):
    copies = {}
    for g in ARRIVAL:
        part = pl.ds(g * GROUP, GROUP)
        copies[g] = pltpu.make_async_copy(v_hbm.at[part], v_ref.at[part], sems.at[g])
        copies[g].start()
    for n, g in enumerate(ARRIVAL[:EARLY]):
        copies[g].wait()
        if n == 0:
            write_edges(v_ref.at[KEEP - 1], first_ref, second_ref, swap_ref)
        for m in range(n + 1):
            gram_block(v_ref, sums_ref, ARRIVAL[m], g)
    for g in ARRIVAL[EARLY:]:
        copies[g].wait()


def start_call(basis):
    return pl.pallas_call(
        start_kernel,
        in_specs=[pl.BlockSpec(memory_space=pltpu.HBM)],
        out_specs=(VMEM_SPEC,) * 5,
        out_shape=(
            pltpu.VMEM((KEEP, ROWS, ZS), F32),
            *EDGE_SHAPES,
            pltpu.VMEM((KEEP, KEEP, 128), F32),
        ),
        scratch_shapes=[pltpu.SemaphoreType.DMA((KEEP // GROUP,))],
        compiler_params=PARAMS,
        name="start",
    )(pltpu.with_memory_space_constraint(basis, pltpu.HBM))


def gram_kernel(v_ref, early_ref, out_ref, sums_ref, matrix_ref):
    for ga, gb in LATE_PAIRS:
        gram_block(v_ref, sums_ref, ga, gb)
    early = sorted(g * GROUP + a for g in ARRIVAL[:EARLY] for a in range(GROUP))

    def line(i, start):
        part = sums_ref[i, pl.ds(start, HALF), :]
        if i in early:
            sub = iota((HALF, 128), 0) + start
            in_early = (sub < (EARLY - 1) * GROUP) | (sub >= KEEP - GROUP)
            part = jnp.where(in_early, early_ref[i, pl.ds(start, HALF), :], part)
        return part

    sub = iota((HALF, 128), 0)
    lane = iota((HALF, 128), 1)
    packed = jnp.zeros((HALF, 128), F32)
    diagonal = jnp.zeros((HALF, 128), F32)
    for i in range(KEEP):
        part = line(i, 0)
        if i < HALF:
            diagonal = jnp.where(sub == i, part, diagonal)
            part = jnp.where(sub < i, part, line(HALF + i, HALF))
        packed = jnp.where(lane == i, jnp.sum(part, axis=1, keepdims=True), packed)
    packed = jnp.where(lane == KEEP, jnp.sum(diagonal, axis=1, keepdims=True), packed)
    matrix_ref[pl.ds(0, HALF), :] = packed
    packed = matrix_ref[pl.ds(0, PACK), :]
    for p in range(1, HALF // PACK):
        packed = packed + pltpu.roll(matrix_ref[pl.ds(p * PACK, PACK), :], p * PACK_LANES, 1)
    for r in range(PACK):
        out_ref[:, pl.ds(r * 128, 128)] = packed[r : r + 1]


def gram_call(v, early):
    return pl.pallas_call(
        gram_kernel,
        in_specs=[VMEM_SPEC, VMEM_SPEC],
        out_specs=VMEM_SPEC,
        out_shape=jax.ShapeDtypeStruct((1, PACK * 128), F32),
        scratch_shapes=[pltpu.VMEM((KEEP, KEEP, 128), F32), pltpu.VMEM((BASIS, 128), F32)],
        compiler_params=PARAMS,
        name="gram",
    )(v, early)


def dot_all(v_ref, others, x_refs, dots_refs, chunks=ROWS // CHUNK, skip=False):
    batch = 12 // len(x_refs)
    for dots_ref in dots_refs:
        dots_ref[...] = jnp.zeros((BASIS, 128), F32)

    def run(reads, base):
        def step(c, accs):
            start = c * CHUNK
            if skip:
                start = start + (c // (2 * YS // CHUNK)) * YS
            rows = pl.ds(pl.multiple_of(start, CHUNK), CHUNK)
            xs = [x_ref[rows, :] for x_ref in x_refs]
            new = []
            for n, read in enumerate(reads):
                value = read(rows)
                new += [accs[n * len(xs) + m] + fold_tiles(value * x) for m, x in enumerate(xs)]
            return tuple(new)

        zero = jnp.zeros((8, ZS), F32)
        accs = lax.fori_loop(0, chunks, step, (zero,) * (len(reads) * len(x_refs)))
        for n, acc in enumerate(accs):
            row = base + n // len(x_refs)
            dots_refs[n % len(x_refs)][pl.ds(row, 1), :] = fold_row(acc)

    for first in range(0, KEEP, batch):
        run([lambda rows, i=i: v_ref[i, rows, :] for i in range(first, first + batch)], first)
    if others:
        run([lambda rows, r=r: r[rows, :] for r in others], KEEP)
    return [to_row(jnp.sum(dots_ref[...], axis=1, keepdims=True)) for dots_ref in dots_refs]


CENTER = -6.0 - 1.5 * sum(WIND_SPEEDS)
NEAR = [1.0 + 2.0 * s for s in WIND_SPEEDS]
FAR = [-0.5 * s for s in WIND_SPEEDS]


def inner_image(source, swap_ref, reaction_ref, pad_ref, x):
    upper = lax.axis_index("gy").astype(F32)
    lane = iota((YS, ZS), 1)
    mine = source[pl.ds(x * YS, YS), :]
    pad_ref[x, pl.ds(8, YS), :] = mine
    edge = swap_ref[pl.ds(2 * x, 2), :]
    pad_ref[x, pl.ds(6, 2), :] = edge * upper
    pad_ref[x, pl.ds(72, 1), :] = edge[0:1] * (1.0 - upper)
    image = (CENTER - reaction_ref[pl.ds(x * YS, YS), :]) * mine
    for distance, factor in ((1, 1.0), (-1, NEAR[0]), (-2, FAR[0])):
        if 0 <= x + distance < XS:
            image = image + factor * source[pl.ds((x + distance) * YS, YS), :]
    image = (
        image
        + pad_ref[x, pl.ds(9, YS), :]
        + NEAR[1] * pad_ref[x, pl.ds(7, YS), :]
        + FAR[1] * pad_ref[x, pl.ds(6, YS), :]
    )
    return (
        image
        + jnp.where(lane < ZS - 1, pltpu.roll(mine, ZS - 1, 1), 0.0)
        + NEAR[2] * jnp.where(lane >= 1, pltpu.roll(mine, 1, 1), 0.0)
        + FAR[2] * jnp.where(lane >= 2, pltpu.roll(mine, 2, 1), 0.0)
    )


def outer_image(first_ref, second_ref):
    odd = lax.axis_index("gx") % 2 == 1

    def below(rows):
        return jnp.where(odd, first_ref[rows, :], second_ref[rows, :])

    two, one = below(pl.ds(0, YS)), below(pl.ds(YS, YS))
    rows = pl.ds(0, YS)
    above = jnp.where(odd, second_ref[rows, :], first_ref[rows, :])
    return {0: NEAR[0] * one + FAR[0] * two, 1: FAR[0] * one, XS - 1: above}


LAST_SHAPES = (
    jax.ShapeDtypeStruct((1, 128), F32),
    jax.ShapeDtypeStruct((1, 128), F32),
    jax.ShapeDtypeStruct((1,), jnp.int32),
)


def write_for_all(out_ref, rows):
    count = len(rows)
    period = count
    while period % 8:
        period += count
    for tile in range(period // 8):
        sub = iota((8, 128), 0)
        block = jnp.zeros((8, 128), F32)
        for r in range(8):
            block = jnp.where(sub == r, rows[(8 * tile + r) % count], block)
        for p in range(out_ref.shape[0] // period):
            out_ref[pl.ds(p * period + 8 * tile, 8), :] = block


def first_image_kernel(
    v_ref, first_ref, second_ref, swap_ref, reaction_ref, extra_ref, w_ref, out_ref, dots_ref, pad_ref
):
    outer = outer_image(first_ref, second_ref)
    for x in range(XS):
        image = inner_image(v_ref.at[KEEP - 1], swap_ref, reaction_ref, pad_ref, x)
        w_ref[pl.ds(x * YS, YS), :] = image + outer[x] if x in outer else image
    rows = dot_all(v_ref, [], [w_ref], [dots_ref])
    rows += [extra_ref[:, pl.ds(128 * r, 128)] for r in range(PACK)]
    write_for_all(out_ref, rows)


def first_image_call(v, halo, reaction, extra, devices):
    return pl.pallas_call(
        first_image_kernel,
        in_specs=[VMEM_SPEC] * 6,
        out_specs=(VMEM_SPEC, VMEM_SPEC),
        out_shape=(
            pltpu.VMEM((ROWS, ZS), F32),
            jax.ShapeDtypeStruct((devices * (1 + PACK), 128), F32),
        ),
        scratch_shapes=[
            pltpu.VMEM((BASIS, 128), F32),
            pltpu.VMEM((XS, YS + 16, ZS), F32),
        ],
        compiler_params=PARAMS,
        name="image_0",
    )(v, *halo, reaction, extra)


def inner_kernel(count, *refs):
    v_ref, near_ref, far_ref, *older = refs[: 2 + count]
    swap_ref, reaction_ref, u_ref, w_ref, out_ref, dots_ref, more_ref, pad_ref = refs[2 + count :]
    odd = lax.axis_index("gx") % 2 == 1
    for x in range(2):
        rows = pl.ds(x * YS, YS)
        near, far = near_ref[rows, :], far_ref[rows, :]
        u_ref[pl.ds(x * YS, YS), :] = jnp.where(odd, near, far)
        u_ref[pl.ds((2 + x) * YS, YS), :] = jnp.where(odd, far, near)
    for x in range(XS):
        w_ref[pl.ds(x * YS, YS), :] = inner_image(u_ref, swap_ref, reaction_ref, pad_ref, x)
    rows = dot_all(v_ref, [*older, u_ref], [w_ref, u_ref], [dots_ref, more_ref])
    for n, row in enumerate(rows):
        out_ref[pl.ds(n, 1), :] = row


def inner_call(v, near, far, older, swap, reaction):
    count = 1 + len(older)
    return pl.pallas_call(
        functools.partial(inner_kernel, count),
        in_specs=[VMEM_SPEC] * (4 + count),
        out_specs=(VMEM_SPEC,) * 3,
        out_shape=(
            pltpu.VMEM((ROWS, ZS), F32),
            pltpu.VMEM((ROWS, ZS), F32),
            jax.ShapeDtypeStruct((2, 128), F32),
        ),
        scratch_shapes=[
            pltpu.VMEM((BASIS, 128), F32),
            pltpu.VMEM((BASIS, 128), F32),
            pltpu.VMEM((XS, YS + 16, ZS), F32),
        ],
        compiler_params=PARAMS,
    )(v, near, far, *older, swap, reaction)


def outer_kernel(count, *refs):
    v_ref, *others = refs[: 1 + count]
    first_ref, second_ref, inner_ref, extra_ref = refs[1 + count : 5 + count]
    w_ref, out_ref, dots_ref, delta_ref = refs[5 + count :]
    outer = outer_image(first_ref, second_ref)
    for x in range(XS):
        rows = pl.ds(x * YS, YS)
        image = inner_ref[rows, :]
        if x in outer:
            delta_ref[rows, :] = outer[x]
            image = image + outer[x]
        w_ref[rows, :] = image
    (row,) = dot_all(v_ref, others, [delta_ref], [dots_ref], 3 * YS // CHUNK, True)
    row = row + extra_ref[pl.ds(0, 1), :]
    if count == STEPS - 1:
        square = jnp.zeros((8, ZS), F32)
        for c in range(ROWS // CHUNK):
            image = w_ref[pl.ds(c * CHUNK, CHUNK), :]
            square = square + fold_tiles(image * image)
        square = jnp.sum(fold_row(square), axis=1, keepdims=True)
        row = jnp.where(iota((1, 128), 1) == BASIS - 1, square, row)
    write_for_all(out_ref, [row, extra_ref[pl.ds(1, 1), :]])


def outer_call(v, created, first, second, inner, extra, devices):
    count = len(created)
    return pl.pallas_call(
        functools.partial(outer_kernel, count),
        in_specs=[VMEM_SPEC] * (5 + count),
        out_specs=(VMEM_SPEC, VMEM_SPEC),
        out_shape=(
            pltpu.VMEM((ROWS, ZS), F32),
            jax.ShapeDtypeStruct((2 * devices, 128), F32),
        ),
        scratch_shapes=[pltpu.VMEM((BASIS, 128), F32), pltpu.VMEM((ROWS, ZS), F32)],
        compiler_params=PARAMS,
    )(v, *created, first, second, inner, extra)


STATE_G, STATE_H, STATE_D, STATE_ROWS = 0, BASIS, 2 * BASIS, 2 * BASIS + 8


def summed_rows(recv_ref, count):
    period = count
    while period % 8:
        period += count
    total = jnp.sum(recv_ref[...].reshape(-1, period, 128), axis=0)
    if count in (1, 2):
        while count < 8:
            total = total + pltpu.roll(total, 8 - count, 0)
            count *= 2
        return total
    return sum(total[p : p + count] for p in range(0, period, count))


def unpacked_gram(packed, pack_ref):
    pack_ref[...] = jnp.zeros((128, 128), F32)
    for p in range(HALF // PACK):
        part = packed
        if p:
            part = pltpu.roll(part, 128 - p * PACK_LANES, 1)
        pack_ref[pl.ds(p * PACK, PACK), :] = part
    turned = jnp.transpose(pack_ref[...])
    plain = pack_ref[pl.ds(0, HALF), :]
    lane = iota((HALF, 128), 1)
    sub = iota((HALF, 128), 0)
    diagonal = jnp.sum(jnp.where(lane == KEEP, plain, 0.0), axis=1, keepdims=True)
    top = jnp.where((lane > sub) | (lane >= HALF), plain, turned[:HALF])
    top = jnp.where(lane == sub, diagonal, top)
    last = jnp.where(lane <= sub, plain, turned[:HALF])
    pack_ref[...] = turned
    bottom = jnp.where(lane < HALF, pack_ref[pl.ds(HALF, HALF), :], pltpu.roll(last, HALF, 1))
    pack_ref[pl.ds(0, HALF), :] = jnp.where(lane < KEEP, top, 0.0)
    pack_ref[pl.ds(HALF, HALF), :] = jnp.where(lane < KEEP, bottom, 0.0)
    pack_ref[pl.ds(KEEP, STEPS), :] = jnp.zeros((STEPS, 128), F32)


def solve_weights(count, cells, recv_ref, state_in, state_ref, weight_ref, pack_ref):
    lane = iota((1, 128), 1)
    lanes = iota((BASIS, 128), 1)
    subs = iota((BASIS, 128), 0)
    sub = iota((BASIS, 1), 0)
    scale = 1.0 / cells

    def spread(values):
        return jnp.sum(values, axis=1, keepdims=True)

    if count == 0:
        total = summed_rows(recv_ref, 1 + PACK) * scale
        unpacked_gram(total[1 : 1 + PACK], pack_ref)
        gram = pack_ref[pl.ds(0, BASIS), :]
        hess = jnp.zeros((BASIS, 128), F32)
        inverse_row = jnp.where(lane < KEEP, 1.0, 0.0)
        inverse_column = jnp.where(sub < KEEP, 1.0, 0.0)
        first_row = total[0:1]
        inverse = jnp.ones((1, 1), F32)
        image_square = None
        first = to_column(first_row)
        folded = spread(gram * first_row)
    else:
        total = summed_rows(recv_ref, 2) * scale
        newest = KEEP + count - 1
        raw_first, raw_gram = total[0:1], total[1:2]
        inverse_row = state_in[pl.ds(STATE_D, 1), :]
        gram = state_in[pl.ds(STATE_G, BASIS), :]
        hess = state_in[pl.ds(STATE_H, BASIS), :]
        part_first, part_gram = raw_first * inverse_row, raw_gram * inverse_row
        square = spread(jnp.where(lane == newest, raw_gram, 0.0))
        first_newest = spread(jnp.where(lane == newest, raw_first, 0.0))
        image_square = spread(jnp.where(lane == BASIS - 1, raw_first, 0.0))
        crossed = spread(part_gram * part_first)
        first_column, gram_column = to_column(part_first), to_column(part_gram)
        inverse_column = to_column(inverse_row)
        folded = spread(gram * part_first)
        norm = jnp.sqrt(square + EPSILON)
        inverse = 1.0 / norm
        own = square * inverse * inverse
        first_newest = first_newest * inverse * inverse
        image_square = image_square * inverse * inverse
        mine = sub == newest
        first = jnp.where(mine, first_newest, first_column * inverse)
        gram_column = gram_column * inverse
        folded = jnp.where(
            mine,
            crossed * inverse * inverse + own * first_newest,
            folded * inverse + gram_column * first_newest,
        )
        gram = jnp.where(lanes == newest, gram_column, gram)
        gram = jnp.where(subs == newest, part_gram * inverse, gram)
        gram = jnp.where((lanes == newest) & (subs == newest), own, gram)
        hess = jnp.where((subs == newest) & (lanes == count - 1), norm, hess)
        inverse_row = jnp.where(lane == newest, inverse, inverse_row)
        inverse_column = jnp.where(mine, inverse, inverse_column)
    weights = first + (first - folded)
    weight_ref[pl.ds(0, BASIS), :] = jnp.broadcast_to(weights * inverse_column, (BASIS, ZS))
    weight_ref[pl.ds(BASIS, 8), :] = jnp.broadcast_to(inverse, (8, ZS))
    hess = jnp.where((lanes == count) & (subs < KEEP + count), weights, hess)
    state_ref[pl.ds(STATE_G, BASIS), :] = gram
    state_ref[pl.ds(STATE_H, BASIS), :] = hess
    state_ref[pl.ds(STATE_D, 8), :] = jnp.broadcast_to(inverse_row, (8, 128))
    return weights, first, gram, image_square


def combined(rows, weight_ref, w_ref, v_ref, others):
    value = w_ref[rows, :] * weight_ref[pl.ds(BASIS, 1), :]
    for i in range(KEEP):
        value = value - weight_ref[pl.ds(i, 1), :] * v_ref[i, rows, :]
    for i, other in enumerate(others):
        value = value - weight_ref[pl.ds(KEEP + i, 1), :] * other[rows, :]
    return value


def combine_half(out_ref, high, weight_ref, w_ref, v_ref, others):
    start = high.astype(jnp.int32) * (ROWS // 2)

    def step(c, carry):
        rows = pl.ds(pl.multiple_of(start + c * CHUNK, CHUNK), CHUNK)
        out_ref[pl.ds(pl.multiple_of(c * CHUNK, CHUNK), CHUNK), :] = combined(
            rows, weight_ref, w_ref, v_ref, others
        )
        return carry

    lax.fori_loop(0, ROWS // 2 // CHUNK, step, 0)


HALF_SHAPE = jax.ShapeDtypeStruct((ROWS // 2, ZS), F32)
WEIGHT_SHAPE = (BASIS + 8, ZS)


def far_kernel(count, cells, *refs):
    recv_ref, w_ref, v_ref, *others = refs[: 3 + count]
    *states, far_ref, weight_ref, state_ref, pack_ref = refs[3 + count :]
    state_in = states[0] if states else None
    solve_weights(count, cells, recv_ref, state_in, state_ref, weight_ref, pack_ref)
    odd = lax.axis_index("gx") % 2 == 1
    combine_half(far_ref, odd, weight_ref, w_ref, v_ref, others)


def far_call(recv, w, v, created, state, cells):
    count = len(created)
    states = [state] if created else []
    return pl.pallas_call(
        functools.partial(far_kernel, count, cells),
        in_specs=[VMEM_SPEC] * (3 + count + len(states)),
        out_specs=(VMEM_SPEC,) * 3,
        out_shape=(
            HALF_SHAPE,
            pltpu.VMEM(WEIGHT_SHAPE, F32),
            jax.ShapeDtypeStruct((STATE_ROWS, 128), F32),
        ),
        scratch_shapes=[pltpu.VMEM((128, 128), F32)],
        compiler_params=PARAMS,
    )(recv, w, v, *created, *states)


def near_kernel(count, *refs):
    weight_ref, far_ref, w_ref, v_ref, *others = refs[: 4 + count]
    near_ref, swap_ref = refs[4 + count :]
    odd = lax.axis_index("gx") % 2 == 1
    upper = lax.axis_index("gy") == 1
    combine_half(near_ref, jnp.logical_not(odd), weight_ref, w_ref, v_ref, others)
    for x in range(XS):
        sides = []
        for y in (0, YS - 2):
            rows = pl.ds((x % 2) * YS + y, 2)
            low, high = (near_ref, far_ref) if x < 2 else (far_ref, near_ref)
            sides.append(jnp.where(odd, low[rows, :], high[rows, :]))
        swap_ref[pl.ds(2 * x, 2), :] = jnp.where(upper, *sides)


def near_call(weight, far, w, v, created):
    count = len(created)
    return pl.pallas_call(
        functools.partial(near_kernel, count),
        in_specs=[VMEM_SPEC] * (4 + count),
        out_specs=(VMEM_SPEC,) * 2,
        out_shape=(HALF_SHAPE, jax.ShapeDtypeStruct((2 * XS, ZS), F32)),
        compiler_params=PARAMS,
    )(weight, far, w, v, *created)


def last_kernel(cells, *refs):
    count = STEPS - 1
    recv_ref, w_ref, v_ref, *others = refs[: 3 + count]
    state_in, u_ref, state_ref, square_ref, guess_ref, sound_ref, weight_ref = refs[3 + count :]
    weights, first, gram, image_square = solve_weights(
        count, cells, recv_ref, state_in, state_ref, weight_ref, None
    )
    again = jnp.sum(gram * to_row(weights), axis=1, keepdims=True)
    guess = image_square - jnp.sum(weights * (2.0 * first - again), axis=0, keepdims=True)
    guess_ref[...] = jnp.where(iota((1, 128), 1) == 0, guess, 0.0)
    sound = jnp.where(guess > SOUND_SHARE * image_square, 1, 0)
    sound_ref[0] = sound[0, 0]

    def step(c, acc):
        rows = pl.ds(pl.multiple_of(c * CHUNK, CHUNK), CHUNK)
        value = combined(rows, weight_ref, w_ref, v_ref, others)
        u_ref[rows, :] = value
        return acc + fold_tiles(value * value)

    acc = lax.fori_loop(0, ROWS // CHUNK, step, jnp.zeros((8, ZS), F32))
    square_ref[...] = fold_row(acc)


def last_call(recv, w, v, created, state, cells):
    return pl.pallas_call(
        functools.partial(last_kernel, cells),
        in_specs=[VMEM_SPEC] * (4 + len(created)),
        out_specs=(VMEM_SPEC,) * 4 + (SMEM_SPEC,),
        out_shape=(
            pltpu.VMEM((ROWS, ZS), F32),
            jax.ShapeDtypeStruct((STATE_ROWS, 128), F32),
            *LAST_SHAPES,
        ),
        scratch_shapes=[pltpu.VMEM(WEIGHT_SHAPE, F32)],
        compiler_params=PARAMS,
        name="last",
    )(recv, w, v, *created, state)


def finish_kernel(*refs):
    square_ref, state_ref, *created = refs[: 2 + STEPS]
    new_ref, hess_ref = refs[2 + STEPS :]
    lane = iota((1, 128), 1)
    norm = jnp.sqrt(jnp.sum(square_ref[...], axis=1, keepdims=True) + EPSILON)
    lanes = iota((BASIS, 128), 1)
    subs = iota((BASIS, 128), 0)
    hess = state_ref[pl.ds(STATE_H, BASIS), :]
    hess = jnp.where((subs == BASIS - 1) & (lanes == STEPS - 1), norm, hess)
    hess_ref[...] = jnp.transpose(jnp.concatenate([hess, jnp.zeros((128 - BASIS, 128), F32)], axis=0))[:STEPS, :BASIS]
    inverse_row = state_ref[pl.ds(STATE_D, 1), :]
    for j, u_ref in enumerate(created):
        if j == STEPS - 1:
            inverse = 1.0 / norm
        else:
            inverse = jnp.sum(jnp.where(lane == KEEP + j, inverse_row, 0.0), axis=1, keepdims=True)
        for c in range(ROWS // CHUNK):
            rows = pl.ds(c * CHUNK, CHUNK)
            new_ref[j, rows, :] = u_ref[rows, :] * inverse


def finish_call(square, state, created):
    return pl.pallas_call(
        finish_kernel,
        in_specs=[VMEM_SPEC] * (2 + STEPS),
        out_specs=(VMEM_SPEC, VMEM_SPEC),
        out_shape=(
            jax.ShapeDtypeStruct((STEPS, ROWS, ZS), F32),
            jax.ShapeDtypeStruct((STEPS, BASIS), F32),
        ),
        compiler_params=PARAMS,
        name="finish",
    )(square, state, *created)


def paired(half, start):
    lower = range(start, lax.axis_size("gx") - 1, 2)
    return lax.ppermute(half, "gx", [(i, i + 1) for i in lower] + [(i + 1, i) for i in lower])


def across(edge):
    return lax.ppermute(edge, "gy", [(0, 1), (1, 0)])


def from_all(payload):
    axes = ("gy", "gx")
    devices = lax.axis_size(axes)
    copies = payload.reshape(devices, 1, -1)
    got = lax.all_to_all(copies, axes, split_axis=0, concat_axis=0, tiled=True)
    return got.reshape(-1, 128)


def body(basis_vectors, reaction):
    devices = lax.axis_size(("gy", "gx"))
    cells = float(ROWS * ZS * devices)
    basis = basis_vectors.reshape(KEEP, ROWS, ZS)
    v, near, far, swap, early = start_call(basis)
    second = paired(far, 1)
    first = paired(near, 0)
    swap = across(swap)
    reaction = reaction.reshape(ROWS, ZS)
    extra = gram_call(v, early)
    w, payload = first_image_call(v, (first, second, swap), reaction, extra, devices)
    created = []
    state = None
    for _ in range(1, STEPS):
        recv = from_all(payload)
        far, weight, state = far_call(recv, w, v, created, state, cells)
        second = paired(far, 1)
        near, swap = near_call(weight, far, w, v, created)
        first = paired(near, 0)
        swap = across(swap)
        u, inner, extra = inner_call(v, near, far, created, swap, reaction)
        created.append(u)
        w, payload = outer_call(v, created, first, second, inner, extra, devices)
    u, state, square, guess, sound = last_call(from_all(payload), w, v, created, state, cells)
    created.append(u)
    square = lax.cond(
        sound[0] == 1,
        lambda guess, square: guess,
        lambda guess, square: jnp.sum(from_all(square), axis=0, keepdims=True) * (1.0 / cells),
        guess,
        jnp.broadcast_to(square, (devices, 128)),
    )
    new, hessenberg = finish_call(square, state, created)
    return new.reshape(STEPS, XS, YS, ZS), hessenberg.T


def solution(mesh):
    return jax.shard_map(
        body,
        mesh=mesh,
        in_specs=(P(None, "gx", "gy", None), P("gx", "gy", None)),
        out_specs=(P(None, "gx", "gy", None), P()),
        check_vma=False,
    )
```

```python
import functools

import jax
import jax.numpy as jnp
from jax import lax
from jax.experimental import pallas as pl
from jax.experimental.pallas import tpu as pltpu
from jax.sharding import PartitionSpec as P


KEEP = 36
STEPS = 4
BASIS = KEEP + STEPS
WIND_SPEEDS = (0.9, 0.6, 0.4)
EPSILON = 1e-06
F32 = jnp.float32

XS, YS, ZS = 4, 64, 256
ROWS = XS * YS
GROUP = 4
GRAM_ROWS = 64
HALF = KEEP // 2
PACK = 6
PACK_LANES = 40
FREE_LANE = 117
CHUNK = 32
BLOCK = 64
SOUND_SHARE = 0.05

PARAMS = pltpu.CompilerParams(vmem_limit_bytes=16 * 2**20)
SMEM_SPEC = pl.BlockSpec(memory_space=pltpu.SMEM)
VMEM_SPEC = pl.BlockSpec(memory_space=pltpu.VMEM)


def iota(shape, axis):
    return lax.broadcasted_iota(jnp.int32, shape, axis)


def to_column(row):
    pick = iota((BASIS, 128), 0) == iota((BASIS, 128), 1)
    return jnp.sum(jnp.where(pick, row, 0.0), axis=1, keepdims=True)


def to_row(column):
    pick = iota((BASIS, 128), 0) == iota((BASIS, 128), 1)
    return jnp.sum(jnp.where(pick, column, 0.0), axis=0, keepdims=True)


def fold_tiles(block):
    return jnp.sum(block.reshape(-1, 8, ZS), axis=0)


def fold_row(acc):
    return jnp.sum(acc[:, :128] + acc[:, 128:], axis=0, keepdims=True)


def gram_block(v_ref, sums_ref, ga, gb):
    pairs = [(a, b) for a in range(GROUP) for b in range(GROUP) if ga != gb or a <= b]

    def step(t, accs):
        accs = list(accs)
        for part in range(GRAM_ROWS // 8):
            rows = pl.ds(pl.multiple_of(t * GRAM_ROWS, GRAM_ROWS) + 8 * part, 8)
            for half in range(2):
                lanes = pl.ds(half * 128, 128)
                left = [v_ref[ga * GROUP + a, rows, lanes] for a in range(GROUP)]
                right = left
                if ga != gb:
                    right = [v_ref[gb * GROUP + b, rows, lanes] for b in range(GROUP)]
                for n, (a, b) in enumerate(pairs):
                    accs[n] = accs[n] + left[a] * right[b]
        return tuple(accs)

    zero = jnp.zeros((8, 128), F32)
    accs = lax.fori_loop(0, ROWS // GRAM_ROWS, step, tuple(zero for _ in pairs))
    for (a, b), acc in zip(pairs, accs):
        row = jnp.sum(acc, axis=0, keepdims=True)
        i, j = ga * GROUP + a, gb * GROUP + b
        sums_ref[i, pl.ds(j, 1), :] = row
        if i != j:
            sums_ref[j, pl.ds(i, 1), :] = row


def write_edges(u_ref, first_ref, second_ref, swap_ref):
    odd = lax.axis_index("gx") % 2 == 1
    upper = lax.axis_index("gy") == 1
    for x in range(2):
        low = u_ref[pl.ds(x * YS, YS), :]
        high = u_ref[pl.ds((XS - 2 + x) * YS, YS), :]
        first_ref[pl.ds(x * YS, YS), :] = jnp.where(odd, low, high)
        second_ref[pl.ds(x * YS, YS), :] = jnp.where(odd, high, low)
    for x in range(XS):
        low = u_ref[pl.ds(x * YS, 2), :]
        high = u_ref[pl.ds(x * YS + YS - 2, 2), :]
        swap_ref[pl.ds(2 * x, 2), :] = jnp.where(upper, low, high)


EDGE_SHAPES = (
    jax.ShapeDtypeStruct((2 * YS, ZS), F32),
    jax.ShapeDtypeStruct((2 * YS, ZS), F32),
    jax.ShapeDtypeStruct((2 * XS, ZS), F32),
)


ARRIVAL = [KEEP // GROUP - 1, *range(KEEP // GROUP - 1)]
EARLY = 4
LATE_PAIRS = [
    (ARRIVAL[m], ARRIVAL[n]) for n in range(EARLY, len(ARRIVAL)) for m in range(n + 1)
]


def start_kernel(v_hbm, v_ref, first_ref, second_ref, swap_ref, sums_ref, sems):
    copies = {}
    for g in ARRIVAL:
        part = pl.ds(g * GROUP, GROUP)
        copies[g] = pltpu.make_async_copy(v_hbm.at[part], v_ref.at[part], sems.at[g])
        copies[g].start()
    for n, g in enumerate(ARRIVAL[:EARLY]):
        copies[g].wait()
        if n == 0:
            write_edges(v_ref.at[KEEP - 1], first_ref, second_ref, swap_ref)
        for m in range(n + 1):
            gram_block(v_ref, sums_ref, ARRIVAL[m], g)
    for g in ARRIVAL[EARLY:]:
        copies[g].wait()


def start_call(basis):
    return pl.pallas_call(
        start_kernel,
        in_specs=[pl.BlockSpec(memory_space=pltpu.HBM)],
        out_specs=(VMEM_SPEC,) * 5,
        out_shape=(
            pltpu.VMEM((KEEP, ROWS, ZS), F32),
            *EDGE_SHAPES,
            pltpu.VMEM((KEEP, KEEP, 128), F32),
        ),
        scratch_shapes=[pltpu.SemaphoreType.DMA((KEEP // GROUP,))],
        compiler_params=PARAMS,
        name="start",
    )(pltpu.with_memory_space_constraint(basis, pltpu.HBM))


def gram_kernel(v_ref, early_ref, out_ref, sums_ref, matrix_ref):
    for ga, gb in LATE_PAIRS:
        gram_block(v_ref, sums_ref, ga, gb)
    early = sorted(g * GROUP + a for g in ARRIVAL[:EARLY] for a in range(GROUP))

    def line(i, start):
        part = sums_ref[i, pl.ds(start, HALF), :]
        if i in early:
            sub = iota((HALF, 128), 0) + start
            in_early = (sub < (EARLY - 1) * GROUP) | (sub >= KEEP - GROUP)
            part = jnp.where(in_early, early_ref[i, pl.ds(start, HALF), :], part)
        return part

    sub = iota((HALF, 128), 0)
    lane = iota((HALF, 128), 1)
    packed = jnp.zeros((HALF, 128), F32)
    diagonal = jnp.zeros((HALF, 128), F32)
    for i in range(KEEP):
        part = line(i, 0)
        if i < HALF:
            diagonal = jnp.where(sub == i, part, diagonal)
            part = jnp.where(sub < i, part, line(HALF + i, HALF))
        packed = jnp.where(lane == i, jnp.sum(part, axis=1, keepdims=True), packed)
    packed = jnp.where(lane == KEEP, jnp.sum(diagonal, axis=1, keepdims=True), packed)
    matrix_ref[pl.ds(0, HALF), :] = packed
    packed = matrix_ref[pl.ds(0, PACK), :]
    for p in range(1, HALF // PACK):
        packed = packed + pltpu.roll(matrix_ref[pl.ds(p * PACK, PACK), :], p * PACK_LANES, 1)
    for r in range(PACK):
        out_ref[:, pl.ds(r * 128, 128)] = packed[r : r + 1]


def gram_call(v, early):
    return pl.pallas_call(
        gram_kernel,
        in_specs=[VMEM_SPEC, VMEM_SPEC],
        out_specs=VMEM_SPEC,
        out_shape=jax.ShapeDtypeStruct((1, PACK * 128), F32),
        scratch_shapes=[pltpu.VMEM((KEEP, KEEP, 128), F32), pltpu.VMEM((BASIS, 128), F32)],
        compiler_params=PARAMS,
        name="gram",
    )(v, early)


ALL_PLANES = ((0, XS),)


def dot_all(v_ref, others, x_refs, dots_refs, planes=ALL_PLANES):
    batch = 12 // len(x_refs)
    for dots_ref in dots_refs:
        dots_ref[...] = jnp.zeros((BASIS, 128), F32)

    def run(reads, base):
        def step(c, accs):
            rows = pl.ds(pl.multiple_of(c * CHUNK, CHUNK), CHUNK)
            xs = [x_ref[rows, :] for x_ref in x_refs]
            new = []
            for n, read in enumerate(reads):
                value = read(rows)
                new += [accs[n * len(xs) + m] + fold_tiles(value * x) for m, x in enumerate(xs)]
            return tuple(new)

        zero = jnp.zeros((8, ZS), F32)
        accs = (zero,) * (len(reads) * len(x_refs))
        for first, end in planes:
            accs = lax.fori_loop(first * YS // CHUNK, end * YS // CHUNK, step, accs)
        for n, acc in enumerate(accs):
            row = base + n // len(x_refs)
            dots_refs[n % len(x_refs)][pl.ds(row, 1), :] = fold_row(acc)

    for first in range(0, KEEP, batch):
        run([lambda rows, i=i: v_ref[i, rows, :] for i in range(first, first + batch)], first)
    if others:
        run([lambda rows, r=r: r[rows, :] for r in others], KEEP)
    return [to_row(jnp.sum(dots_ref[...], axis=1, keepdims=True)) for dots_ref in dots_refs]


CENTER = -6.0 - 1.5 * sum(WIND_SPEEDS)
NEAR = [1.0 + 2.0 * s for s in WIND_SPEEDS]
FAR = [-0.5 * s for s in WIND_SPEEDS]


def inner_image(source, swap_ref, reaction_ref, pad_ref, x):
    upper = lax.axis_index("gy").astype(F32)
    lane = iota((YS, ZS), 1)
    mine = source[pl.ds(x * YS, YS), :]
    pad_ref[x, pl.ds(8, YS), :] = mine
    edge = swap_ref[pl.ds(2 * x, 2), :]
    pad_ref[x, pl.ds(6, 2), :] = edge * upper
    pad_ref[x, pl.ds(72, 1), :] = edge[0:1] * (1.0 - upper)
    image = (CENTER - reaction_ref[pl.ds(x * YS, YS), :]) * mine
    for distance, factor in ((1, 1.0), (-1, NEAR[0]), (-2, FAR[0])):
        if 0 <= x + distance < XS:
            image = image + factor * source[pl.ds((x + distance) * YS, YS), :]
    image = (
        image
        + pad_ref[x, pl.ds(9, YS), :]
        + NEAR[1] * pad_ref[x, pl.ds(7, YS), :]
        + FAR[1] * pad_ref[x, pl.ds(6, YS), :]
    )
    return (
        image
        + jnp.where(lane < ZS - 1, pltpu.roll(mine, ZS - 1, 1), 0.0)
        + NEAR[2] * jnp.where(lane >= 1, pltpu.roll(mine, 1, 1), 0.0)
        + FAR[2] * jnp.where(lane >= 2, pltpu.roll(mine, 2, 1), 0.0)
    )


def outer_image(first_ref, second_ref):
    odd = lax.axis_index("gx") % 2 == 1

    def below(rows):
        return jnp.where(odd, first_ref[rows, :], second_ref[rows, :])

    two, one = below(pl.ds(0, YS)), below(pl.ds(YS, YS))
    rows = pl.ds(0, YS)
    above = jnp.where(odd, second_ref[rows, :], first_ref[rows, :])
    return {0: NEAR[0] * one + FAR[0] * two, 1: FAR[0] * one, XS - 1: above}


LAST_SHAPES = (
    jax.ShapeDtypeStruct((1, 128), F32),
    jax.ShapeDtypeStruct((1, 128), F32),
    jax.ShapeDtypeStruct((1,), jnp.int32),
)


def write_for_all(out_ref, rows):
    count = len(rows)
    period = count
    while period % 8:
        period += count
    for tile in range(period // 8):
        sub = iota((8, 128), 0)
        block = jnp.zeros((8, 128), F32)
        for r in range(8):
            block = jnp.where(sub == r, rows[(8 * tile + r) % count], block)
        for p in range(out_ref.shape[0] // period):
            out_ref[pl.ds(p * period + 8 * tile, 8), :] = block


def first_image_kernel(
    v_ref, first_ref, second_ref, swap_ref, reaction_ref, extra_ref, w_ref, out_ref, dots_ref, pad_ref
):
    outer = outer_image(first_ref, second_ref)
    for x in range(XS):
        image = inner_image(v_ref.at[KEEP - 1], swap_ref, reaction_ref, pad_ref, x)
        w_ref[pl.ds(x * YS, YS), :] = image + outer[x] if x in outer else image
    (row,) = dot_all(v_ref, [], [w_ref], [dots_ref])
    lane = iota((1, 128), 1)
    free = (lane >= FREE_LANE) & (lane < FREE_LANE + PACK)
    rows = []
    for r in range(PACK):
        part = jnp.where(free, pltpu.roll(row, FREE_LANE - r * PACK, 1), 0.0)
        rows.append(extra_ref[:, pl.ds(128 * r, 128)] + part)
    write_for_all(out_ref, rows)


def first_image_call(v, halo, reaction, extra, devices):
    return pl.pallas_call(
        first_image_kernel,
        in_specs=[VMEM_SPEC] * 6,
        out_specs=(VMEM_SPEC, VMEM_SPEC),
        out_shape=(
            pltpu.VMEM((ROWS, ZS), F32),
            jax.ShapeDtypeStruct((devices * PACK, 128), F32),
        ),
        scratch_shapes=[
            pltpu.VMEM((BASIS, 128), F32),
            pltpu.VMEM((XS, YS + 16, ZS), F32),
        ],
        compiler_params=PARAMS,
        name="image_0",
    )(v, *halo, reaction, extra)


def inner_kernel(count, *refs):
    v_ref, near_ref, far_ref, *older = refs[: 2 + count]
    swap_ref, reaction_ref, u_ref, w_ref, out_ref, dots_ref, more_ref, pad_ref = refs[2 + count :]
    odd = lax.axis_index("gx") % 2 == 1
    for x in range(2):
        rows = pl.ds(x * YS, YS)
        near, far = near_ref[rows, :], far_ref[rows, :]
        u_ref[pl.ds(x * YS, YS), :] = jnp.where(odd, near, far)
        u_ref[pl.ds((2 + x) * YS, YS), :] = jnp.where(odd, far, near)
    for x in range(XS):
        w_ref[pl.ds(x * YS, YS), :] = inner_image(u_ref, swap_ref, reaction_ref, pad_ref, x)
    rows = dot_all(v_ref, [*older, u_ref], [w_ref, u_ref], [dots_ref, more_ref])
    for n, row in enumerate(rows):
        out_ref[pl.ds(n, 1), :] = row


def inner_call(v, near, far, older, swap, reaction):
    count = 1 + len(older)
    return pl.pallas_call(
        functools.partial(inner_kernel, count),
        in_specs=[VMEM_SPEC] * (4 + count),
        out_specs=(VMEM_SPEC,) * 3,
        out_shape=(
            pltpu.VMEM((ROWS, ZS), F32),
            pltpu.VMEM((ROWS, ZS), F32),
            jax.ShapeDtypeStruct((2, 128), F32),
        ),
        scratch_shapes=[
            pltpu.VMEM((BASIS, 128), F32),
            pltpu.VMEM((BASIS, 128), F32),
            pltpu.VMEM((XS, YS + 16, ZS), F32),
        ],
        compiler_params=PARAMS,
    )(v, near, far, *older, swap, reaction)


def outer_kernel(count, *refs):
    v_ref, *others = refs[: 1 + count]
    first_ref, second_ref, inner_ref, extra_ref = refs[1 + count : 5 + count]
    w_ref, out_ref, dots_ref, delta_ref = refs[5 + count :]
    outer = outer_image(first_ref, second_ref)
    for x in range(XS):
        rows = pl.ds(x * YS, YS)
        image = inner_ref[rows, :]
        if x in outer:
            delta_ref[rows, :] = outer[x]
            image = image + outer[x]
        w_ref[rows, :] = image
    (row,) = dot_all(v_ref, others, [delta_ref], [dots_ref], ((0, 2), (3, 4)))
    row = row + extra_ref[pl.ds(0, 1), :]
    if count == STEPS - 1:
        square = jnp.zeros((8, ZS), F32)
        for c in range(ROWS // CHUNK):
            image = w_ref[pl.ds(c * CHUNK, CHUNK), :]
            square = square + fold_tiles(image * image)
        square = jnp.sum(fold_row(square), axis=1, keepdims=True)
        row = jnp.where(iota((1, 128), 1) == BASIS - 1, square, row)
    write_for_all(out_ref, [row, extra_ref[pl.ds(1, 1), :]])


def outer_call(v, created, first, second, inner, extra, devices):
    count = len(created)
    return pl.pallas_call(
        functools.partial(outer_kernel, count),
        in_specs=[VMEM_SPEC] * (5 + count),
        out_specs=(VMEM_SPEC, VMEM_SPEC),
        out_shape=(
            pltpu.VMEM((ROWS, ZS), F32),
            jax.ShapeDtypeStruct((2 * devices, 128), F32),
        ),
        scratch_shapes=[pltpu.VMEM((BASIS, 128), F32), pltpu.VMEM((ROWS, ZS), F32)],
        compiler_params=PARAMS,
    )(v, *created, first, second, inner, extra)


STATE_G, STATE_H, STATE_D, STATE_ROWS = 0, BASIS, 2 * BASIS, 2 * BASIS + 8


def summed_rows(recv_ref, count):
    period = count
    while period % 8:
        period += count
    total = jnp.sum(recv_ref[...].reshape(-1, period, 128), axis=0)
    if count in (1, 2):
        while count < 8:
            total = total + pltpu.roll(total, 8 - count, 0)
            count *= 2
        return total
    return sum(total[p : p + count] for p in range(0, period, count))


def unpacked_gram(packed, pack_ref):
    pack_ref[...] = jnp.zeros((128, 128), F32)
    for p in range(HALF // PACK):
        part = packed
        if p:
            part = pltpu.roll(part, 128 - p * PACK_LANES, 1)
        pack_ref[pl.ds(p * PACK, PACK), :] = part
    turned = jnp.transpose(pack_ref[...])
    plain = pack_ref[pl.ds(0, HALF), :]
    lane = iota((HALF, 128), 1)
    sub = iota((HALF, 128), 0)
    diagonal = jnp.sum(jnp.where(lane == KEEP, plain, 0.0), axis=1, keepdims=True)
    top = jnp.where((lane > sub) | (lane >= HALF), plain, turned[:HALF])
    top = jnp.where(lane == sub, diagonal, top)
    last = jnp.where(lane <= sub, plain, turned[:HALF])
    pack_ref[...] = turned
    bottom = jnp.where(lane < HALF, pack_ref[pl.ds(HALF, HALF), :], pltpu.roll(last, HALF, 1))
    pack_ref[pl.ds(0, HALF), :] = jnp.where(lane < KEEP, top, 0.0)
    pack_ref[pl.ds(HALF, HALF), :] = jnp.where(lane < KEEP, bottom, 0.0)
    pack_ref[pl.ds(KEEP, STEPS), :] = jnp.zeros((STEPS, 128), F32)


def solve_weights(count, cells, recv_ref, state_in, state_ref, weight_ref, pack_ref):
    lane = iota((1, 128), 1)
    lanes = iota((BASIS, 128), 1)
    subs = iota((BASIS, 128), 0)
    sub = iota((BASIS, 1), 0)
    scale = 1.0 / cells

    def spread(values):
        return jnp.sum(values, axis=1, keepdims=True)

    if count == 0:
        total = summed_rows(recv_ref, PACK) * scale
        unpacked_gram(total[:PACK], pack_ref)
        gram = pack_ref[pl.ds(0, BASIS), :]
        hess = jnp.zeros((BASIS, 128), F32)
        inverse_row = jnp.where(lane < KEEP, 1.0, 0.0)
        inverse_column = jnp.where(sub < KEEP, 1.0, 0.0)
        first_row = jnp.zeros((1, 128), F32)
        for r in range(PACK):
            part = pltpu.roll(total[r : r + 1], 128 - FREE_LANE + r * PACK, 1)
            mine = (lane >= r * PACK) & (lane < (r + 1) * PACK)
            first_row = jnp.where(mine, part, first_row)
        inverse = jnp.ones((1, 1), F32)
        image_square = None
        first = to_column(first_row)
        folded = spread(gram * first_row)
    else:
        total = summed_rows(recv_ref, 2) * scale
        newest = KEEP + count - 1
        raw_first, raw_gram = total[0:1], total[1:2]
        inverse_row = state_in[pl.ds(STATE_D, 1), :]
        gram = state_in[pl.ds(STATE_G, BASIS), :]
        hess = state_in[pl.ds(STATE_H, BASIS), :]
        part_first, part_gram = raw_first * inverse_row, raw_gram * inverse_row
        square = spread(jnp.where(lane == newest, raw_gram, 0.0))
        first_newest = spread(jnp.where(lane == newest, raw_first, 0.0))
        image_square = spread(jnp.where(lane == BASIS - 1, raw_first, 0.0))
        crossed = spread(part_gram * part_first)
        first_column, gram_column = to_column(part_first), to_column(part_gram)
        inverse_column = to_column(inverse_row)
        folded = spread(gram * part_first)
        norm = jnp.sqrt(square + EPSILON)
        inverse = 1.0 / norm
        own = square * inverse * inverse
        first_newest = first_newest * inverse * inverse
        image_square = image_square * inverse * inverse
        mine = sub == newest
        first = jnp.where(mine, first_newest, first_column * inverse)
        gram_column = gram_column * inverse
        folded = jnp.where(
            mine,
            crossed * inverse * inverse + own * first_newest,
            folded * inverse + gram_column * first_newest,
        )
        gram = jnp.where(lanes == newest, gram_column, gram)
        gram = jnp.where(subs == newest, part_gram * inverse, gram)
        gram = jnp.where((lanes == newest) & (subs == newest), own, gram)
        hess = jnp.where((subs == newest) & (lanes == count - 1), norm, hess)
        inverse_row = jnp.where(lane == newest, inverse, inverse_row)
        inverse_column = jnp.where(mine, inverse, inverse_column)
    weights = first + (first - folded)
    weight_ref[pl.ds(0, BASIS), :] = jnp.broadcast_to(weights * inverse_column, (BASIS, ZS))
    weight_ref[pl.ds(BASIS, 8), :] = jnp.broadcast_to(inverse, (8, ZS))
    hess = jnp.where((lanes == count) & (subs < KEEP + count), weights, hess)
    state_ref[pl.ds(STATE_G, BASIS), :] = gram
    state_ref[pl.ds(STATE_H, BASIS), :] = hess
    state_ref[pl.ds(STATE_D, 8), :] = jnp.broadcast_to(inverse_row, (8, 128))
    return weights, first, gram, image_square


def combined(rows, weight_ref, w_ref, v_ref, others):
    value = w_ref[rows, :] * weight_ref[pl.ds(BASIS, 1), :]
    for i in range(KEEP):
        value = value - weight_ref[pl.ds(i, 1), :] * v_ref[i, rows, :]
    for i, other in enumerate(others):
        value = value - weight_ref[pl.ds(KEEP + i, 1), :] * other[rows, :]
    return value


def combine_half(out_ref, high, weight_ref, w_ref, v_ref, others):
    start = high.astype(jnp.int32) * (ROWS // 2)

    def step(c, carry):
        rows = pl.ds(pl.multiple_of(start + c * BLOCK, BLOCK), BLOCK)
        out_ref[pl.ds(pl.multiple_of(c * BLOCK, BLOCK), BLOCK), :] = combined(
            rows, weight_ref, w_ref, v_ref, others
        )
        return carry

    lax.fori_loop(0, ROWS // 2 // BLOCK, step, 0)


HALF_SHAPE = jax.ShapeDtypeStruct((ROWS // 2, ZS), F32)
WEIGHT_SHAPE = (BASIS + 8, ZS)


def far_kernel(count, cells, *refs):
    recv_ref, w_ref, v_ref, *others = refs[: 3 + count]
    *states, far_ref, weight_ref, state_ref, pack_ref = refs[3 + count :]
    state_in = states[0] if states else None
    solve_weights(count, cells, recv_ref, state_in, state_ref, weight_ref, pack_ref)
    odd = lax.axis_index("gx") % 2 == 1
    combine_half(far_ref, odd, weight_ref, w_ref, v_ref, others)


def far_call(recv, w, v, created, state, cells):
    count = len(created)
    states = [state] if created else []
    return pl.pallas_call(
        functools.partial(far_kernel, count, cells),
        in_specs=[VMEM_SPEC] * (3 + count + len(states)),
        out_specs=(VMEM_SPEC,) * 3,
        out_shape=(
            HALF_SHAPE,
            pltpu.VMEM(WEIGHT_SHAPE, F32),
            jax.ShapeDtypeStruct((STATE_ROWS, 128), F32),
        ),
        scratch_shapes=[pltpu.VMEM((128, 128), F32)],
        compiler_params=PARAMS,
    )(recv, w, v, *created, *states)


def near_kernel(count, *refs):
    weight_ref, far_ref, w_ref, v_ref, *others = refs[: 4 + count]
    near_ref, swap_ref = refs[4 + count :]
    odd = lax.axis_index("gx") % 2 == 1
    upper = lax.axis_index("gy") == 1
    combine_half(near_ref, jnp.logical_not(odd), weight_ref, w_ref, v_ref, others)
    for x in range(XS):
        sides = []
        for y in (0, YS - 2):
            rows = pl.ds((x % 2) * YS + y, 2)
            low, high = (near_ref, far_ref) if x < 2 else (far_ref, near_ref)
            sides.append(jnp.where(odd, low[rows, :], high[rows, :]))
        swap_ref[pl.ds(2 * x, 2), :] = jnp.where(upper, *sides)


def near_call(weight, far, w, v, created):
    count = len(created)
    return pl.pallas_call(
        functools.partial(near_kernel, count),
        in_specs=[VMEM_SPEC] * (4 + count),
        out_specs=(VMEM_SPEC,) * 2,
        out_shape=(HALF_SHAPE, jax.ShapeDtypeStruct((2 * XS, ZS), F32)),
        compiler_params=PARAMS,
    )(weight, far, w, v, *created)


def last_kernel(cells, *refs):
    count = STEPS - 1
    recv_ref, w_ref, v_ref, *others = refs[: 3 + count]
    state_in, u_ref, state_ref, square_ref, guess_ref, sound_ref, weight_ref = refs[3 + count :]
    weights, first, gram, image_square = solve_weights(
        count, cells, recv_ref, state_in, state_ref, weight_ref, None
    )
    again = jnp.sum(gram * to_row(weights), axis=1, keepdims=True)
    guess = image_square - jnp.sum(weights * (2.0 * first - again), axis=0, keepdims=True)
    guess_ref[...] = jnp.where(iota((1, 128), 1) == 0, guess, 0.0)
    sound = jnp.where(guess > SOUND_SHARE * image_square, 1, 0)
    sound_ref[0] = sound[0, 0]

    def step(c, acc):
        rows = pl.ds(pl.multiple_of(c * BLOCK, BLOCK), BLOCK)
        value = combined(rows, weight_ref, w_ref, v_ref, others)
        u_ref[rows, :] = value
        return acc + fold_tiles(value * value)

    acc = lax.fori_loop(0, ROWS // BLOCK, step, jnp.zeros((8, ZS), F32))
    square_ref[...] = fold_row(acc)


def last_call(recv, w, v, created, state, cells):
    return pl.pallas_call(
        functools.partial(last_kernel, cells),
        in_specs=[VMEM_SPEC] * (4 + len(created)),
        out_specs=(VMEM_SPEC,) * 4 + (SMEM_SPEC,),
        out_shape=(
            pltpu.VMEM((ROWS, ZS), F32),
            jax.ShapeDtypeStruct((STATE_ROWS, 128), F32),
            *LAST_SHAPES,
        ),
        scratch_shapes=[pltpu.VMEM(WEIGHT_SHAPE, F32)],
        compiler_params=PARAMS,
        name="last",
    )(recv, w, v, *created, state)


def finish_kernel(*refs):
    square_ref, state_ref, *created = refs[: 2 + STEPS]
    new_ref, hess_ref = refs[2 + STEPS :]
    lane = iota((1, 128), 1)
    norm = jnp.sqrt(jnp.sum(square_ref[...], axis=1, keepdims=True) + EPSILON)
    lanes = iota((BASIS, 128), 1)
    subs = iota((BASIS, 128), 0)
    hess = state_ref[pl.ds(STATE_H, BASIS), :]
    hess = jnp.where((subs == BASIS - 1) & (lanes == STEPS - 1), norm, hess)
    hess_ref[...] = jnp.transpose(jnp.concatenate([hess, jnp.zeros((128 - BASIS, 128), F32)], axis=0))[:STEPS, :BASIS]
    inverse_row = state_ref[pl.ds(STATE_D, 1), :]
    for j, u_ref in enumerate(created):
        if j == STEPS - 1:
            inverse = 1.0 / norm
        else:
            inverse = jnp.sum(jnp.where(lane == KEEP + j, inverse_row, 0.0), axis=1, keepdims=True)
        for c in range(ROWS // CHUNK):
            rows = pl.ds(c * CHUNK, CHUNK)
            new_ref[j, rows, :] = u_ref[rows, :] * inverse


def finish_call(square, state, created):
    return pl.pallas_call(
        finish_kernel,
        in_specs=[VMEM_SPEC] * (2 + STEPS),
        out_specs=(VMEM_SPEC, VMEM_SPEC),
        out_shape=(
            jax.ShapeDtypeStruct((STEPS, ROWS, ZS), F32),
            jax.ShapeDtypeStruct((STEPS, BASIS), F32),
        ),
        compiler_params=PARAMS,
        name="finish",
    )(square, state, *created)


def paired(half, start):
    lower = range(start, lax.axis_size("gx") - 1, 2)
    return lax.ppermute(half, "gx", [(i, i + 1) for i in lower] + [(i + 1, i) for i in lower])


def across(edge):
    return lax.ppermute(edge, "gy", [(0, 1), (1, 0)])


def from_all(payload):
    axes = ("gy", "gx")
    devices = lax.axis_size(axes)
    copies = payload.reshape(devices, 1, -1)
    got = lax.all_to_all(copies, axes, split_axis=0, concat_axis=0, tiled=True)
    return got.reshape(-1, 128)


def body(basis_vectors, reaction):
    devices = lax.axis_size(("gy", "gx"))
    cells = float(ROWS * ZS * devices)
    basis = basis_vectors.reshape(KEEP, ROWS, ZS)
    v, near, far, swap, early = start_call(basis)
    second = paired(far, 1)
    first = paired(near, 0)
    swap = across(swap)
    reaction = reaction.reshape(ROWS, ZS)
    extra = gram_call(v, early)
    w, payload = first_image_call(v, (first, second, swap), reaction, extra, devices)
    created = []
    state = None
    for _ in range(1, STEPS):
        recv = from_all(payload)
        far, weight, state = far_call(recv, w, v, created, state, cells)
        second = paired(far, 1)
        near, swap = near_call(weight, far, w, v, created)
        first = paired(near, 0)
        swap = across(swap)
        u, inner, extra = inner_call(v, near, far, created, swap, reaction)
        created.append(u)
        w, payload = outer_call(v, created, first, second, inner, extra, devices)
    u, state, square, guess, sound = last_call(from_all(payload), w, v, created, state, cells)
    created.append(u)
    square = lax.cond(
        sound[0] == 1,
        lambda guess, square: guess,
        lambda guess, square: jnp.sum(from_all(square), axis=0, keepdims=True) * (1.0 / cells),
        guess,
        jnp.broadcast_to(square, (devices, 128)),
    )
    new, hessenberg = finish_call(square, state, created)
    return new.reshape(STEPS, XS, YS, ZS), hessenberg.T


def solution(mesh):
    return jax.shard_map(
        body,
        mesh=mesh,
        in_specs=(P(None, "gx", "gy", None), P("gx", "gy", None)),
        out_specs=(P(None, "gx", "gy", None), P()),
        check_vma=False,
    )
```

```python
import functools

import jax
import jax.numpy as jnp
from jax import lax
from jax.experimental import pallas as pl
from jax.experimental.pallas import tpu as pltpu
from jax.sharding import PartitionSpec as P


KEEP = 36
STEPS = 4
BASIS = KEEP + STEPS
WIND_SPEEDS = (0.9, 0.6, 0.4)
EPSILON = 1e-06
F32 = jnp.float32

XS, YS, ZS = 4, 64, 256
ROWS = XS * YS
GROUP = 4
GRAM_ROWS = 64
HALF = KEEP // 2
PACK = 6
PACK_LANES = 40
FREE_LANE = 117
OWN_LANE = 64
CHUNK = 32
BLOCK = 64
SOUND_SHARE = 0.05

PARAMS = pltpu.CompilerParams(vmem_limit_bytes=16 * 2**20)
SMEM_SPEC = pl.BlockSpec(memory_space=pltpu.SMEM)
VMEM_SPEC = pl.BlockSpec(memory_space=pltpu.VMEM)


def iota(shape, axis):
    return lax.broadcasted_iota(jnp.int32, shape, axis)


def to_column(row):
    pick = iota((BASIS, 128), 0) == iota((BASIS, 128), 1)
    return jnp.sum(jnp.where(pick, row, 0.0), axis=1, keepdims=True)


def to_row(column):
    pick = iota((BASIS, 128), 0) == iota((BASIS, 128), 1)
    return jnp.sum(jnp.where(pick, column, 0.0), axis=0, keepdims=True)


def fold_tiles(block):
    return jnp.sum(block.reshape(-1, 8, ZS), axis=0)


def fold_row(acc):
    return jnp.sum(acc[:, :128] + acc[:, 128:], axis=0, keepdims=True)


def gram_block(v_ref, sums_ref, ga, gb):
    pairs = [(a, b) for a in range(GROUP) for b in range(GROUP) if ga != gb or a <= b]

    def step(t, accs):
        accs = list(accs)
        for part in range(GRAM_ROWS // 8):
            rows = pl.ds(pl.multiple_of(t * GRAM_ROWS, GRAM_ROWS) + 8 * part, 8)
            for half in range(2):
                lanes = pl.ds(half * 128, 128)
                left = [v_ref[ga * GROUP + a, rows, lanes] for a in range(GROUP)]
                right = left
                if ga != gb:
                    right = [v_ref[gb * GROUP + b, rows, lanes] for b in range(GROUP)]
                for n, (a, b) in enumerate(pairs):
                    accs[n] = accs[n] + left[a] * right[b]
        return tuple(accs)

    zero = jnp.zeros((8, 128), F32)
    accs = lax.fori_loop(0, ROWS // GRAM_ROWS, step, tuple(zero for _ in pairs))
    for (a, b), acc in zip(pairs, accs):
        row = jnp.sum(acc, axis=0, keepdims=True)
        i, j = ga * GROUP + a, gb * GROUP + b
        sums_ref[i, pl.ds(j, 1), :] = row
        if i != j:
            sums_ref[j, pl.ds(i, 1), :] = row


def write_edges(u_ref, first_ref, second_ref, swap_ref):
    odd = lax.axis_index("gx") % 2 == 1
    upper = lax.axis_index("gy") == 1
    for x in range(2):
        low = u_ref[pl.ds(x * YS, YS), :]
        high = u_ref[pl.ds((XS - 2 + x) * YS, YS), :]
        first_ref[pl.ds(x * YS, YS), :] = jnp.where(odd, low, high)
        second_ref[pl.ds(x * YS, YS), :] = jnp.where(odd, high, low)
    for x in range(XS):
        low = u_ref[pl.ds(x * YS, 2), :]
        high = u_ref[pl.ds(x * YS + YS - 2, 2), :]
        swap_ref[pl.ds(2 * x, 2), :] = jnp.where(upper, low, high)


EDGE_SHAPES = (
    jax.ShapeDtypeStruct((2 * YS, ZS), F32),
    jax.ShapeDtypeStruct((2 * YS, ZS), F32),
    jax.ShapeDtypeStruct((2 * XS, ZS), F32),
)


ARRIVAL = [KEEP // GROUP - 1, *range(KEEP // GROUP - 1)]
EARLY = 4
LATE_PAIRS = [
    (ARRIVAL[m], ARRIVAL[n]) for n in range(EARLY, len(ARRIVAL)) for m in range(n + 1)
]


def start_kernel(v_hbm, v_ref, first_ref, second_ref, swap_ref, sums_ref, sems):
    copies = {}
    for g in ARRIVAL:
        part = pl.ds(g * GROUP, GROUP)
        copies[g] = pltpu.make_async_copy(v_hbm.at[part], v_ref.at[part], sems.at[g])
        copies[g].start()
    for n, g in enumerate(ARRIVAL[:EARLY]):
        copies[g].wait()
        if n == 0:
            write_edges(v_ref.at[KEEP - 1], first_ref, second_ref, swap_ref)
        for m in range(n + 1):
            gram_block(v_ref, sums_ref, ARRIVAL[m], g)
    for g in ARRIVAL[EARLY:]:
        copies[g].wait()


def start_call(basis):
    return pl.pallas_call(
        start_kernel,
        in_specs=[pl.BlockSpec(memory_space=pltpu.HBM)],
        out_specs=(VMEM_SPEC,) * 5,
        out_shape=(
            pltpu.VMEM((KEEP, ROWS, ZS), F32),
            *EDGE_SHAPES,
            pltpu.VMEM((KEEP, KEEP, 128), F32),
        ),
        scratch_shapes=[pltpu.SemaphoreType.DMA((KEEP // GROUP,))],
        compiler_params=PARAMS,
        name="start",
    )(pltpu.with_memory_space_constraint(basis, pltpu.HBM))


def gram_kernel(v_ref, early_ref, out_ref, sums_ref, matrix_ref):
    for ga, gb in LATE_PAIRS:
        gram_block(v_ref, sums_ref, ga, gb)
    early = sorted(g * GROUP + a for g in ARRIVAL[:EARLY] for a in range(GROUP))

    def line(i, start):
        part = sums_ref[i, pl.ds(start, HALF), :]
        if i in early:
            sub = iota((HALF, 128), 0) + start
            in_early = (sub < (EARLY - 1) * GROUP) | (sub >= KEEP - GROUP)
            part = jnp.where(in_early, early_ref[i, pl.ds(start, HALF), :], part)
        return part

    sub = iota((HALF, 128), 0)
    lane = iota((HALF, 128), 1)
    packed = jnp.zeros((HALF, 128), F32)
    diagonal = jnp.zeros((HALF, 128), F32)
    for i in range(KEEP):
        part = line(i, 0)
        if i < HALF:
            diagonal = jnp.where(sub == i, part, diagonal)
            part = jnp.where(sub < i, part, line(HALF + i, HALF))
        packed = jnp.where(lane == i, jnp.sum(part, axis=1, keepdims=True), packed)
    packed = jnp.where(lane == KEEP, jnp.sum(diagonal, axis=1, keepdims=True), packed)
    matrix_ref[pl.ds(0, HALF), :] = packed
    packed = matrix_ref[pl.ds(0, PACK), :]
    for p in range(1, HALF // PACK):
        packed = packed + pltpu.roll(matrix_ref[pl.ds(p * PACK, PACK), :], p * PACK_LANES, 1)
    for r in range(PACK):
        out_ref[:, pl.ds(r * 128, 128)] = packed[r : r + 1]


def gram_call(v, early):
    return pl.pallas_call(
        gram_kernel,
        in_specs=[VMEM_SPEC, VMEM_SPEC],
        out_specs=VMEM_SPEC,
        out_shape=jax.ShapeDtypeStruct((1, PACK * 128), F32),
        scratch_shapes=[pltpu.VMEM((KEEP, KEEP, 128), F32), pltpu.VMEM((BASIS, 128), F32)],
        compiler_params=PARAMS,
        name="gram",
    )(v, early)


ALL_PLANES = ((0, XS),)


def dot_all(v_ref, others, x_refs, dots_refs, planes=ALL_PLANES):
    batch = 12 // len(x_refs)
    for dots_ref in dots_refs:
        dots_ref[...] = jnp.zeros((BASIS, 128), F32)

    def run(reads, base):
        def step(c, accs):
            rows = pl.ds(pl.multiple_of(c * CHUNK, CHUNK), CHUNK)
            xs = [x_ref[rows, :] for x_ref in x_refs]
            new = []
            for n, read in enumerate(reads):
                value = read(rows)
                new += [accs[n * len(xs) + m] + fold_tiles(value * x) for m, x in enumerate(xs)]
            return tuple(new)

        zero = jnp.zeros((8, ZS), F32)
        accs = (zero,) * (len(reads) * len(x_refs))
        for first, end in planes:
            accs = lax.fori_loop(first * YS // CHUNK, end * YS // CHUNK, step, accs)
        for n, acc in enumerate(accs):
            row = base + n // len(x_refs)
            dots_refs[n % len(x_refs)][pl.ds(row, 1), :] = fold_row(acc)

    for first in range(0, KEEP, batch):
        run([lambda rows, i=i: v_ref[i, rows, :] for i in range(first, first + batch)], first)
    if others:
        run([lambda rows, r=r: r[rows, :] for r in others], KEEP)
    return [to_row(jnp.sum(dots_ref[...], axis=1, keepdims=True)) for dots_ref in dots_refs]


CENTER = -6.0 - 1.5 * sum(WIND_SPEEDS)
NEAR = [1.0 + 2.0 * s for s in WIND_SPEEDS]
FAR = [-0.5 * s for s in WIND_SPEEDS]


def inner_image(source, swap_ref, reaction_ref, pad_ref, x):
    upper = lax.axis_index("gy").astype(F32)
    lane = iota((YS, ZS), 1)
    mine = source[pl.ds(x * YS, YS), :]
    pad_ref[x, pl.ds(8, YS), :] = mine
    edge = swap_ref[pl.ds(2 * x, 2), :]
    pad_ref[x, pl.ds(6, 2), :] = edge * upper
    pad_ref[x, pl.ds(72, 1), :] = edge[0:1] * (1.0 - upper)
    image = (CENTER - reaction_ref[pl.ds(x * YS, YS), :]) * mine
    for distance, factor in ((1, 1.0), (-1, NEAR[0]), (-2, FAR[0])):
        if 0 <= x + distance < XS:
            image = image + factor * source[pl.ds((x + distance) * YS, YS), :]
    image = (
        image
        + pad_ref[x, pl.ds(9, YS), :]
        + NEAR[1] * pad_ref[x, pl.ds(7, YS), :]
        + FAR[1] * pad_ref[x, pl.ds(6, YS), :]
    )
    return (
        image
        + jnp.where(lane < ZS - 1, pltpu.roll(mine, ZS - 1, 1), 0.0)
        + NEAR[2] * jnp.where(lane >= 1, pltpu.roll(mine, 1, 1), 0.0)
        + FAR[2] * jnp.where(lane >= 2, pltpu.roll(mine, 2, 1), 0.0)
    )


def outer_image(first_ref, second_ref):
    odd = lax.axis_index("gx") % 2 == 1

    def below(rows):
        return jnp.where(odd, first_ref[rows, :], second_ref[rows, :])

    two, one = below(pl.ds(0, YS)), below(pl.ds(YS, YS))
    rows = pl.ds(0, YS)
    above = jnp.where(odd, second_ref[rows, :], first_ref[rows, :])
    return {0: NEAR[0] * one + FAR[0] * two, 1: FAR[0] * one, XS - 1: above}


LAST_SHAPES = (
    jax.ShapeDtypeStruct((1, 128), F32),
    jax.ShapeDtypeStruct((1, 128), F32),
    jax.ShapeDtypeStruct((1,), jnp.int32),
)


def write_for_all(out_ref, rows):
    count = len(rows)
    period = count
    while period % 8:
        period += count
    for tile in range(period // 8):
        sub = iota((8, 128), 0)
        block = jnp.zeros((8, 128), F32)
        for r in range(8):
            block = jnp.where(sub == r, rows[(8 * tile + r) % count], block)
        for p in range(out_ref.shape[0] // period):
            out_ref[pl.ds(p * period + 8 * tile, 8), :] = block


def first_image_kernel(
    v_ref, first_ref, second_ref, swap_ref, reaction_ref, extra_ref, w_ref, out_ref, dots_ref, pad_ref
):
    outer = outer_image(first_ref, second_ref)
    for x in range(XS):
        image = inner_image(v_ref.at[KEEP - 1], swap_ref, reaction_ref, pad_ref, x)
        w_ref[pl.ds(x * YS, YS), :] = image + outer[x] if x in outer else image
    (row,) = dot_all(v_ref, [], [w_ref], [dots_ref])
    lane = iota((1, 128), 1)
    free = (lane >= FREE_LANE) & (lane < FREE_LANE + PACK)
    rows = []
    for r in range(PACK):
        part = jnp.where(free, pltpu.roll(row, FREE_LANE - r * PACK, 1), 0.0)
        rows.append(extra_ref[:, pl.ds(128 * r, 128)] + part)
    write_for_all(out_ref, rows)


def first_image_call(v, halo, reaction, extra, devices):
    return pl.pallas_call(
        first_image_kernel,
        in_specs=[VMEM_SPEC] * 6,
        out_specs=(VMEM_SPEC, VMEM_SPEC),
        out_shape=(
            pltpu.VMEM((ROWS, ZS), F32),
            jax.ShapeDtypeStruct((devices * PACK, 128), F32),
        ),
        scratch_shapes=[
            pltpu.VMEM((BASIS, 128), F32),
            pltpu.VMEM((XS, YS + 16, ZS), F32),
        ],
        compiler_params=PARAMS,
        name="image_0",
    )(v, *halo, reaction, extra)


def inner_kernel(count, *refs):
    v_ref, near_ref, far_ref, *older = refs[: 2 + count]
    swap_ref, reaction_ref, u_ref, w_ref, out_ref, dots_ref, more_ref, pad_ref = refs[2 + count :]
    odd = lax.axis_index("gx") % 2 == 1
    for x in range(2):
        rows = pl.ds(x * YS, YS)
        near, far = near_ref[rows, :], far_ref[rows, :]
        u_ref[pl.ds(x * YS, YS), :] = jnp.where(odd, near, far)
        u_ref[pl.ds((2 + x) * YS, YS), :] = jnp.where(odd, far, near)
    for x in range(XS):
        w_ref[pl.ds(x * YS, YS), :] = inner_image(u_ref, swap_ref, reaction_ref, pad_ref, x)
    row, own = dot_all(v_ref, [*older, u_ref], [w_ref, u_ref], [dots_ref, more_ref])
    out_ref[...] = row + pltpu.roll(own, OWN_LANE, 1)


def inner_call(v, near, far, older, swap, reaction):
    count = 1 + len(older)
    return pl.pallas_call(
        functools.partial(inner_kernel, count),
        in_specs=[VMEM_SPEC] * (4 + count),
        out_specs=(VMEM_SPEC,) * 3,
        out_shape=(
            pltpu.VMEM((ROWS, ZS), F32),
            pltpu.VMEM((ROWS, ZS), F32),
            jax.ShapeDtypeStruct((1, 128), F32),
        ),
        scratch_shapes=[
            pltpu.VMEM((BASIS, 128), F32),
            pltpu.VMEM((BASIS, 128), F32),
            pltpu.VMEM((XS, YS + 16, ZS), F32),
        ],
        compiler_params=PARAMS,
    )(v, near, far, *older, swap, reaction)


def outer_kernel(count, *refs):
    v_ref, *others = refs[: 1 + count]
    first_ref, second_ref, inner_ref, extra_ref = refs[1 + count : 5 + count]
    w_ref, out_ref, dots_ref, delta_ref = refs[5 + count :]
    outer = outer_image(first_ref, second_ref)
    for x in range(XS):
        rows = pl.ds(x * YS, YS)
        image = inner_ref[rows, :]
        if x in outer:
            delta_ref[rows, :] = outer[x]
            image = image + outer[x]
        w_ref[rows, :] = image
    (row,) = dot_all(v_ref, others, [delta_ref], [dots_ref], ((0, 2), (3, 4)))
    row = row + extra_ref[...]
    if count == STEPS - 1:
        square = jnp.zeros((8, ZS), F32)
        for c in range(ROWS // CHUNK):
            image = w_ref[pl.ds(c * CHUNK, CHUNK), :]
            square = square + fold_tiles(image * image)
        square = jnp.sum(fold_row(square), axis=1, keepdims=True)
        row = jnp.where(iota((1, 128), 1) == BASIS - 1, square, row)
    write_for_all(out_ref, [row])


def outer_call(v, created, first, second, inner, extra, devices):
    count = len(created)
    return pl.pallas_call(
        functools.partial(outer_kernel, count),
        in_specs=[VMEM_SPEC] * (5 + count),
        out_specs=(VMEM_SPEC, VMEM_SPEC),
        out_shape=(
            pltpu.VMEM((ROWS, ZS), F32),
            jax.ShapeDtypeStruct((devices, 128), F32),
        ),
        scratch_shapes=[pltpu.VMEM((BASIS, 128), F32), pltpu.VMEM((ROWS, ZS), F32)],
        compiler_params=PARAMS,
    )(v, *created, first, second, inner, extra)


STATE_G, STATE_H, STATE_D, STATE_ROWS = 0, BASIS, 2 * BASIS, 2 * BASIS + 8


def summed_rows(recv_ref, count):
    period = count
    while period % 8:
        period += count
    total = jnp.sum(recv_ref[...].reshape(-1, period, 128), axis=0)
    if count in (1, 2):
        while count < 8:
            total = total + pltpu.roll(total, 8 - count, 0)
            count *= 2
        return total
    return sum(total[p : p + count] for p in range(0, period, count))


def unpacked_gram(packed, pack_ref):
    pack_ref[...] = jnp.zeros((128, 128), F32)
    for p in range(HALF // PACK):
        part = packed
        if p:
            part = pltpu.roll(part, 128 - p * PACK_LANES, 1)
        pack_ref[pl.ds(p * PACK, PACK), :] = part
    turned = jnp.transpose(pack_ref[...])
    plain = pack_ref[pl.ds(0, HALF), :]
    lane = iota((HALF, 128), 1)
    sub = iota((HALF, 128), 0)
    diagonal = jnp.sum(jnp.where(lane == KEEP, plain, 0.0), axis=1, keepdims=True)
    top = jnp.where((lane > sub) | (lane >= HALF), plain, turned[:HALF])
    top = jnp.where(lane == sub, diagonal, top)
    last = jnp.where(lane <= sub, plain, turned[:HALF])
    pack_ref[...] = turned
    bottom = jnp.where(lane < HALF, pack_ref[pl.ds(HALF, HALF), :], pltpu.roll(last, HALF, 1))
    pack_ref[pl.ds(0, HALF), :] = jnp.where(lane < KEEP, top, 0.0)
    pack_ref[pl.ds(HALF, HALF), :] = jnp.where(lane < KEEP, bottom, 0.0)
    pack_ref[pl.ds(KEEP, STEPS), :] = jnp.zeros((STEPS, 128), F32)


def solve_weights(count, cells, recv_ref, state_in, state_ref, weight_ref, pack_ref):
    lane = iota((1, 128), 1)
    lanes = iota((BASIS, 128), 1)
    subs = iota((BASIS, 128), 0)
    sub = iota((BASIS, 1), 0)
    scale = 1.0 / cells

    def spread(values):
        return jnp.sum(values, axis=1, keepdims=True)

    if count == 0:
        total = summed_rows(recv_ref, PACK) * scale
        unpacked_gram(total[:PACK], pack_ref)
        gram = pack_ref[pl.ds(0, BASIS), :]
        hess = jnp.zeros((BASIS, 128), F32)
        inverse_row = jnp.where(lane < KEEP, 1.0, 0.0)
        inverse_column = jnp.where(sub < KEEP, 1.0, 0.0)
        first_row = jnp.zeros((1, 128), F32)
        for r in range(PACK):
            part = pltpu.roll(total[r : r + 1], 128 - FREE_LANE + r * PACK, 1)
            mine = (lane >= r * PACK) & (lane < (r + 1) * PACK)
            first_row = jnp.where(mine, part, first_row)
        inverse = jnp.ones((1, 1), F32)
        image_square = None
        first = to_column(first_row)
        folded = spread(gram * first_row)
    else:
        total = summed_rows(recv_ref, 1)[0:1] * scale
        newest = KEEP + count - 1
        raw_first = total
        raw_gram = pltpu.roll(total, 128 - OWN_LANE, 1)
        inverse_row = state_in[pl.ds(STATE_D, 1), :]
        gram = state_in[pl.ds(STATE_G, BASIS), :]
        hess = state_in[pl.ds(STATE_H, BASIS), :]
        part_first, part_gram = raw_first * inverse_row, raw_gram * inverse_row
        square = spread(jnp.where(lane == newest, raw_gram, 0.0))
        first_newest = spread(jnp.where(lane == newest, raw_first, 0.0))
        image_square = spread(jnp.where(lane == BASIS - 1, raw_first, 0.0))
        crossed = spread(part_gram * part_first)
        first_column, gram_column = to_column(part_first), to_column(part_gram)
        inverse_column = to_column(inverse_row)
        folded = spread(gram * part_first)
        norm = jnp.sqrt(square + EPSILON)
        inverse = 1.0 / norm
        own = square * inverse * inverse
        first_newest = first_newest * inverse * inverse
        image_square = image_square * inverse * inverse
        mine = sub == newest
        first = jnp.where(mine, first_newest, first_column * inverse)
        gram_column = gram_column * inverse
        folded = jnp.where(
            mine,
            crossed * inverse * inverse + own * first_newest,
            folded * inverse + gram_column * first_newest,
        )
        gram = jnp.where(lanes == newest, gram_column, gram)
        gram = jnp.where(subs == newest, part_gram * inverse, gram)
        gram = jnp.where((lanes == newest) & (subs == newest), own, gram)
        hess = jnp.where((subs == newest) & (lanes == count - 1), norm, hess)
        inverse_row = jnp.where(lane == newest, inverse, inverse_row)
        inverse_column = jnp.where(mine, inverse, inverse_column)
    weights = first + (first - folded)
    weight_ref[pl.ds(0, BASIS), :] = jnp.broadcast_to(weights * inverse_column, (BASIS, ZS))
    weight_ref[pl.ds(BASIS, 8), :] = jnp.broadcast_to(inverse, (8, ZS))
    hess = jnp.where((lanes == count) & (subs < KEEP + count), weights, hess)
    state_ref[pl.ds(STATE_G, BASIS), :] = gram
    state_ref[pl.ds(STATE_H, BASIS), :] = hess
    state_ref[pl.ds(STATE_D, 8), :] = jnp.broadcast_to(inverse_row, (8, 128))
    return weights, first, gram, image_square


def combined(rows, weight_ref, w_ref, v_ref, others):
    value = w_ref[rows, :] * weight_ref[pl.ds(BASIS, 1), :]
    for i in range(KEEP):
        value = value - weight_ref[pl.ds(i, 1), :] * v_ref[i, rows, :]
    for i, other in enumerate(others):
        value = value - weight_ref[pl.ds(KEEP + i, 1), :] * other[rows, :]
    return value


def combine_half(out_ref, high, weight_ref, w_ref, v_ref, others):
    start = high.astype(jnp.int32) * (ROWS // 2)

    def step(c, carry):
        rows = pl.ds(pl.multiple_of(start + c * CHUNK, CHUNK), CHUNK)
        out_ref[pl.ds(pl.multiple_of(c * CHUNK, CHUNK), CHUNK), :] = combined(
            rows, weight_ref, w_ref, v_ref, others
        )
        return carry

    lax.fori_loop(0, ROWS // 2 // CHUNK, step, 0)


HALF_SHAPE = jax.ShapeDtypeStruct((ROWS // 2, ZS), F32)
WEIGHT_SHAPE = (BASIS + 8, ZS)


def far_kernel(count, cells, *refs):
    recv_ref, w_ref, v_ref, *others = refs[: 3 + count]
    *states, far_ref, weight_ref, state_ref, pack_ref = refs[3 + count :]
    state_in = states[0] if states else None
    solve_weights(count, cells, recv_ref, state_in, state_ref, weight_ref, pack_ref)
    odd = lax.axis_index("gx") % 2 == 1
    combine_half(far_ref, odd, weight_ref, w_ref, v_ref, others)


def far_call(recv, w, v, created, state, cells):
    count = len(created)
    states = [state] if created else []
    return pl.pallas_call(
        functools.partial(far_kernel, count, cells),
        in_specs=[VMEM_SPEC] * (3 + count + len(states)),
        out_specs=(VMEM_SPEC,) * 3,
        out_shape=(
            HALF_SHAPE,
            pltpu.VMEM(WEIGHT_SHAPE, F32),
            jax.ShapeDtypeStruct((STATE_ROWS, 128), F32),
        ),
        scratch_shapes=[pltpu.VMEM((128, 128), F32)],
        compiler_params=PARAMS,
    )(recv, w, v, *created, *states)


def near_kernel(count, *refs):
    weight_ref, far_ref, w_ref, v_ref, *others = refs[: 4 + count]
    near_ref, swap_ref = refs[4 + count :]
    odd = lax.axis_index("gx") % 2 == 1
    upper = lax.axis_index("gy") == 1
    combine_half(near_ref, jnp.logical_not(odd), weight_ref, w_ref, v_ref, others)
    for x in range(XS):
        sides = []
        for y in (0, YS - 2):
            rows = pl.ds((x % 2) * YS + y, 2)
            low, high = (near_ref, far_ref) if x < 2 else (far_ref, near_ref)
            sides.append(jnp.where(odd, low[rows, :], high[rows, :]))
        swap_ref[pl.ds(2 * x, 2), :] = jnp.where(upper, *sides)


def near_call(weight, far, w, v, created):
    count = len(created)
    return pl.pallas_call(
        functools.partial(near_kernel, count),
        in_specs=[VMEM_SPEC] * (4 + count),
        out_specs=(VMEM_SPEC,) * 2,
        out_shape=(HALF_SHAPE, jax.ShapeDtypeStruct((2 * XS, ZS), F32)),
        compiler_params=PARAMS,
    )(weight, far, w, v, *created)


def last_kernel(cells, *refs):
    count = STEPS - 1
    recv_ref, w_ref, v_ref, *others = refs[: 3 + count]
    state_in, u_ref, state_ref, square_ref, guess_ref, sound_ref, weight_ref = refs[3 + count :]
    weights, first, gram, image_square = solve_weights(
        count, cells, recv_ref, state_in, state_ref, weight_ref, None
    )
    again = jnp.sum(gram * to_row(weights), axis=1, keepdims=True)
    guess = image_square - jnp.sum(weights * (2.0 * first - again), axis=0, keepdims=True)
    guess_ref[...] = jnp.where(iota((1, 128), 1) == 0, guess, 0.0)
    sound = jnp.where(guess > SOUND_SHARE * image_square, 1, 0)
    sound_ref[0] = sound[0, 0]

    def step(c, acc):
        rows = pl.ds(pl.multiple_of(c * BLOCK, BLOCK), BLOCK)
        value = combined(rows, weight_ref, w_ref, v_ref, others)
        u_ref[rows, :] = value
        return acc + fold_tiles(value * value)

    acc = lax.fori_loop(0, ROWS // BLOCK, step, jnp.zeros((8, ZS), F32))
    square_ref[...] = fold_row(acc)


def last_call(recv, w, v, created, state, cells):
    return pl.pallas_call(
        functools.partial(last_kernel, cells),
        in_specs=[VMEM_SPEC] * (4 + len(created)),
        out_specs=(VMEM_SPEC,) * 4 + (SMEM_SPEC,),
        out_shape=(
            pltpu.VMEM((ROWS, ZS), F32),
            jax.ShapeDtypeStruct((STATE_ROWS, 128), F32),
            *LAST_SHAPES,
        ),
        scratch_shapes=[pltpu.VMEM(WEIGHT_SHAPE, F32)],
        compiler_params=PARAMS,
        name="last",
    )(recv, w, v, *created, state)


def finish_kernel(*refs):
    square_ref, state_ref, *created = refs[: 2 + STEPS]
    new_ref, hess_ref = refs[2 + STEPS :]
    lane = iota((1, 128), 1)
    norm = jnp.sqrt(jnp.sum(square_ref[...], axis=1, keepdims=True) + EPSILON)
    lanes = iota((BASIS, 128), 1)
    subs = iota((BASIS, 128), 0)
    hess = state_ref[pl.ds(STATE_H, BASIS), :]
    hess = jnp.where((subs == BASIS - 1) & (lanes == STEPS - 1), norm, hess)
    hess_ref[...] = jnp.transpose(jnp.concatenate([hess, jnp.zeros((128 - BASIS, 128), F32)], axis=0))[:STEPS, :BASIS]
    inverse_row = state_ref[pl.ds(STATE_D, 1), :]
    for j, u_ref in enumerate(created):
        if j == STEPS - 1:
            inverse = 1.0 / norm
        else:
            inverse = jnp.sum(jnp.where(lane == KEEP + j, inverse_row, 0.0), axis=1, keepdims=True)
        for c in range(ROWS // CHUNK):
            rows = pl.ds(c * CHUNK, CHUNK)
            new_ref[j, rows, :] = u_ref[rows, :] * inverse


def finish_call(square, state, created):
    return pl.pallas_call(
        finish_kernel,
        in_specs=[VMEM_SPEC] * (2 + STEPS),
        out_specs=(VMEM_SPEC, VMEM_SPEC),
        out_shape=(
            jax.ShapeDtypeStruct((STEPS, ROWS, ZS), F32),
            jax.ShapeDtypeStruct((STEPS, BASIS), F32),
        ),
        compiler_params=PARAMS,
        name="finish",
    )(square, state, *created)


def paired(half, start):
    lower = range(start, lax.axis_size("gx") - 1, 2)
    return lax.ppermute(half, "gx", [(i, i + 1) for i in lower] + [(i + 1, i) for i in lower])


def across(edge):
    return lax.ppermute(edge, "gy", [(0, 1), (1, 0)])


def from_all(payload):
    axes = ("gy", "gx")
    devices = lax.axis_size(axes)
    copies = payload.reshape(devices, 1, -1)
    got = lax.all_to_all(copies, axes, split_axis=0, concat_axis=0, tiled=True)
    return got.reshape(-1, 128)


def body(basis_vectors, reaction):
    devices = lax.axis_size(("gy", "gx"))
    cells = float(ROWS * ZS * devices)
    basis = basis_vectors.reshape(KEEP, ROWS, ZS)
    v, near, far, swap, early = start_call(basis)
    second = paired(far, 1)
    first = paired(near, 0)
    swap = across(swap)
    reaction = reaction.reshape(ROWS, ZS)
    extra = gram_call(v, early)
    w, payload = first_image_call(v, (first, second, swap), reaction, extra, devices)
    created = []
    state = None
    for _ in range(1, STEPS):
        recv = from_all(payload)
        far, weight, state = far_call(recv, w, v, created, state, cells)
        second = paired(far, 1)
        near, swap = near_call(weight, far, w, v, created)
        first = paired(near, 0)
        swap = across(swap)
        u, inner, extra = inner_call(v, near, far, created, swap, reaction)
        created.append(u)
        w, payload = outer_call(v, created, first, second, inner, extra, devices)
    u, state, square, guess, sound = last_call(from_all(payload), w, v, created, state, cells)
    created.append(u)
    square = lax.cond(
        sound[0] == 1,
        lambda guess, square: guess,
        lambda guess, square: jnp.sum(from_all(square), axis=0, keepdims=True) * (1.0 / cells),
        guess,
        jnp.broadcast_to(square, (devices, 128)),
    )
    new, hessenberg = finish_call(square, state, created)
    return new.reshape(STEPS, XS, YS, ZS), hessenberg.T


def solution(mesh):
    return jax.shard_map(
        body,
        mesh=mesh,
        in_specs=(P(None, "gx", "gy", None), P("gx", "gy", None)),
        out_specs=(P(None, "gx", "gy", None), P()),
        check_vma=False,
    )
```

```python
import functools

import jax
import jax.numpy as jnp
from jax import lax
from jax.experimental import pallas as pl
from jax.experimental.pallas import tpu as pltpu
from jax.sharding import PartitionSpec as P


KEEP = 36
STEPS = 4
BASIS = KEEP + STEPS
WIND_SPEEDS = (0.9, 0.6, 0.4)
EPSILON = 1e-06
F32 = jnp.float32

XS, YS, ZS = 4, 64, 256
ROWS = XS * YS
GROUP = 4
GRAM_ROWS = 64
HALF = KEEP // 2
PACK = 6
PACK_LANES = 38
FREE_LANE = 113
SHARE = PACK // 2
FREE = KEEP // SHARE
OWN_LANE = 64
CHUNK = 32
BLOCK = 64
SOUND_SHARE = 0.05

PARAMS = pltpu.CompilerParams(vmem_limit_bytes=16 * 2**20)
SMEM_SPEC = pl.BlockSpec(memory_space=pltpu.SMEM)
VMEM_SPEC = pl.BlockSpec(memory_space=pltpu.VMEM)


def iota(shape, axis):
    return lax.broadcasted_iota(jnp.int32, shape, axis)


def to_column(row):
    pick = iota((BASIS, 128), 0) == iota((BASIS, 128), 1)
    return jnp.sum(jnp.where(pick, row, 0.0), axis=1, keepdims=True)


def to_row(column):
    pick = iota((BASIS, 128), 0) == iota((BASIS, 128), 1)
    return jnp.sum(jnp.where(pick, column, 0.0), axis=0, keepdims=True)


def fold_tiles(block):
    return jnp.sum(block.reshape(-1, 8, ZS), axis=0)


def fold_row(acc):
    return jnp.sum(acc[:, :128] + acc[:, 128:], axis=0, keepdims=True)


def gram_block(v_ref, sums_ref, ga, gb):
    pairs = [(a, b) for a in range(GROUP) for b in range(GROUP) if ga != gb or a <= b]

    def step(t, accs):
        accs = list(accs)
        for part in range(GRAM_ROWS // 8):
            rows = pl.ds(pl.multiple_of(t * GRAM_ROWS, GRAM_ROWS) + 8 * part, 8)
            for half in range(2):
                lanes = pl.ds(half * 128, 128)
                left = [v_ref[ga * GROUP + a, rows, lanes] for a in range(GROUP)]
                right = left
                if ga != gb:
                    right = [v_ref[gb * GROUP + b, rows, lanes] for b in range(GROUP)]
                for n, (a, b) in enumerate(pairs):
                    accs[n] = accs[n] + left[a] * right[b]
        return tuple(accs)

    zero = jnp.zeros((8, 128), F32)
    accs = lax.fori_loop(0, ROWS // GRAM_ROWS, step, tuple(zero for _ in pairs))
    for (a, b), acc in zip(pairs, accs):
        row = jnp.sum(acc, axis=0, keepdims=True)
        i, j = ga * GROUP + a, gb * GROUP + b
        sums_ref[i, pl.ds(j, 1), :] = row
        if i != j:
            sums_ref[j, pl.ds(i, 1), :] = row


def write_edges(u_ref, first_ref, second_ref, swap_ref):
    odd = lax.axis_index("gx") % 2 == 1
    upper = lax.axis_index("gy") == 1
    for x in range(2):
        low = u_ref[pl.ds(x * YS, YS), :]
        high = u_ref[pl.ds((XS - 2 + x) * YS, YS), :]
        first_ref[pl.ds(x * YS, YS), :] = jnp.where(odd, low, high)
        second_ref[pl.ds(x * YS, YS), :] = jnp.where(odd, high, low)
    for x in range(XS):
        low = u_ref[pl.ds(x * YS, 2), :]
        high = u_ref[pl.ds(x * YS + YS - 2, 2), :]
        swap_ref[pl.ds(2 * x, 2), :] = jnp.where(upper, low, high)


EDGE_SHAPES = (
    jax.ShapeDtypeStruct((2 * YS, ZS), F32),
    jax.ShapeDtypeStruct((2 * YS, ZS), F32),
    jax.ShapeDtypeStruct((2 * XS, ZS), F32),
)


ARRIVAL = [KEEP // GROUP - 1, *range(KEEP // GROUP - 1)]
EARLY = 4
LATE_PAIRS = [
    (ARRIVAL[m], ARRIVAL[n]) for n in range(EARLY, len(ARRIVAL)) for m in range(n + 1)
]


def start_kernel(v_hbm, v_ref, first_ref, second_ref, swap_ref, sums_ref, sems):
    copies = {}
    for g in ARRIVAL:
        part = pl.ds(g * GROUP, GROUP)
        copies[g] = pltpu.make_async_copy(v_hbm.at[part], v_ref.at[part], sems.at[g])
        copies[g].start()
    for n, g in enumerate(ARRIVAL[:EARLY]):
        copies[g].wait()
        if n == 0:
            write_edges(v_ref.at[KEEP - 1], first_ref, second_ref, swap_ref)
        for m in range(n + 1):
            gram_block(v_ref, sums_ref, ARRIVAL[m], g)
    for g in ARRIVAL[EARLY:]:
        copies[g].wait()


def start_call(basis):
    return pl.pallas_call(
        start_kernel,
        in_specs=[pl.BlockSpec(memory_space=pltpu.HBM)],
        out_specs=(VMEM_SPEC,) * 5,
        out_shape=(
            pltpu.VMEM((KEEP, ROWS, ZS), F32),
            *EDGE_SHAPES,
            pltpu.VMEM((KEEP, KEEP, 128), F32),
        ),
        scratch_shapes=[pltpu.SemaphoreType.DMA((KEEP // GROUP,))],
        compiler_params=PARAMS,
        name="start",
    )(pltpu.with_memory_space_constraint(basis, pltpu.HBM))


def gram_kernel(v_ref, early_ref, keep_ref, give_ref, sums_ref, matrix_ref):
    for ga, gb in LATE_PAIRS:
        gram_block(v_ref, sums_ref, ga, gb)
    early = sorted(g * GROUP + a for g in ARRIVAL[:EARLY] for a in range(GROUP))

    def line(i, start):
        part = sums_ref[i, pl.ds(start, HALF), :]
        if i in early:
            sub = iota((HALF, 128), 0) + start
            in_early = (sub < (EARLY - 1) * GROUP) | (sub >= KEEP - GROUP)
            part = jnp.where(in_early, early_ref[i, pl.ds(start, HALF), :], part)
        return part

    sub = iota((HALF, 128), 0)
    lane = iota((HALF, 128), 1)
    packed = jnp.zeros((HALF, 128), F32)
    diagonal = jnp.zeros((HALF, 128), F32)
    for i in range(KEEP):
        part = line(i, 0)
        if i < HALF:
            diagonal = jnp.where(sub == i, part, diagonal)
            part = jnp.where(sub < i, part, line(HALF + i, HALF))
        packed = jnp.where(lane == i, jnp.sum(part, axis=1, keepdims=True), packed)
    packed = jnp.where(lane == KEEP, jnp.sum(diagonal, axis=1, keepdims=True), packed)
    matrix_ref[pl.ds(0, HALF), :] = packed
    packed = matrix_ref[pl.ds(0, PACK), :]
    for p in range(1, HALF // PACK):
        packed = packed + pltpu.roll(matrix_ref[pl.ds(p * PACK, PACK), :], p * PACK_LANES, 1)
    upper = lax.axis_index("gy") == 1
    low, high = packed[:SHARE], packed[SHARE:]
    keep_ref[...] = jnp.where(upper, high, low)
    give_ref[...] = jnp.where(upper, low, high)


def gram_call(v, early):
    return pl.pallas_call(
        gram_kernel,
        in_specs=[VMEM_SPEC, VMEM_SPEC],
        out_specs=(VMEM_SPEC, VMEM_SPEC),
        out_shape=(jax.ShapeDtypeStruct((SHARE, 128), F32),) * 2,
        scratch_shapes=[pltpu.VMEM((KEEP, KEEP, 128), F32), pltpu.VMEM((BASIS, 128), F32)],
        compiler_params=PARAMS,
        name="gram",
    )(v, early)


ALL_PLANES = ((0, XS),)


def dot_all(v_ref, others, x_refs, dots_refs, planes=ALL_PLANES):
    batch = 12 // len(x_refs)
    for dots_ref in dots_refs:
        dots_ref[...] = jnp.zeros((BASIS, 128), F32)

    def run(reads, base):
        def step(c, accs):
            rows = pl.ds(pl.multiple_of(c * CHUNK, CHUNK), CHUNK)
            xs = [x_ref[rows, :] for x_ref in x_refs]
            new = []
            for n, read in enumerate(reads):
                value = read(rows)
                new += [accs[n * len(xs) + m] + fold_tiles(value * x) for m, x in enumerate(xs)]
            return tuple(new)

        zero = jnp.zeros((8, ZS), F32)
        accs = (zero,) * (len(reads) * len(x_refs))
        for first, end in planes:
            accs = lax.fori_loop(first * YS // CHUNK, end * YS // CHUNK, step, accs)
        for n, acc in enumerate(accs):
            row = base + n // len(x_refs)
            dots_refs[n % len(x_refs)][pl.ds(row, 1), :] = fold_row(acc)

    for first in range(0, KEEP, batch):
        run([lambda rows, i=i: v_ref[i, rows, :] for i in range(first, first + batch)], first)
    if others:
        run([lambda rows, r=r: r[rows, :] for r in others], KEEP)
    return [to_row(jnp.sum(dots_ref[...], axis=1, keepdims=True)) for dots_ref in dots_refs]


CENTER = -6.0 - 1.5 * sum(WIND_SPEEDS)
NEAR = [1.0 + 2.0 * s for s in WIND_SPEEDS]
FAR = [-0.5 * s for s in WIND_SPEEDS]


def inner_image(source, swap_ref, reaction_ref, pad_ref, x):
    upper = lax.axis_index("gy").astype(F32)
    lane = iota((YS, ZS), 1)
    mine = source[pl.ds(x * YS, YS), :]
    pad_ref[x, pl.ds(8, YS), :] = mine
    edge = swap_ref[pl.ds(2 * x, 2), :]
    pad_ref[x, pl.ds(6, 2), :] = edge * upper
    pad_ref[x, pl.ds(72, 1), :] = edge[0:1] * (1.0 - upper)
    image = (CENTER - reaction_ref[pl.ds(x * YS, YS), :]) * mine
    for distance, factor in ((1, 1.0), (-1, NEAR[0]), (-2, FAR[0])):
        if 0 <= x + distance < XS:
            image = image + factor * source[pl.ds((x + distance) * YS, YS), :]
    image = (
        image
        + pad_ref[x, pl.ds(9, YS), :]
        + NEAR[1] * pad_ref[x, pl.ds(7, YS), :]
        + FAR[1] * pad_ref[x, pl.ds(6, YS), :]
    )
    return (
        image
        + jnp.where(lane < ZS - 1, pltpu.roll(mine, ZS - 1, 1), 0.0)
        + NEAR[2] * jnp.where(lane >= 1, pltpu.roll(mine, 1, 1), 0.0)
        + FAR[2] * jnp.where(lane >= 2, pltpu.roll(mine, 2, 1), 0.0)
    )


def outer_image(first_ref, second_ref):
    odd = lax.axis_index("gx") % 2 == 1

    def below(rows):
        return jnp.where(odd, first_ref[rows, :], second_ref[rows, :])

    two, one = below(pl.ds(0, YS)), below(pl.ds(YS, YS))
    rows = pl.ds(0, YS)
    above = jnp.where(odd, second_ref[rows, :], first_ref[rows, :])
    return {0: NEAR[0] * one + FAR[0] * two, 1: FAR[0] * one, XS - 1: above}


LAST_SHAPES = (
    jax.ShapeDtypeStruct((1, 128), F32),
    jax.ShapeDtypeStruct((1, 128), F32),
    jax.ShapeDtypeStruct((1,), jnp.int32),
)


def write_for_all(out_ref, rows):
    count = len(rows)
    period = count
    while period % 8:
        period += count
    for tile in range(period // 8):
        sub = iota((8, 128), 0)
        block = jnp.zeros((8, 128), F32)
        for r in range(8):
            block = jnp.where(sub == r, rows[(8 * tile + r) % count], block)
        for p in range(out_ref.shape[0] // period):
            out_ref[pl.ds(p * period + 8 * tile, 8), :] = block


def first_image_kernel(
    v_ref, first_ref, second_ref, swap_ref, reaction_ref, w_ref, out_ref, dots_ref, pad_ref
):
    outer = outer_image(first_ref, second_ref)
    for x in range(XS):
        image = inner_image(v_ref.at[KEEP - 1], swap_ref, reaction_ref, pad_ref, x)
        w_ref[pl.ds(x * YS, YS), :] = image + outer[x] if x in outer else image
    (out_ref[...],) = dot_all(v_ref, [], [w_ref], [dots_ref])


def first_image_call(v, halo, reaction):
    return pl.pallas_call(
        first_image_kernel,
        in_specs=[VMEM_SPEC] * 5,
        out_specs=(VMEM_SPEC, VMEM_SPEC),
        out_shape=(pltpu.VMEM((ROWS, ZS), F32), jax.ShapeDtypeStruct((1, 128), F32)),
        scratch_shapes=[
            pltpu.VMEM((BASIS, 128), F32),
            pltpu.VMEM((XS, YS + 16, ZS), F32),
        ],
        compiler_params=PARAMS,
        name="image_0",
    )(v, *halo, reaction)


def first_payload_kernel(row_ref, keep_ref, got_ref, out_ref):
    gram = keep_ref[...] + got_ref[...]
    row = row_ref[...]
    lane = iota((1, 128), 1)
    free = (lane >= FREE_LANE) & (lane < FREE_LANE + FREE)
    rows = []
    for r in range(SHARE):
        part = jnp.where(free, pltpu.roll(row, FREE_LANE - r * FREE, 1), 0.0)
        rows.append(gram[r : r + 1] + part)
    write_for_all(out_ref, rows)


def first_payload_call(row, keep, got, devices):
    return pl.pallas_call(
        first_payload_kernel,
        in_specs=[VMEM_SPEC] * 3,
        out_specs=VMEM_SPEC,
        out_shape=jax.ShapeDtypeStruct((devices * SHARE, 128), F32),
        compiler_params=PARAMS,
        name="payload_0",
    )(row, keep, got)


def inner_kernel(count, *refs):
    v_ref, near_ref, far_ref, *older = refs[: 2 + count]
    swap_ref, reaction_ref, u_ref, w_ref, out_ref, dots_ref, more_ref, pad_ref = refs[2 + count :]
    odd = lax.axis_index("gx") % 2 == 1
    for x in range(2):
        rows = pl.ds(x * YS, YS)
        near, far = near_ref[rows, :], far_ref[rows, :]
        u_ref[pl.ds(x * YS, YS), :] = jnp.where(odd, near, far)
        u_ref[pl.ds((2 + x) * YS, YS), :] = jnp.where(odd, far, near)
    for x in range(XS):
        w_ref[pl.ds(x * YS, YS), :] = inner_image(u_ref, swap_ref, reaction_ref, pad_ref, x)
    row, own = dot_all(v_ref, [*older, u_ref], [w_ref, u_ref], [dots_ref, more_ref])
    out_ref[...] = row + pltpu.roll(own, OWN_LANE, 1)


def inner_call(v, near, far, older, swap, reaction):
    count = 1 + len(older)
    return pl.pallas_call(
        functools.partial(inner_kernel, count),
        in_specs=[VMEM_SPEC] * (4 + count),
        out_specs=(VMEM_SPEC,) * 3,
        out_shape=(
            pltpu.VMEM((ROWS, ZS), F32),
            pltpu.VMEM((ROWS, ZS), F32),
            jax.ShapeDtypeStruct((1, 128), F32),
        ),
        scratch_shapes=[
            pltpu.VMEM((BASIS, 128), F32),
            pltpu.VMEM((BASIS, 128), F32),
            pltpu.VMEM((XS, YS + 16, ZS), F32),
        ],
        compiler_params=PARAMS,
    )(v, near, far, *older, swap, reaction)


def outer_kernel(count, *refs):
    v_ref, *others = refs[: 1 + count]
    first_ref, second_ref, inner_ref, extra_ref = refs[1 + count : 5 + count]
    w_ref, out_ref, dots_ref, delta_ref = refs[5 + count :]
    outer = outer_image(first_ref, second_ref)
    for x in range(XS):
        rows = pl.ds(x * YS, YS)
        image = inner_ref[rows, :]
        if x in outer:
            delta_ref[rows, :] = outer[x]
            image = image + outer[x]
        w_ref[rows, :] = image
    (row,) = dot_all(v_ref, others, [delta_ref], [dots_ref], ((0, 2), (3, 4)))
    row = row + extra_ref[...]
    if count == STEPS - 1:
        square = jnp.zeros((8, ZS), F32)
        for c in range(ROWS // CHUNK):
            image = w_ref[pl.ds(c * CHUNK, CHUNK), :]
            square = square + fold_tiles(image * image)
        square = jnp.sum(fold_row(square), axis=1, keepdims=True)
        row = jnp.where(iota((1, 128), 1) == BASIS - 1, square, row)
    write_for_all(out_ref, [row])


def outer_call(v, created, first, second, inner, extra, devices):
    count = len(created)
    return pl.pallas_call(
        functools.partial(outer_kernel, count),
        in_specs=[VMEM_SPEC] * (5 + count),
        out_specs=(VMEM_SPEC, VMEM_SPEC),
        out_shape=(
            pltpu.VMEM((ROWS, ZS), F32),
            jax.ShapeDtypeStruct((devices, 128), F32),
        ),
        scratch_shapes=[pltpu.VMEM((BASIS, 128), F32), pltpu.VMEM((ROWS, ZS), F32)],
        compiler_params=PARAMS,
    )(v, *created, first, second, inner, extra)


STATE_G, STATE_H, STATE_D, STATE_ROWS = 0, BASIS, 2 * BASIS, 2 * BASIS + 8


def summed_rows(recv_ref, count):
    period = count
    while period % 8:
        period += count
    total = jnp.sum(recv_ref[...].reshape(-1, period, 128), axis=0)
    if count in (1, 2):
        while count < 8:
            total = total + pltpu.roll(total, 8 - count, 0)
            count *= 2
        return total
    return sum(total[p : p + count] for p in range(0, period, count))


def unpacked_gram(packed, pack_ref):
    pack_ref[...] = jnp.zeros((128, 128), F32)
    for p in range(HALF // PACK):
        part = packed
        if p:
            part = pltpu.roll(part, 128 - p * PACK_LANES, 1)
        pack_ref[pl.ds(p * PACK, PACK), :] = part
    turned = jnp.transpose(pack_ref[...])
    plain = pack_ref[pl.ds(0, HALF), :]
    lane = iota((HALF, 128), 1)
    sub = iota((HALF, 128), 0)
    diagonal = jnp.sum(jnp.where(lane == KEEP, plain, 0.0), axis=1, keepdims=True)
    top = jnp.where((lane > sub) | (lane >= HALF), plain, turned[:HALF])
    top = jnp.where(lane == sub, diagonal, top)
    last = jnp.where(lane <= sub, plain, turned[:HALF])
    pack_ref[...] = turned
    bottom = jnp.where(lane < HALF, pack_ref[pl.ds(HALF, HALF), :], pltpu.roll(last, HALF, 1))
    pack_ref[pl.ds(0, HALF), :] = jnp.where(lane < KEEP, top, 0.0)
    pack_ref[pl.ds(HALF, HALF), :] = jnp.where(lane < KEEP, bottom, 0.0)
    pack_ref[pl.ds(KEEP, STEPS), :] = jnp.zeros((STEPS, 128), F32)


def solve_weights(count, cells, recv_ref, state_in, state_ref, weight_ref, pack_ref):
    lane = iota((1, 128), 1)
    lanes = iota((BASIS, 128), 1)
    subs = iota((BASIS, 128), 0)
    sub = iota((BASIS, 1), 0)
    scale = 1.0 / cells

    def spread(values):
        return jnp.sum(values, axis=1, keepdims=True)

    if count == 0:
        half = recv_ref.shape[0] // 2
        low = summed_rows(recv_ref.at[pl.ds(0, half)], SHARE) * scale
        high = summed_rows(recv_ref.at[pl.ds(half, half)], SHARE) * scale
        pack_ref[pl.ds(0, SHARE), :] = low
        pack_ref[pl.ds(SHARE, SHARE), :] = high
        total = low + high
        unpacked_gram(pack_ref[pl.ds(0, PACK), :], pack_ref)
        gram = pack_ref[pl.ds(0, BASIS), :]
        hess = jnp.zeros((BASIS, 128), F32)
        inverse_row = jnp.where(lane < KEEP, 1.0, 0.0)
        inverse_column = jnp.where(sub < KEEP, 1.0, 0.0)
        first_row = jnp.zeros((1, 128), F32)
        for r in range(SHARE):
            part = pltpu.roll(total[r : r + 1], 128 - FREE_LANE + r * FREE, 1)
            mine = (lane >= r * FREE) & (lane < (r + 1) * FREE)
            first_row = jnp.where(mine, part, first_row)
        inverse = jnp.ones((1, 1), F32)
        image_square = None
        first = to_column(first_row)
        folded = spread(gram * first_row)
    else:
        total = summed_rows(recv_ref, 1)[0:1] * scale
        newest = KEEP + count - 1
        raw_first = total
        raw_gram = pltpu.roll(total, 128 - OWN_LANE, 1)
        inverse_row = state_in[pl.ds(STATE_D, 1), :]
        gram = state_in[pl.ds(STATE_G, BASIS), :]
        hess = state_in[pl.ds(STATE_H, BASIS), :]
        part_first, part_gram = raw_first * inverse_row, raw_gram * inverse_row
        square = spread(jnp.where(lane == newest, raw_gram, 0.0))
        first_newest = spread(jnp.where(lane == newest, raw_first, 0.0))
        image_square = spread(jnp.where(lane == BASIS - 1, raw_first, 0.0))
        crossed = spread(part_gram * part_first)
        first_column, gram_column = to_column(part_first), to_column(part_gram)
        inverse_column = to_column(inverse_row)
        folded = spread(gram * part_first)
        norm = jnp.sqrt(square + EPSILON)
        inverse = 1.0 / norm
        own = square * inverse * inverse
        first_newest = first_newest * inverse * inverse
        image_square = image_square * inverse * inverse
        mine = sub == newest
        first = jnp.where(mine, first_newest, first_column * inverse)
        gram_column = gram_column * inverse
        folded = jnp.where(
            mine,
            crossed * inverse * inverse + own * first_newest,
            folded * inverse + gram_column * first_newest,
        )
        gram = jnp.where(lanes == newest, gram_column, gram)
        gram = jnp.where(subs == newest, part_gram * inverse, gram)
        gram = jnp.where((lanes == newest) & (subs == newest), own, gram)
        hess = jnp.where((subs == newest) & (lanes == count - 1), norm, hess)
        inverse_row = jnp.where(lane == newest, inverse, inverse_row)
        inverse_column = jnp.where(mine, inverse, inverse_column)
    weights = first + (first - folded)
    weight_ref[pl.ds(0, BASIS), :] = jnp.broadcast_to(weights * inverse_column, (BASIS, ZS))
    weight_ref[pl.ds(BASIS, 8), :] = jnp.broadcast_to(inverse, (8, ZS))
    hess = jnp.where((lanes == count) & (subs < KEEP + count), weights, hess)
    state_ref[pl.ds(STATE_G, BASIS), :] = gram
    state_ref[pl.ds(STATE_H, BASIS), :] = hess
    state_ref[pl.ds(STATE_D, 8), :] = jnp.broadcast_to(inverse_row, (8, 128))
    return weights, first, gram, image_square


def combined(rows, weight_ref, w_ref, v_ref, others):
    value = w_ref[rows, :] * weight_ref[pl.ds(BASIS, 1), :]
    for i in range(KEEP):
        value = value - weight_ref[pl.ds(i, 1), :] * v_ref[i, rows, :]
    for i, other in enumerate(others):
        value = value - weight_ref[pl.ds(KEEP + i, 1), :] * other[rows, :]
    return value


def combine_half(out_ref, high, weight_ref, w_ref, v_ref, others):
    start = high.astype(jnp.int32) * (ROWS // 2)

    def step(c, carry):
        rows = pl.ds(pl.multiple_of(start + c * CHUNK, CHUNK), CHUNK)
        out_ref[pl.ds(pl.multiple_of(c * CHUNK, CHUNK), CHUNK), :] = combined(
            rows, weight_ref, w_ref, v_ref, others
        )
        return carry

    lax.fori_loop(0, ROWS // 2 // CHUNK, step, 0)


HALF_SHAPE = jax.ShapeDtypeStruct((ROWS // 2, ZS), F32)
WEIGHT_SHAPE = (BASIS + 8, ZS)


def far_kernel(count, cells, *refs):
    recv_ref, w_ref, v_ref, *others = refs[: 3 + count]
    *states, far_ref, weight_ref, state_ref, pack_ref = refs[3 + count :]
    state_in = states[0] if states else None
    solve_weights(count, cells, recv_ref, state_in, state_ref, weight_ref, pack_ref)
    odd = lax.axis_index("gx") % 2 == 1
    combine_half(far_ref, odd, weight_ref, w_ref, v_ref, others)


def far_call(recv, w, v, created, state, cells):
    count = len(created)
    states = [state] if created else []
    return pl.pallas_call(
        functools.partial(far_kernel, count, cells),
        in_specs=[VMEM_SPEC] * (3 + count + len(states)),
        out_specs=(VMEM_SPEC,) * 3,
        out_shape=(
            HALF_SHAPE,
            pltpu.VMEM(WEIGHT_SHAPE, F32),
            jax.ShapeDtypeStruct((STATE_ROWS, 128), F32),
        ),
        scratch_shapes=[pltpu.VMEM((128, 128), F32)],
        compiler_params=PARAMS,
    )(recv, w, v, *created, *states)


def near_kernel(count, *refs):
    weight_ref, far_ref, w_ref, v_ref, *others = refs[: 4 + count]
    near_ref, swap_ref = refs[4 + count :]
    odd = lax.axis_index("gx") % 2 == 1
    upper = lax.axis_index("gy") == 1
    combine_half(near_ref, jnp.logical_not(odd), weight_ref, w_ref, v_ref, others)
    for x in range(XS):
        sides = []
        for y in (0, YS - 2):
            rows = pl.ds((x % 2) * YS + y, 2)
            low, high = (near_ref, far_ref) if x < 2 else (far_ref, near_ref)
            sides.append(jnp.where(odd, low[rows, :], high[rows, :]))
        swap_ref[pl.ds(2 * x, 2), :] = jnp.where(upper, *sides)


def near_call(weight, far, w, v, created):
    count = len(created)
    return pl.pallas_call(
        functools.partial(near_kernel, count),
        in_specs=[VMEM_SPEC] * (4 + count),
        out_specs=(VMEM_SPEC,) * 2,
        out_shape=(HALF_SHAPE, jax.ShapeDtypeStruct((2 * XS, ZS), F32)),
        compiler_params=PARAMS,
    )(weight, far, w, v, *created)


def last_kernel(cells, *refs):
    count = STEPS - 1
    recv_ref, w_ref, v_ref, *others = refs[: 3 + count]
    state_in, u_ref, state_ref, square_ref, guess_ref, sound_ref, weight_ref = refs[3 + count :]
    weights, first, gram, image_square = solve_weights(
        count, cells, recv_ref, state_in, state_ref, weight_ref, None
    )
    again = jnp.sum(gram * to_row(weights), axis=1, keepdims=True)
    guess = image_square - jnp.sum(weights * (2.0 * first - again), axis=0, keepdims=True)
    guess_ref[...] = jnp.where(iota((1, 128), 1) == 0, guess, 0.0)
    sound = jnp.where(guess > SOUND_SHARE * image_square, 1, 0)
    sound_ref[0] = sound[0, 0]

    def step(c, acc):
        rows = pl.ds(pl.multiple_of(c * BLOCK, BLOCK), BLOCK)
        value = combined(rows, weight_ref, w_ref, v_ref, others)
        u_ref[rows, :] = value
        return acc + fold_tiles(value * value)

    acc = lax.fori_loop(0, ROWS // BLOCK, step, jnp.zeros((8, ZS), F32))
    square_ref[...] = fold_row(acc)


def last_call(recv, w, v, created, state, cells):
    return pl.pallas_call(
        functools.partial(last_kernel, cells),
        in_specs=[VMEM_SPEC] * (4 + len(created)),
        out_specs=(VMEM_SPEC,) * 4 + (SMEM_SPEC,),
        out_shape=(
            pltpu.VMEM((ROWS, ZS), F32),
            jax.ShapeDtypeStruct((STATE_ROWS, 128), F32),
            *LAST_SHAPES,
        ),
        scratch_shapes=[pltpu.VMEM(WEIGHT_SHAPE, F32)],
        compiler_params=PARAMS,
        name="last",
    )(recv, w, v, *created, state)


def finish_kernel(*refs):
    square_ref, state_ref, *created = refs[: 2 + STEPS]
    new_ref, hess_ref = refs[2 + STEPS :]
    lane = iota((1, 128), 1)
    norm = jnp.sqrt(jnp.sum(square_ref[...], axis=1, keepdims=True) + EPSILON)
    lanes = iota((BASIS, 128), 1)
    subs = iota((BASIS, 128), 0)
    hess = state_ref[pl.ds(STATE_H, BASIS), :]
    hess = jnp.where((subs == BASIS - 1) & (lanes == STEPS - 1), norm, hess)
    hess_ref[...] = jnp.transpose(jnp.concatenate([hess, jnp.zeros((128 - BASIS, 128), F32)], axis=0))[:STEPS, :BASIS]
    inverse_row = state_ref[pl.ds(STATE_D, 1), :]
    for j, u_ref in enumerate(created):
        if j == STEPS - 1:
            inverse = 1.0 / norm
        else:
            inverse = jnp.sum(jnp.where(lane == KEEP + j, inverse_row, 0.0), axis=1, keepdims=True)
        for c in range(ROWS // CHUNK):
            rows = pl.ds(c * CHUNK, CHUNK)
            new_ref[j, rows, :] = u_ref[rows, :] * inverse


def finish_call(square, state, created):
    return pl.pallas_call(
        finish_kernel,
        in_specs=[VMEM_SPEC] * (2 + STEPS),
        out_specs=(VMEM_SPEC, VMEM_SPEC),
        out_shape=(
            jax.ShapeDtypeStruct((STEPS, ROWS, ZS), F32),
            jax.ShapeDtypeStruct((STEPS, BASIS), F32),
        ),
        compiler_params=PARAMS,
        name="finish",
    )(square, state, *created)


def paired(half, start):
    lower = range(start, lax.axis_size("gx") - 1, 2)
    return lax.ppermute(half, "gx", [(i, i + 1) for i in lower] + [(i + 1, i) for i in lower])


def across(edge):
    return lax.ppermute(edge, "gy", [(0, 1), (1, 0)])


def from_all(payload):
    axes = ("gy", "gx")
    devices = lax.axis_size(axes)
    copies = payload.reshape(devices, 1, -1)
    got = lax.all_to_all(copies, axes, split_axis=0, concat_axis=0, tiled=True)
    return got.reshape(-1, 128)


def body(basis_vectors, reaction):
    devices = lax.axis_size(("gy", "gx"))
    cells = float(ROWS * ZS * devices)
    basis = basis_vectors.reshape(KEEP, ROWS, ZS)
    v, near, far, swap, early = start_call(basis)
    second = paired(far, 1)
    first = paired(near, 0)
    swap = across(swap)
    reaction = reaction.reshape(ROWS, ZS)
    keep, give = gram_call(v, early)
    got = across(give)
    w, row = first_image_call(v, (first, second, swap), reaction)
    payload = first_payload_call(row, keep, got, devices)
    created = []
    state = None
    for _ in range(1, STEPS):
        recv = from_all(payload)
        far, weight, state = far_call(recv, w, v, created, state, cells)
        second = paired(far, 1)
        near, swap = near_call(weight, far, w, v, created)
        first = paired(near, 0)
        swap = across(swap)
        u, inner, extra = inner_call(v, near, far, created, swap, reaction)
        created.append(u)
        w, payload = outer_call(v, created, first, second, inner, extra, devices)
    u, state, square, guess, sound = last_call(from_all(payload), w, v, created, state, cells)
    created.append(u)
    square = lax.cond(
        sound[0] == 1,
        lambda guess, square: guess,
        lambda guess, square: jnp.sum(from_all(square), axis=0, keepdims=True) * (1.0 / cells),
        guess,
        jnp.broadcast_to(square, (devices, 128)),
    )
    new, hessenberg = finish_call(square, state, created)
    return new.reshape(STEPS, XS, YS, ZS), hessenberg.T


def solution(mesh):
    return jax.shard_map(
        body,
        mesh=mesh,
        in_specs=(P(None, "gx", "gy", None), P("gx", "gy", None)),
        out_specs=(P(None, "gx", "gy", None), P()),
        check_vma=False,
    )
```

```python
import functools

import jax
import jax.numpy as jnp
from jax import lax
from jax.experimental import pallas as pl
from jax.experimental.pallas import tpu as pltpu
from jax.sharding import PartitionSpec as P


KEEP = 36
STEPS = 4
BASIS = KEEP + STEPS
WIND_SPEEDS = (0.9, 0.6, 0.4)
EPSILON = 1e-06
F32 = jnp.float32

XS, YS, ZS = 4, 64, 256
ROWS = XS * YS
GROUP = 4
GRAM_ROWS = 64
HALF = KEEP // 2
PACK = 6
PACK_LANES = 38
FREE_LANE = 113
SHARE = PACK // 2
FREE = KEEP // SHARE
OWN_LANE = 64
CHUNK = 32
BLOCK = 64
SOUND_SHARE = 0.05

PARAMS = pltpu.CompilerParams(vmem_limit_bytes=16 * 2**20)
SMEM_SPEC = pl.BlockSpec(memory_space=pltpu.SMEM)
VMEM_SPEC = pl.BlockSpec(memory_space=pltpu.VMEM)


def iota(shape, axis):
    return lax.broadcasted_iota(jnp.int32, shape, axis)


def to_column(row):
    pick = iota((BASIS, 128), 0) == iota((BASIS, 128), 1)
    return jnp.sum(jnp.where(pick, row, 0.0), axis=1, keepdims=True)


def to_row(column):
    pick = iota((BASIS, 128), 0) == iota((BASIS, 128), 1)
    return jnp.sum(jnp.where(pick, column, 0.0), axis=0, keepdims=True)


def fold_tiles(block):
    return jnp.sum(block.reshape(-1, 8, ZS), axis=0)


def fold_row(acc):
    return jnp.sum(acc[:, :128] + acc[:, 128:], axis=0, keepdims=True)


def gram_block(v_ref, sums_ref, ga, gb):
    pairs = [(a, b) for a in range(GROUP) for b in range(GROUP) if ga != gb or a <= b]

    def step(t, accs):
        accs = list(accs)
        for part in range(GRAM_ROWS // 8):
            rows = pl.ds(pl.multiple_of(t * GRAM_ROWS, GRAM_ROWS) + 8 * part, 8)
            for half in range(2):
                lanes = pl.ds(half * 128, 128)
                left = [v_ref[ga * GROUP + a, rows, lanes] for a in range(GROUP)]
                right = left
                if ga != gb:
                    right = [v_ref[gb * GROUP + b, rows, lanes] for b in range(GROUP)]
                for n, (a, b) in enumerate(pairs):
                    accs[n] = accs[n] + left[a] * right[b]
        return tuple(accs)

    zero = jnp.zeros((8, 128), F32)
    accs = lax.fori_loop(0, ROWS // GRAM_ROWS, step, tuple(zero for _ in pairs))
    for (a, b), acc in zip(pairs, accs):
        row = jnp.sum(acc, axis=0, keepdims=True)
        i, j = ga * GROUP + a, gb * GROUP + b
        sums_ref[i, pl.ds(j, 1), :] = row
        if i != j:
            sums_ref[j, pl.ds(i, 1), :] = row


def write_edges(u_ref, first_ref, second_ref, swap_ref):
    odd = lax.axis_index("gx") % 2 == 1
    upper = lax.axis_index("gy") == 1
    for x in range(2):
        low = u_ref[pl.ds(x * YS, YS), :]
        high = u_ref[pl.ds((XS - 2 + x) * YS, YS), :]
        first_ref[pl.ds(x * YS, YS), :] = jnp.where(odd, low, high)
        second_ref[pl.ds(x * YS, YS), :] = jnp.where(odd, high, low)
    for x in range(XS):
        low = u_ref[pl.ds(x * YS, 2), :]
        high = u_ref[pl.ds(x * YS + YS - 2, 2), :]
        swap_ref[pl.ds(2 * x, 2), :] = jnp.where(upper, low, high)


EDGE_SHAPES = (
    jax.ShapeDtypeStruct((2 * YS, ZS), F32),
    jax.ShapeDtypeStruct((2 * YS, ZS), F32),
    jax.ShapeDtypeStruct((2 * XS, ZS), F32),
)


ARRIVAL = [KEEP // GROUP - 1, *range(KEEP // GROUP - 1)]
EARLY = 4
LATE_PAIRS = [
    (ARRIVAL[m], ARRIVAL[n]) for n in range(EARLY, len(ARRIVAL)) for m in range(n + 1)
]


def start_kernel(v_hbm, v_ref, first_ref, second_ref, swap_ref, sums_ref, sems):
    copies = {}
    for g in ARRIVAL:
        part = pl.ds(g * GROUP, GROUP)
        copies[g] = pltpu.make_async_copy(v_hbm.at[part], v_ref.at[part], sems.at[g])
        copies[g].start()
    for n, g in enumerate(ARRIVAL[:EARLY]):
        copies[g].wait()
        if n == 0:
            write_edges(v_ref.at[KEEP - 1], first_ref, second_ref, swap_ref)
        for m in range(n + 1):
            gram_block(v_ref, sums_ref, ARRIVAL[m], g)
    for g in ARRIVAL[EARLY:]:
        copies[g].wait()


def start_call(basis):
    return pl.pallas_call(
        start_kernel,
        in_specs=[pl.BlockSpec(memory_space=pltpu.HBM)],
        out_specs=(VMEM_SPEC,) * 5,
        out_shape=(
            pltpu.VMEM((KEEP, ROWS, ZS), F32),
            *EDGE_SHAPES,
            pltpu.VMEM((KEEP, KEEP, 128), F32),
        ),
        scratch_shapes=[pltpu.SemaphoreType.DMA((KEEP // GROUP,))],
        compiler_params=PARAMS,
        name="start",
    )(pltpu.with_memory_space_constraint(basis, pltpu.HBM))


def gram_kernel(v_ref, early_ref, keep_ref, give_ref, sums_ref, matrix_ref):
    for ga, gb in LATE_PAIRS:
        gram_block(v_ref, sums_ref, ga, gb)
    early = sorted(g * GROUP + a for g in ARRIVAL[:EARLY] for a in range(GROUP))

    def line(i, start):
        part = sums_ref[i, pl.ds(start, HALF), :]
        if i in early:
            sub = iota((HALF, 128), 0) + start
            in_early = (sub < (EARLY - 1) * GROUP) | (sub >= KEEP - GROUP)
            part = jnp.where(in_early, early_ref[i, pl.ds(start, HALF), :], part)
        return part

    sub = iota((HALF, 128), 0)
    lane = iota((HALF, 128), 1)
    packed = jnp.zeros((HALF, 128), F32)
    diagonal = jnp.zeros((HALF, 128), F32)
    for i in range(KEEP):
        part = line(i, 0)
        if i < HALF:
            diagonal = jnp.where(sub == i, part, diagonal)
            part = jnp.where(sub < i, part, line(HALF + i, HALF))
        packed = jnp.where(lane == i, jnp.sum(part, axis=1, keepdims=True), packed)
    packed = jnp.where(lane == KEEP, jnp.sum(diagonal, axis=1, keepdims=True), packed)
    matrix_ref[pl.ds(0, HALF), :] = packed
    packed = matrix_ref[pl.ds(0, PACK), :]
    for p in range(1, HALF // PACK):
        packed = packed + pltpu.roll(matrix_ref[pl.ds(p * PACK, PACK), :], p * PACK_LANES, 1)
    upper = lax.axis_index("gy") == 1
    low, high = packed[:SHARE], packed[SHARE:]
    keep_ref[...] = jnp.where(upper, high, low)
    give_ref[...] = jnp.where(upper, low, high)


def gram_call(v, early):
    return pl.pallas_call(
        gram_kernel,
        in_specs=[VMEM_SPEC, VMEM_SPEC],
        out_specs=(VMEM_SPEC, VMEM_SPEC),
        out_shape=(jax.ShapeDtypeStruct((SHARE, 128), F32),) * 2,
        scratch_shapes=[pltpu.VMEM((KEEP, KEEP, 128), F32), pltpu.VMEM((BASIS, 128), F32)],
        compiler_params=PARAMS,
        name="gram",
    )(v, early)


ALL_PLANES = ((0, XS),)


def dot_all(v_ref, others, x_refs, dots_refs, planes=ALL_PLANES):
    batch = 12 // len(x_refs)
    for dots_ref in dots_refs:
        dots_ref[...] = jnp.zeros((BASIS, 128), F32)

    def run(reads, base):
        def step(c, accs):
            rows = pl.ds(pl.multiple_of(c * CHUNK, CHUNK), CHUNK)
            xs = [x_ref[rows, :] for x_ref in x_refs]
            new = []
            for n, read in enumerate(reads):
                value = read(rows)
                new += [accs[n * len(xs) + m] + fold_tiles(value * x) for m, x in enumerate(xs)]
            return tuple(new)

        zero = jnp.zeros((8, ZS), F32)
        accs = (zero,) * (len(reads) * len(x_refs))
        for first, end in planes:
            accs = lax.fori_loop(first * YS // CHUNK, end * YS // CHUNK, step, accs)
        for n, acc in enumerate(accs):
            row = base + n // len(x_refs)
            dots_refs[n % len(x_refs)][pl.ds(row, 1), :] = fold_row(acc)

    for first in range(0, KEEP, batch):
        run([lambda rows, i=i: v_ref[i, rows, :] for i in range(first, first + batch)], first)
    if others:
        run([lambda rows, r=r: r[rows, :] for r in others], KEEP)
    return [to_row(jnp.sum(dots_ref[...], axis=1, keepdims=True)) for dots_ref in dots_refs]


CENTER = -6.0 - 1.5 * sum(WIND_SPEEDS)
NEAR = [1.0 + 2.0 * s for s in WIND_SPEEDS]
FAR = [-0.5 * s for s in WIND_SPEEDS]


def inner_image(source, swap_ref, reaction_ref, pad_ref, x):
    upper = lax.axis_index("gy").astype(F32)
    lane = iota((YS, ZS), 1)
    mine = source[pl.ds(x * YS, YS), :]
    pad_ref[x, pl.ds(8, YS), :] = mine
    edge = swap_ref[pl.ds(2 * x, 2), :]
    pad_ref[x, pl.ds(6, 2), :] = edge * upper
    pad_ref[x, pl.ds(72, 1), :] = edge[0:1] * (1.0 - upper)
    image = (CENTER - reaction_ref[pl.ds(x * YS, YS), :]) * mine
    for distance, factor in ((1, 1.0), (-1, NEAR[0]), (-2, FAR[0])):
        if 0 <= x + distance < XS:
            image = image + factor * source[pl.ds((x + distance) * YS, YS), :]
    image = (
        image
        + pad_ref[x, pl.ds(9, YS), :]
        + NEAR[1] * pad_ref[x, pl.ds(7, YS), :]
        + FAR[1] * pad_ref[x, pl.ds(6, YS), :]
    )
    return (
        image
        + jnp.where(lane < ZS - 1, pltpu.roll(mine, ZS - 1, 1), 0.0)
        + NEAR[2] * jnp.where(lane >= 1, pltpu.roll(mine, 1, 1), 0.0)
        + FAR[2] * jnp.where(lane >= 2, pltpu.roll(mine, 2, 1), 0.0)
    )


def outer_image(first_ref, second_ref):
    odd = lax.axis_index("gx") % 2 == 1

    def below(rows):
        return jnp.where(odd, first_ref[rows, :], second_ref[rows, :])

    two, one = below(pl.ds(0, YS)), below(pl.ds(YS, YS))
    rows = pl.ds(0, YS)
    above = jnp.where(odd, second_ref[rows, :], first_ref[rows, :])
    return {0: NEAR[0] * one + FAR[0] * two, 1: FAR[0] * one, XS - 1: above}


LAST_SHAPES = (
    jax.ShapeDtypeStruct((1, 128), F32),
    jax.ShapeDtypeStruct((1, 128), F32),
    jax.ShapeDtypeStruct((1,), jnp.int32),
)


def write_for_all(out_ref, rows):
    count = len(rows)
    period = count
    while period % 8:
        period += count
    for tile in range(period // 8):
        sub = iota((8, 128), 0)
        block = jnp.zeros((8, 128), F32)
        for r in range(8):
            block = jnp.where(sub == r, rows[(8 * tile + r) % count], block)
        for p in range(out_ref.shape[0] // period):
            out_ref[pl.ds(p * period + 8 * tile, 8), :] = block


def first_image_kernel(
    v_ref, first_ref, second_ref, swap_ref, reaction_ref, w_ref, out_ref, dots_ref, pad_ref
):
    outer = outer_image(first_ref, second_ref)
    for x in range(XS):
        image = inner_image(v_ref.at[KEEP - 1], swap_ref, reaction_ref, pad_ref, x)
        w_ref[pl.ds(x * YS, YS), :] = image + outer[x] if x in outer else image
    (out_ref[...],) = dot_all(v_ref, [], [w_ref], [dots_ref])


def first_image_call(v, halo, reaction):
    return pl.pallas_call(
        first_image_kernel,
        in_specs=[VMEM_SPEC] * 5,
        out_specs=(VMEM_SPEC, VMEM_SPEC),
        out_shape=(pltpu.VMEM((ROWS, ZS), F32), jax.ShapeDtypeStruct((1, 128), F32)),
        scratch_shapes=[
            pltpu.VMEM((BASIS, 128), F32),
            pltpu.VMEM((XS, YS + 16, ZS), F32),
        ],
        compiler_params=PARAMS,
        name="image_0",
    )(v, *halo, reaction)


def first_payload_kernel(row_ref, keep_ref, got_ref, out_ref):
    gram = keep_ref[...] + got_ref[...]
    row = row_ref[...]
    lane = iota((1, 128), 1)
    free = (lane >= FREE_LANE) & (lane < FREE_LANE + FREE)
    rows = []
    for r in range(SHARE):
        part = jnp.where(free, pltpu.roll(row, FREE_LANE - r * FREE, 1), 0.0)
        rows.append(gram[r : r + 1] + part)
    write_for_all(out_ref, rows)


def first_payload_call(row, keep, got, devices):
    return pl.pallas_call(
        first_payload_kernel,
        in_specs=[VMEM_SPEC] * 3,
        out_specs=VMEM_SPEC,
        out_shape=jax.ShapeDtypeStruct((devices * SHARE, 128), F32),
        compiler_params=PARAMS,
        name="payload_0",
    )(row, keep, got)


def own_kernel(count, *refs):
    v_ref, near_ref, far_ref, *older = refs[: 2 + count]
    u_ref, out_ref, dots_ref = refs[2 + count :]
    odd = lax.axis_index("gx") % 2 == 1
    for x in range(2):
        rows = pl.ds(x * YS, YS)
        near, far = near_ref[rows, :], far_ref[rows, :]
        u_ref[pl.ds(x * YS, YS), :] = jnp.where(odd, near, far)
        u_ref[pl.ds((2 + x) * YS, YS), :] = jnp.where(odd, far, near)
    (out_ref[...],) = dot_all(v_ref, [*older, u_ref], [u_ref], [dots_ref])


def own_call(v, near, far, older):
    count = 1 + len(older)
    return pl.pallas_call(
        functools.partial(own_kernel, count),
        in_specs=[VMEM_SPEC] * (2 + count),
        out_specs=(VMEM_SPEC,) * 2,
        out_shape=(pltpu.VMEM((ROWS, ZS), F32), jax.ShapeDtypeStruct((1, 128), F32)),
        scratch_shapes=[pltpu.VMEM((BASIS, 128), F32)],
        compiler_params=PARAMS,
    )(v, near, far, *older)


def inner_kernel(count, *refs):
    v_ref, *others = refs[: 1 + count]
    swap_ref, reaction_ref, own_ref, w_ref, out_ref, dots_ref, pad_ref = refs[1 + count :]
    for x in range(XS):
        w_ref[pl.ds(x * YS, YS), :] = inner_image(others[-1], swap_ref, reaction_ref, pad_ref, x)
    (row,) = dot_all(v_ref, others, [w_ref], [dots_ref])
    out_ref[...] = row + pltpu.roll(own_ref[...], OWN_LANE, 1)


def inner_call(v, created, swap, reaction, own):
    count = len(created)
    return pl.pallas_call(
        functools.partial(inner_kernel, count),
        in_specs=[VMEM_SPEC] * (4 + count),
        out_specs=(VMEM_SPEC,) * 2,
        out_shape=(pltpu.VMEM((ROWS, ZS), F32), jax.ShapeDtypeStruct((1, 128), F32)),
        scratch_shapes=[
            pltpu.VMEM((BASIS, 128), F32),
            pltpu.VMEM((XS, YS + 16, ZS), F32),
        ],
        compiler_params=PARAMS,
    )(v, *created, swap, reaction, own)


def outer_kernel(count, *refs):
    v_ref, *others = refs[: 1 + count]
    first_ref, second_ref, inner_ref, extra_ref = refs[1 + count : 5 + count]
    w_ref, out_ref, dots_ref, delta_ref = refs[5 + count :]
    outer = outer_image(first_ref, second_ref)
    for x in range(XS):
        rows = pl.ds(x * YS, YS)
        image = inner_ref[rows, :]
        if x in outer:
            delta_ref[rows, :] = outer[x]
            image = image + outer[x]
        w_ref[rows, :] = image
    (row,) = dot_all(v_ref, others, [delta_ref], [dots_ref], ((0, 2), (3, 4)))
    row = row + extra_ref[...]
    if count == STEPS - 1:
        square = jnp.zeros((8, ZS), F32)
        for c in range(ROWS // CHUNK):
            image = w_ref[pl.ds(c * CHUNK, CHUNK), :]
            square = square + fold_tiles(image * image)
        square = jnp.sum(fold_row(square), axis=1, keepdims=True)
        row = jnp.where(iota((1, 128), 1) == BASIS - 1, square, row)
    write_for_all(out_ref, [row])


def outer_call(v, created, first, second, inner, extra, devices):
    count = len(created)
    return pl.pallas_call(
        functools.partial(outer_kernel, count),
        in_specs=[VMEM_SPEC] * (5 + count),
        out_specs=(VMEM_SPEC, VMEM_SPEC),
        out_shape=(
            pltpu.VMEM((ROWS, ZS), F32),
            jax.ShapeDtypeStruct((devices, 128), F32),
        ),
        scratch_shapes=[pltpu.VMEM((BASIS, 128), F32), pltpu.VMEM((ROWS, ZS), F32)],
        compiler_params=PARAMS,
    )(v, *created, first, second, inner, extra)


STATE_G, STATE_H, STATE_D, STATE_ROWS = 0, BASIS, 2 * BASIS, 2 * BASIS + 8


def summed_rows(recv_ref, count):
    period = count
    while period % 8:
        period += count
    total = jnp.sum(recv_ref[...].reshape(-1, period, 128), axis=0)
    if count in (1, 2):
        while count < 8:
            total = total + pltpu.roll(total, 8 - count, 0)
            count *= 2
        return total
    return sum(total[p : p + count] for p in range(0, period, count))


def unpacked_gram(packed, pack_ref):
    pack_ref[...] = jnp.zeros((128, 128), F32)
    for p in range(HALF // PACK):
        part = packed
        if p:
            part = pltpu.roll(part, 128 - p * PACK_LANES, 1)
        pack_ref[pl.ds(p * PACK, PACK), :] = part
    turned = jnp.transpose(pack_ref[...])
    plain = pack_ref[pl.ds(0, HALF), :]
    lane = iota((HALF, 128), 1)
    sub = iota((HALF, 128), 0)
    diagonal = jnp.sum(jnp.where(lane == KEEP, plain, 0.0), axis=1, keepdims=True)
    top = jnp.where((lane > sub) | (lane >= HALF), plain, turned[:HALF])
    top = jnp.where(lane == sub, diagonal, top)
    last = jnp.where(lane <= sub, plain, turned[:HALF])
    pack_ref[...] = turned
    bottom = jnp.where(lane < HALF, pack_ref[pl.ds(HALF, HALF), :], pltpu.roll(last, HALF, 1))
    pack_ref[pl.ds(0, HALF), :] = jnp.where(lane < KEEP, top, 0.0)
    pack_ref[pl.ds(HALF, HALF), :] = jnp.where(lane < KEEP, bottom, 0.0)
    pack_ref[pl.ds(KEEP, STEPS), :] = jnp.zeros((STEPS, 128), F32)


def solve_weights(count, cells, recv_ref, state_in, state_ref, weight_ref, pack_ref):
    lane = iota((1, 128), 1)
    lanes = iota((BASIS, 128), 1)
    subs = iota((BASIS, 128), 0)
    sub = iota((BASIS, 1), 0)
    scale = 1.0 / cells

    def spread(values):
        return jnp.sum(values, axis=1, keepdims=True)

    if count == 0:
        half = recv_ref.shape[0] // 2
        low = summed_rows(recv_ref.at[pl.ds(0, half)], SHARE) * scale
        high = summed_rows(recv_ref.at[pl.ds(half, half)], SHARE) * scale
        pack_ref[pl.ds(0, SHARE), :] = low
        pack_ref[pl.ds(SHARE, SHARE), :] = high
        total = low + high
        unpacked_gram(pack_ref[pl.ds(0, PACK), :], pack_ref)
        gram = pack_ref[pl.ds(0, BASIS), :]
        hess = jnp.zeros((BASIS, 128), F32)
        inverse_row = jnp.where(lane < KEEP, 1.0, 0.0)
        inverse_column = jnp.where(sub < KEEP, 1.0, 0.0)
        first_row = jnp.zeros((1, 128), F32)
        for r in range(SHARE):
            part = pltpu.roll(total[r : r + 1], 128 - FREE_LANE + r * FREE, 1)
            mine = (lane >= r * FREE) & (lane < (r + 1) * FREE)
            first_row = jnp.where(mine, part, first_row)
        inverse = jnp.ones((1, 1), F32)
        image_square = None
        first = to_column(first_row)
        folded = spread(gram * first_row)
    else:
        total = summed_rows(recv_ref, 1)[0:1] * scale
        newest = KEEP + count - 1
        raw_first = total
        raw_gram = pltpu.roll(total, 128 - OWN_LANE, 1)
        inverse_row = state_in[pl.ds(STATE_D, 1), :]
        gram = state_in[pl.ds(STATE_G, BASIS), :]
        hess = state_in[pl.ds(STATE_H, BASIS), :]
        part_first, part_gram = raw_first * inverse_row, raw_gram * inverse_row
        square = spread(jnp.where(lane == newest, raw_gram, 0.0))
        first_newest = spread(jnp.where(lane == newest, raw_first, 0.0))
        image_square = spread(jnp.where(lane == BASIS - 1, raw_first, 0.0))
        crossed = spread(part_gram * part_first)
        first_column, gram_column = to_column(part_first), to_column(part_gram)
        inverse_column = to_column(inverse_row)
        folded = spread(gram * part_first)
        norm = jnp.sqrt(square + EPSILON)
        inverse = 1.0 / norm
        own = square * inverse * inverse
        first_newest = first_newest * inverse * inverse
        image_square = image_square * inverse * inverse
        mine = sub == newest
        first = jnp.where(mine, first_newest, first_column * inverse)
        gram_column = gram_column * inverse
        folded = jnp.where(
            mine,
            crossed * inverse * inverse + own * first_newest,
            folded * inverse + gram_column * first_newest,
        )
        gram = jnp.where(lanes == newest, gram_column, gram)
        gram = jnp.where(subs == newest, part_gram * inverse, gram)
        gram = jnp.where((lanes == newest) & (subs == newest), own, gram)
        hess = jnp.where((subs == newest) & (lanes == count - 1), norm, hess)
        inverse_row = jnp.where(lane == newest, inverse, inverse_row)
        inverse_column = jnp.where(mine, inverse, inverse_column)
    weights = first + (first - folded)
    weight_ref[pl.ds(0, BASIS), :] = jnp.broadcast_to(weights * inverse_column, (BASIS, ZS))
    weight_ref[pl.ds(BASIS, 8), :] = jnp.broadcast_to(inverse, (8, ZS))
    hess = jnp.where((lanes == count) & (subs < KEEP + count), weights, hess)
    state_ref[pl.ds(STATE_G, BASIS), :] = gram
    state_ref[pl.ds(STATE_H, BASIS), :] = hess
    state_ref[pl.ds(STATE_D, 8), :] = jnp.broadcast_to(inverse_row, (8, 128))
    return weights, first, gram, image_square


def combined(rows, weight_ref, w_ref, v_ref, others):
    value = w_ref[rows, :] * weight_ref[pl.ds(BASIS, 1), :]
    for i in range(KEEP):
        value = value - weight_ref[pl.ds(i, 1), :] * v_ref[i, rows, :]
    for i, other in enumerate(others):
        value = value - weight_ref[pl.ds(KEEP + i, 1), :] * other[rows, :]
    return value


def combine_half(out_ref, high, weight_ref, w_ref, v_ref, others):
    start = high.astype(jnp.int32) * (ROWS // 2)

    def step(c, carry):
        rows = pl.ds(pl.multiple_of(start + c * CHUNK, CHUNK), CHUNK)
        out_ref[pl.ds(pl.multiple_of(c * CHUNK, CHUNK), CHUNK), :] = combined(
            rows, weight_ref, w_ref, v_ref, others
        )
        return carry

    lax.fori_loop(0, ROWS // 2 // CHUNK, step, 0)


HALF_SHAPE = jax.ShapeDtypeStruct((ROWS // 2, ZS), F32)
WEIGHT_SHAPE = (BASIS + 8, ZS)


def far_kernel(count, cells, *refs):
    recv_ref, w_ref, v_ref, *others = refs[: 3 + count]
    *states, far_ref, weight_ref, state_ref, pack_ref = refs[3 + count :]
    state_in = states[0] if states else None
    solve_weights(count, cells, recv_ref, state_in, state_ref, weight_ref, pack_ref)
    odd = lax.axis_index("gx") % 2 == 1
    combine_half(far_ref, odd, weight_ref, w_ref, v_ref, others)


def far_call(recv, w, v, created, state, cells):
    count = len(created)
    states = [state] if created else []
    return pl.pallas_call(
        functools.partial(far_kernel, count, cells),
        in_specs=[VMEM_SPEC] * (3 + count + len(states)),
        out_specs=(VMEM_SPEC,) * 3,
        out_shape=(
            HALF_SHAPE,
            pltpu.VMEM(WEIGHT_SHAPE, F32),
            jax.ShapeDtypeStruct((STATE_ROWS, 128), F32),
        ),
        scratch_shapes=[pltpu.VMEM((128, 128), F32)],
        compiler_params=PARAMS,
    )(recv, w, v, *created, *states)


def near_kernel(count, *refs):
    weight_ref, far_ref, w_ref, v_ref, *others = refs[: 4 + count]
    near_ref, swap_ref = refs[4 + count :]
    odd = lax.axis_index("gx") % 2 == 1
    upper = lax.axis_index("gy") == 1
    combine_half(near_ref, jnp.logical_not(odd), weight_ref, w_ref, v_ref, others)
    for x in range(XS):
        sides = []
        for y in (0, YS - 2):
            rows = pl.ds((x % 2) * YS + y, 2)
            low, high = (near_ref, far_ref) if x < 2 else (far_ref, near_ref)
            sides.append(jnp.where(odd, low[rows, :], high[rows, :]))
        swap_ref[pl.ds(2 * x, 2), :] = jnp.where(upper, *sides)


def near_call(weight, far, w, v, created):
    count = len(created)
    return pl.pallas_call(
        functools.partial(near_kernel, count),
        in_specs=[VMEM_SPEC] * (4 + count),
        out_specs=(VMEM_SPEC,) * 2,
        out_shape=(HALF_SHAPE, jax.ShapeDtypeStruct((2 * XS, ZS), F32)),
        compiler_params=PARAMS,
    )(weight, far, w, v, *created)


def last_kernel(cells, *refs):
    count = STEPS - 1
    recv_ref, w_ref, v_ref, *others = refs[: 3 + count]
    state_in, u_ref, state_ref, square_ref, guess_ref, sound_ref, weight_ref = refs[3 + count :]
    weights, first, gram, image_square = solve_weights(
        count, cells, recv_ref, state_in, state_ref, weight_ref, None
    )
    again = jnp.sum(gram * to_row(weights), axis=1, keepdims=True)
    guess = image_square - jnp.sum(weights * (2.0 * first - again), axis=0, keepdims=True)
    guess_ref[...] = jnp.where(iota((1, 128), 1) == 0, guess, 0.0)
    sound = jnp.where(guess > SOUND_SHARE * image_square, 1, 0)
    sound_ref[0] = sound[0, 0]

    def step(c, acc):
        rows = pl.ds(pl.multiple_of(c * BLOCK, BLOCK), BLOCK)
        value = combined(rows, weight_ref, w_ref, v_ref, others)
        u_ref[rows, :] = value
        return acc + fold_tiles(value * value)

    acc = lax.fori_loop(0, ROWS // BLOCK, step, jnp.zeros((8, ZS), F32))
    square_ref[...] = fold_row(acc)


def last_call(recv, w, v, created, state, cells):
    return pl.pallas_call(
        functools.partial(last_kernel, cells),
        in_specs=[VMEM_SPEC] * (4 + len(created)),
        out_specs=(VMEM_SPEC,) * 4 + (SMEM_SPEC,),
        out_shape=(
            pltpu.VMEM((ROWS, ZS), F32),
            jax.ShapeDtypeStruct((STATE_ROWS, 128), F32),
            *LAST_SHAPES,
        ),
        scratch_shapes=[pltpu.VMEM(WEIGHT_SHAPE, F32)],
        compiler_params=PARAMS,
        name="last",
    )(recv, w, v, *created, state)


def finish_kernel(*refs):
    square_ref, state_ref, *created = refs[: 2 + STEPS]
    new_ref, hess_ref = refs[2 + STEPS :]
    lane = iota((1, 128), 1)
    norm = jnp.sqrt(jnp.sum(square_ref[...], axis=1, keepdims=True) + EPSILON)
    lanes = iota((BASIS, 128), 1)
    subs = iota((BASIS, 128), 0)
    hess = state_ref[pl.ds(STATE_H, BASIS), :]
    hess = jnp.where((subs == BASIS - 1) & (lanes == STEPS - 1), norm, hess)
    hess_ref[...] = jnp.transpose(jnp.concatenate([hess, jnp.zeros((128 - BASIS, 128), F32)], axis=0))[:STEPS, :BASIS]
    inverse_row = state_ref[pl.ds(STATE_D, 1), :]
    for j, u_ref in enumerate(created):
        if j == STEPS - 1:
            inverse = 1.0 / norm
        else:
            inverse = jnp.sum(jnp.where(lane == KEEP + j, inverse_row, 0.0), axis=1, keepdims=True)
        for c in range(ROWS // CHUNK):
            rows = pl.ds(c * CHUNK, CHUNK)
            new_ref[j, rows, :] = u_ref[rows, :] * inverse


def finish_call(square, state, created):
    return pl.pallas_call(
        finish_kernel,
        in_specs=[VMEM_SPEC] * (2 + STEPS),
        out_specs=(VMEM_SPEC, VMEM_SPEC),
        out_shape=(
            jax.ShapeDtypeStruct((STEPS, ROWS, ZS), F32),
            jax.ShapeDtypeStruct((STEPS, BASIS), F32),
        ),
        compiler_params=PARAMS,
        name="finish",
    )(square, state, *created)


def paired(half, start):
    lower = range(start, lax.axis_size("gx") - 1, 2)
    return lax.ppermute(half, "gx", [(i, i + 1) for i in lower] + [(i + 1, i) for i in lower])


def across(edge):
    return lax.ppermute(edge, "gy", [(0, 1), (1, 0)])


def from_all(payload):
    axes = ("gy", "gx")
    devices = lax.axis_size(axes)
    copies = payload.reshape(devices, 1, -1)
    got = lax.all_to_all(copies, axes, split_axis=0, concat_axis=0, tiled=True)
    return got.reshape(-1, 128)


def body(basis_vectors, reaction):
    devices = lax.axis_size(("gy", "gx"))
    cells = float(ROWS * ZS * devices)
    basis = basis_vectors.reshape(KEEP, ROWS, ZS)
    v, near, far, swap, early = start_call(basis)
    second = paired(far, 1)
    first = paired(near, 0)
    swap = across(swap)
    reaction = reaction.reshape(ROWS, ZS)
    keep, give = gram_call(v, early)
    got = across(give)
    w, row = first_image_call(v, (first, second, swap), reaction)
    payload = first_payload_call(row, keep, got, devices)
    created = []
    state = None
    for _ in range(1, STEPS):
        recv = from_all(payload)
        far, weight, state = far_call(recv, w, v, created, state, cells)
        second = paired(far, 1)
        near, swap = near_call(weight, far, w, v, created)
        first = paired(near, 0)
        swap = across(swap)
        u, own = own_call(v, near, far, created)
        created.append(u)
        inner, extra = inner_call(v, created, swap, reaction, own)
        w, payload = outer_call(v, created, first, second, inner, extra, devices)
    u, state, square, guess, sound = last_call(from_all(payload), w, v, created, state, cells)
    created.append(u)
    square = lax.cond(
        sound[0] == 1,
        lambda guess, square: guess,
        lambda guess, square: jnp.sum(from_all(square), axis=0, keepdims=True) * (1.0 / cells),
        guess,
        jnp.broadcast_to(square, (devices, 128)),
    )
    new, hessenberg = finish_call(square, state, created)
    return new.reshape(STEPS, XS, YS, ZS), hessenberg.T


def solution(mesh):
    return jax.shard_map(
        body,
        mesh=mesh,
        in_specs=(P(None, "gx", "gy", None), P("gx", "gy", None)),
        out_specs=(P(None, "gx", "gy", None), P()),
        check_vma=False,
    )
```

```python
import functools

import jax
import jax.numpy as jnp
from jax import lax
from jax.experimental import pallas as pl
from jax.experimental.pallas import tpu as pltpu
from jax.sharding import PartitionSpec as P


KEEP = 36
STEPS = 4
BASIS = KEEP + STEPS
WIND_SPEEDS = (0.9, 0.6, 0.4)
EPSILON = 1e-06
F32 = jnp.float32

XS, YS, ZS = 4, 64, 256
ROWS = XS * YS
GROUP = 4
GRAM_ROWS = 64
HALF = KEEP // 2
PACK = 6
PACK_LANES = 38
FREE_LANE = 113
SHARE = PACK // 2
FREE = KEEP // SHARE
OWN_LANE = 64
CHUNK = 32
BLOCK = 64
SOUND_SHARE = 0.05

PARAMS = pltpu.CompilerParams(vmem_limit_bytes=16 * 2**20)
SMEM_SPEC = pl.BlockSpec(memory_space=pltpu.SMEM)
HBM_SPEC = pl.BlockSpec(memory_space=pltpu.HBM)
VMEM_SPEC = pl.BlockSpec(memory_space=pltpu.VMEM)


def iota(shape, axis):
    return lax.broadcasted_iota(jnp.int32, shape, axis)


def to_column(row):
    pick = iota((BASIS, 128), 0) == iota((BASIS, 128), 1)
    return jnp.sum(jnp.where(pick, row, 0.0), axis=1, keepdims=True)


def to_row(column):
    pick = iota((BASIS, 128), 0) == iota((BASIS, 128), 1)
    return jnp.sum(jnp.where(pick, column, 0.0), axis=0, keepdims=True)


def fold_tiles(block):
    return jnp.sum(block.reshape(-1, 8, ZS), axis=0)


def fold_row(acc):
    return jnp.sum(acc[:, :128] + acc[:, 128:], axis=0, keepdims=True)


def gram_block(v_ref, sums_ref, ga, gb):
    pairs = [(a, b) for a in range(GROUP) for b in range(GROUP) if ga != gb or a <= b]

    def step(t, accs):
        accs = list(accs)
        for part in range(GRAM_ROWS // 8):
            rows = pl.ds(pl.multiple_of(t * GRAM_ROWS, GRAM_ROWS) + 8 * part, 8)
            for half in range(2):
                lanes = pl.ds(half * 128, 128)
                left = [v_ref[ga * GROUP + a, rows, lanes] for a in range(GROUP)]
                right = left
                if ga != gb:
                    right = [v_ref[gb * GROUP + b, rows, lanes] for b in range(GROUP)]
                for n, (a, b) in enumerate(pairs):
                    accs[n] = accs[n] + left[a] * right[b]
        return tuple(accs)

    zero = jnp.zeros((8, 128), F32)
    accs = lax.fori_loop(0, ROWS // GRAM_ROWS, step, tuple(zero for _ in pairs))
    for (a, b), acc in zip(pairs, accs):
        row = jnp.sum(acc, axis=0, keepdims=True)
        i, j = ga * GROUP + a, gb * GROUP + b
        sums_ref[i, pl.ds(j, 1), :] = row
        if i != j:
            sums_ref[j, pl.ds(i, 1), :] = row


def write_edges(u_ref, first_ref, second_ref, swap_ref):
    odd = lax.axis_index("gx") % 2 == 1
    upper = lax.axis_index("gy") == 1
    for x in range(2):
        low = u_ref[pl.ds(x * YS, YS), :]
        high = u_ref[pl.ds((XS - 2 + x) * YS, YS), :]
        first_ref[pl.ds(x * YS, YS), :] = jnp.where(odd, low, high)
        second_ref[pl.ds(x * YS, YS), :] = jnp.where(odd, high, low)
    for x in range(XS):
        low = u_ref[pl.ds(x * YS, 2), :]
        high = u_ref[pl.ds(x * YS + YS - 2, 2), :]
        swap_ref[pl.ds(2 * x, 2), :] = jnp.where(upper, low, high)


EDGE_SHAPES = (
    jax.ShapeDtypeStruct((2 * YS, ZS), F32),
    jax.ShapeDtypeStruct((2 * YS, ZS), F32),
    jax.ShapeDtypeStruct((2 * XS, ZS), F32),
)


ARRIVAL = [KEEP // GROUP - 1, *range(KEEP // GROUP - 1)]
EARLY = 4
LATE_PAIRS = [
    (ARRIVAL[m], ARRIVAL[n]) for n in range(EARLY, len(ARRIVAL)) for m in range(n + 1)
]


def start_kernel(v_hbm, v_ref, first_ref, second_ref, swap_ref, sums_ref, sems):
    copies = {}
    for g in ARRIVAL:
        part = pl.ds(g * GROUP, GROUP)
        copies[g] = pltpu.make_async_copy(v_hbm.at[part], v_ref.at[part], sems.at[g])
        copies[g].start()
    for n, g in enumerate(ARRIVAL[:EARLY]):
        copies[g].wait()
        if n == 0:
            write_edges(v_ref.at[KEEP - 1], first_ref, second_ref, swap_ref)
        for m in range(n + 1):
            gram_block(v_ref, sums_ref, ARRIVAL[m], g)
    for g in ARRIVAL[EARLY:]:
        copies[g].wait()


def start_call(basis):
    return pl.pallas_call(
        start_kernel,
        in_specs=[pl.BlockSpec(memory_space=pltpu.HBM)],
        out_specs=(VMEM_SPEC,) * 5,
        out_shape=(
            pltpu.VMEM((KEEP, ROWS, ZS), F32),
            *EDGE_SHAPES,
            pltpu.VMEM((KEEP, KEEP, 128), F32),
        ),
        scratch_shapes=[pltpu.SemaphoreType.DMA((KEEP // GROUP,))],
        compiler_params=PARAMS,
        name="start",
    )(pltpu.with_memory_space_constraint(basis, pltpu.HBM))


def gram_kernel(v_ref, early_ref, keep_ref, give_ref, sums_ref, matrix_ref):
    for ga, gb in LATE_PAIRS:
        gram_block(v_ref, sums_ref, ga, gb)
    early = sorted(g * GROUP + a for g in ARRIVAL[:EARLY] for a in range(GROUP))

    def line(i, start):
        part = sums_ref[i, pl.ds(start, HALF), :]
        if i in early:
            sub = iota((HALF, 128), 0) + start
            in_early = (sub < (EARLY - 1) * GROUP) | (sub >= KEEP - GROUP)
            part = jnp.where(in_early, early_ref[i, pl.ds(start, HALF), :], part)
        return part

    sub = iota((HALF, 128), 0)
    lane = iota((HALF, 128), 1)
    packed = jnp.zeros((HALF, 128), F32)
    diagonal = jnp.zeros((HALF, 128), F32)
    for i in range(KEEP):
        part = line(i, 0)
        if i < HALF:
            diagonal = jnp.where(sub == i, part, diagonal)
            part = jnp.where(sub < i, part, line(HALF + i, HALF))
        packed = jnp.where(lane == i, jnp.sum(part, axis=1, keepdims=True), packed)
    packed = jnp.where(lane == KEEP, jnp.sum(diagonal, axis=1, keepdims=True), packed)
    matrix_ref[pl.ds(0, HALF), :] = packed
    packed = matrix_ref[pl.ds(0, PACK), :]
    for p in range(1, HALF // PACK):
        packed = packed + pltpu.roll(matrix_ref[pl.ds(p * PACK, PACK), :], p * PACK_LANES, 1)
    upper = lax.axis_index("gy") == 1
    low, high = packed[:SHARE], packed[SHARE:]
    keep_ref[...] = jnp.where(upper, high, low)
    give_ref[...] = jnp.where(upper, low, high)


def gram_call(v, early):
    return pl.pallas_call(
        gram_kernel,
        in_specs=[VMEM_SPEC, VMEM_SPEC],
        out_specs=(VMEM_SPEC, VMEM_SPEC),
        out_shape=(jax.ShapeDtypeStruct((SHARE, 128), F32),) * 2,
        scratch_shapes=[pltpu.VMEM((KEEP, KEEP, 128), F32), pltpu.VMEM((BASIS, 128), F32)],
        compiler_params=PARAMS,
        name="gram",
    )(v, early)


ALL_PLANES = ((0, XS),)


def dot_all(v_ref, others, x_refs, dots_refs, planes=ALL_PLANES):
    batch = 12 // len(x_refs)
    for dots_ref in dots_refs:
        dots_ref[...] = jnp.zeros((BASIS, 128), F32)

    def run(reads, base):
        def step(c, accs):
            rows = pl.ds(pl.multiple_of(c * CHUNK, CHUNK), CHUNK)
            xs = [x_ref[rows, :] for x_ref in x_refs]
            new = []
            for n, read in enumerate(reads):
                value = read(rows)
                new += [accs[n * len(xs) + m] + fold_tiles(value * x) for m, x in enumerate(xs)]
            return tuple(new)

        zero = jnp.zeros((8, ZS), F32)
        accs = (zero,) * (len(reads) * len(x_refs))
        for first, end in planes:
            accs = lax.fori_loop(first * YS // CHUNK, end * YS // CHUNK, step, accs)
        for n, acc in enumerate(accs):
            row = base + n // len(x_refs)
            dots_refs[n % len(x_refs)][pl.ds(row, 1), :] = fold_row(acc)

    for first in range(0, KEEP, batch):
        run([lambda rows, i=i: v_ref[i, rows, :] for i in range(first, first + batch)], first)
    if others:
        run([lambda rows, r=r: r[rows, :] for r in others], KEEP)
    return [to_row(jnp.sum(dots_ref[...], axis=1, keepdims=True)) for dots_ref in dots_refs]


CENTER = -6.0 - 1.5 * sum(WIND_SPEEDS)
NEAR = [1.0 + 2.0 * s for s in WIND_SPEEDS]
FAR = [-0.5 * s for s in WIND_SPEEDS]


def inner_image(source, swap_ref, reaction_ref, pad_ref, x):
    upper = lax.axis_index("gy").astype(F32)
    lane = iota((YS, ZS), 1)
    mine = source[pl.ds(x * YS, YS), :]
    pad_ref[x, pl.ds(8, YS), :] = mine
    edge = swap_ref[pl.ds(2 * x, 2), :]
    pad_ref[x, pl.ds(6, 2), :] = edge * upper
    pad_ref[x, pl.ds(72, 1), :] = edge[0:1] * (1.0 - upper)
    image = (CENTER - reaction_ref[pl.ds(x * YS, YS), :]) * mine
    for distance, factor in ((1, 1.0), (-1, NEAR[0]), (-2, FAR[0])):
        if 0 <= x + distance < XS:
            image = image + factor * source[pl.ds((x + distance) * YS, YS), :]
    image = (
        image
        + pad_ref[x, pl.ds(9, YS), :]
        + NEAR[1] * pad_ref[x, pl.ds(7, YS), :]
        + FAR[1] * pad_ref[x, pl.ds(6, YS), :]
    )
    return (
        image
        + jnp.where(lane < ZS - 1, pltpu.roll(mine, ZS - 1, 1), 0.0)
        + NEAR[2] * jnp.where(lane >= 1, pltpu.roll(mine, 1, 1), 0.0)
        + FAR[2] * jnp.where(lane >= 2, pltpu.roll(mine, 2, 1), 0.0)
    )


def outer_image(first_ref, second_ref):
    odd = lax.axis_index("gx") % 2 == 1

    def below(rows):
        return jnp.where(odd, first_ref[rows, :], second_ref[rows, :])

    two, one = below(pl.ds(0, YS)), below(pl.ds(YS, YS))
    rows = pl.ds(0, YS)
    above = jnp.where(odd, second_ref[rows, :], first_ref[rows, :])
    return {0: NEAR[0] * one + FAR[0] * two, 1: FAR[0] * one, XS - 1: above}


LAST_SHAPES = (
    jax.ShapeDtypeStruct((1, 128), F32),
    jax.ShapeDtypeStruct((1, 128), F32),
    jax.ShapeDtypeStruct((1,), jnp.int32),
)


def write_for_all(out_ref, rows):
    count = len(rows)
    period = count
    while period % 8:
        period += count
    for tile in range(period // 8):
        sub = iota((8, 128), 0)
        block = jnp.zeros((8, 128), F32)
        for r in range(8):
            block = jnp.where(sub == r, rows[(8 * tile + r) % count], block)
        for p in range(out_ref.shape[0] // period):
            out_ref[pl.ds(p * period + 8 * tile, 8), :] = block


def first_image_kernel(
    v_ref, first_ref, second_ref, swap_ref, reaction_ref, w_ref, out_ref, dots_ref, pad_ref
):
    outer = outer_image(first_ref, second_ref)
    for x in range(XS):
        image = inner_image(v_ref.at[KEEP - 1], swap_ref, reaction_ref, pad_ref, x)
        w_ref[pl.ds(x * YS, YS), :] = image + outer[x] if x in outer else image
    (out_ref[...],) = dot_all(v_ref, [], [w_ref], [dots_ref])


def first_image_call(v, halo, reaction):
    return pl.pallas_call(
        first_image_kernel,
        in_specs=[VMEM_SPEC] * 5,
        out_specs=(VMEM_SPEC, VMEM_SPEC),
        out_shape=(pltpu.VMEM((ROWS, ZS), F32), jax.ShapeDtypeStruct((1, 128), F32)),
        scratch_shapes=[
            pltpu.VMEM((BASIS, 128), F32),
            pltpu.VMEM((XS, YS + 16, ZS), F32),
        ],
        compiler_params=PARAMS,
        name="image_0",
    )(v, *halo, reaction)


def first_payload_kernel(row_ref, keep_ref, got_ref, out_ref):
    gram = keep_ref[...] + got_ref[...]
    row = row_ref[...]
    lane = iota((1, 128), 1)
    free = (lane >= FREE_LANE) & (lane < FREE_LANE + FREE)
    rows = []
    for r in range(SHARE):
        part = jnp.where(free, pltpu.roll(row, FREE_LANE - r * FREE, 1), 0.0)
        rows.append(gram[r : r + 1] + part)
    write_for_all(out_ref, rows)


def first_payload_call(row, keep, got, devices):
    return pl.pallas_call(
        first_payload_kernel,
        in_specs=[VMEM_SPEC] * 3,
        out_specs=VMEM_SPEC,
        out_shape=jax.ShapeDtypeStruct((devices * SHARE, 128), F32),
        compiler_params=PARAMS,
        name="payload_0",
    )(row, keep, got)


def own_kernel(count, *refs):
    v_ref, near_ref, far_ref, *older = refs[: 2 + count]
    u_ref, out_ref, dots_ref = refs[2 + count :]
    odd = lax.axis_index("gx") % 2 == 1
    for x in range(2):
        rows = pl.ds(x * YS, YS)
        near, far = near_ref[rows, :], far_ref[rows, :]
        u_ref[pl.ds(x * YS, YS), :] = jnp.where(odd, near, far)
        u_ref[pl.ds((2 + x) * YS, YS), :] = jnp.where(odd, far, near)
    (out_ref[...],) = dot_all(v_ref, [*older, u_ref], [u_ref], [dots_ref])


def own_call(v, near, far, older):
    count = 1 + len(older)
    return pl.pallas_call(
        functools.partial(own_kernel, count),
        in_specs=[VMEM_SPEC] * (2 + count),
        out_specs=(VMEM_SPEC,) * 2,
        out_shape=(pltpu.VMEM((ROWS, ZS), F32), jax.ShapeDtypeStruct((1, 128), F32)),
        scratch_shapes=[pltpu.VMEM((BASIS, 128), F32)],
        compiler_params=PARAMS,
    )(v, near, far, *older)


def inner_kernel(count, *refs):
    v_ref, *others = refs[: 1 + count]
    swap_ref, reaction_ref, own_ref, w_ref, out_ref, dots_ref, pad_ref = refs[1 + count :]
    for x in range(XS):
        w_ref[pl.ds(x * YS, YS), :] = inner_image(others[-1], swap_ref, reaction_ref, pad_ref, x)
    (row,) = dot_all(v_ref, others, [w_ref], [dots_ref])
    out_ref[...] = row + pltpu.roll(own_ref[...], OWN_LANE, 1)


def inner_call(v, created, swap, reaction, own):
    count = len(created)
    return pl.pallas_call(
        functools.partial(inner_kernel, count),
        in_specs=[VMEM_SPEC] * (4 + count),
        out_specs=(VMEM_SPEC,) * 2,
        out_shape=(pltpu.VMEM((ROWS, ZS), F32), jax.ShapeDtypeStruct((1, 128), F32)),
        scratch_shapes=[
            pltpu.VMEM((BASIS, 128), F32),
            pltpu.VMEM((XS, YS + 16, ZS), F32),
        ],
        compiler_params=PARAMS,
    )(v, *created, swap, reaction, own)


def outer_kernel(count, *refs):
    v_ref, *others = refs[: 1 + count]
    first_ref, second_ref, inner_ref, extra_ref = refs[1 + count : 5 + count]
    w_ref, out_ref, dots_ref, delta_ref = refs[5 + count :]
    outer = outer_image(first_ref, second_ref)
    for x in range(XS):
        rows = pl.ds(x * YS, YS)
        image = inner_ref[rows, :]
        if x in outer:
            delta_ref[rows, :] = outer[x]
            image = image + outer[x]
        w_ref[rows, :] = image
    (row,) = dot_all(v_ref, others, [delta_ref], [dots_ref], ((0, 2), (3, 4)))
    row = row + extra_ref[...]
    if count == STEPS - 1:
        square = jnp.zeros((8, ZS), F32)
        for c in range(ROWS // CHUNK):
            image = w_ref[pl.ds(c * CHUNK, CHUNK), :]
            square = square + fold_tiles(image * image)
        square = jnp.sum(fold_row(square), axis=1, keepdims=True)
        row = jnp.where(iota((1, 128), 1) == BASIS - 1, square, row)
    write_for_all(out_ref, [row])


def outer_call(v, created, first, second, inner, extra, devices):
    count = len(created)
    return pl.pallas_call(
        functools.partial(outer_kernel, count),
        in_specs=[VMEM_SPEC] * (5 + count),
        out_specs=(VMEM_SPEC, VMEM_SPEC),
        out_shape=(
            pltpu.VMEM((ROWS, ZS), F32),
            jax.ShapeDtypeStruct((devices, 128), F32),
        ),
        scratch_shapes=[pltpu.VMEM((BASIS, 128), F32), pltpu.VMEM((ROWS, ZS), F32)],
        compiler_params=PARAMS,
    )(v, *created, first, second, inner, extra)


STATE_G, STATE_H, STATE_D, STATE_ROWS = 0, BASIS, 2 * BASIS, 2 * BASIS + 8


def summed_rows(recv_ref, count):
    period = count
    while period % 8:
        period += count
    total = jnp.sum(recv_ref[...].reshape(-1, period, 128), axis=0)
    if count in (1, 2):
        while count < 8:
            total = total + pltpu.roll(total, 8 - count, 0)
            count *= 2
        return total
    return sum(total[p : p + count] for p in range(0, period, count))


def unpacked_gram(packed, pack_ref):
    pack_ref[...] = jnp.zeros((128, 128), F32)
    for p in range(HALF // PACK):
        part = packed
        if p:
            part = pltpu.roll(part, 128 - p * PACK_LANES, 1)
        pack_ref[pl.ds(p * PACK, PACK), :] = part
    turned = jnp.transpose(pack_ref[...])
    plain = pack_ref[pl.ds(0, HALF), :]
    lane = iota((HALF, 128), 1)
    sub = iota((HALF, 128), 0)
    diagonal = jnp.sum(jnp.where(lane == KEEP, plain, 0.0), axis=1, keepdims=True)
    top = jnp.where((lane > sub) | (lane >= HALF), plain, turned[:HALF])
    top = jnp.where(lane == sub, diagonal, top)
    last = jnp.where(lane <= sub, plain, turned[:HALF])
    pack_ref[...] = turned
    bottom = jnp.where(lane < HALF, pack_ref[pl.ds(HALF, HALF), :], pltpu.roll(last, HALF, 1))
    pack_ref[pl.ds(0, HALF), :] = jnp.where(lane < KEEP, top, 0.0)
    pack_ref[pl.ds(HALF, HALF), :] = jnp.where(lane < KEEP, bottom, 0.0)
    pack_ref[pl.ds(KEEP, STEPS), :] = jnp.zeros((STEPS, 128), F32)


def solve_weights(count, cells, recv_ref, state_in, state_ref, weight_ref, pack_ref):
    lane = iota((1, 128), 1)
    lanes = iota((BASIS, 128), 1)
    subs = iota((BASIS, 128), 0)
    sub = iota((BASIS, 1), 0)
    scale = 1.0 / cells

    def spread(values):
        return jnp.sum(values, axis=1, keepdims=True)

    if count == 0:
        half = recv_ref.shape[0] // 2
        low = summed_rows(recv_ref.at[pl.ds(0, half)], SHARE) * scale
        high = summed_rows(recv_ref.at[pl.ds(half, half)], SHARE) * scale
        pack_ref[pl.ds(0, SHARE), :] = low
        pack_ref[pl.ds(SHARE, SHARE), :] = high
        total = low + high
        unpacked_gram(pack_ref[pl.ds(0, PACK), :], pack_ref)
        gram = pack_ref[pl.ds(0, BASIS), :]
        hess = jnp.zeros((BASIS, 128), F32)
        inverse_row = jnp.where(lane < KEEP, 1.0, 0.0)
        inverse_column = jnp.where(sub < KEEP, 1.0, 0.0)
        first_row = jnp.zeros((1, 128), F32)
        for r in range(SHARE):
            part = pltpu.roll(total[r : r + 1], 128 - FREE_LANE + r * FREE, 1)
            mine = (lane >= r * FREE) & (lane < (r + 1) * FREE)
            first_row = jnp.where(mine, part, first_row)
        inverse = jnp.ones((1, 1), F32)
        image_square = None
        first = to_column(first_row)
        folded = spread(gram * first_row)
    else:
        total = summed_rows(recv_ref, 1)[0:1] * scale
        newest = KEEP + count - 1
        raw_first = total
        raw_gram = pltpu.roll(total, 128 - OWN_LANE, 1)
        inverse_row = state_in[pl.ds(STATE_D, 1), :]
        gram = state_in[pl.ds(STATE_G, BASIS), :]
        hess = state_in[pl.ds(STATE_H, BASIS), :]
        part_first, part_gram = raw_first * inverse_row, raw_gram * inverse_row
        square = spread(jnp.where(lane == newest, raw_gram, 0.0))
        first_newest = spread(jnp.where(lane == newest, raw_first, 0.0))
        image_square = spread(jnp.where(lane == BASIS - 1, raw_first, 0.0))
        crossed = spread(part_gram * part_first)
        first_column, gram_column = to_column(part_first), to_column(part_gram)
        inverse_column = to_column(inverse_row)
        folded = spread(gram * part_first)
        norm = jnp.sqrt(square + EPSILON)
        inverse = 1.0 / norm
        own = square * inverse * inverse
        first_newest = first_newest * inverse * inverse
        image_square = image_square * inverse * inverse
        mine = sub == newest
        first = jnp.where(mine, first_newest, first_column * inverse)
        gram_column = gram_column * inverse
        folded = jnp.where(
            mine,
            crossed * inverse * inverse + own * first_newest,
            folded * inverse + gram_column * first_newest,
        )
        gram = jnp.where(lanes == newest, gram_column, gram)
        gram = jnp.where(subs == newest, part_gram * inverse, gram)
        gram = jnp.where((lanes == newest) & (subs == newest), own, gram)
        hess = jnp.where((subs == newest) & (lanes == count - 1), norm, hess)
        inverse_row = jnp.where(lane == newest, inverse, inverse_row)
        inverse_column = jnp.where(mine, inverse, inverse_column)
    weights = first + (first - folded)
    weight_ref[pl.ds(0, BASIS), :] = jnp.broadcast_to(weights * inverse_column, (BASIS, ZS))
    weight_ref[pl.ds(BASIS, 8), :] = jnp.broadcast_to(inverse, (8, ZS))
    hess = jnp.where((lanes == count) & (subs < KEEP + count), weights, hess)
    state_ref[pl.ds(STATE_G, BASIS), :] = gram
    state_ref[pl.ds(STATE_H, BASIS), :] = hess
    state_ref[pl.ds(STATE_D, 8), :] = jnp.broadcast_to(inverse_row, (8, 128))
    return weights, first, gram, image_square


def combined(rows, weight_ref, w_ref, v_ref, others):
    value = w_ref[rows, :] * weight_ref[pl.ds(BASIS, 1), :]
    for i in range(KEEP):
        value = value - weight_ref[pl.ds(i, 1), :] * v_ref[i, rows, :]
    for i, other in enumerate(others):
        value = value - weight_ref[pl.ds(KEEP + i, 1), :] * other[rows, :]
    return value


def combine_half(out_ref, high, weight_ref, w_ref, v_ref, others):
    start = high.astype(jnp.int32) * (ROWS // 2)

    def step(c, carry):
        rows = pl.ds(pl.multiple_of(start + c * CHUNK, CHUNK), CHUNK)
        out_ref[pl.ds(pl.multiple_of(c * CHUNK, CHUNK), CHUNK), :] = combined(
            rows, weight_ref, w_ref, v_ref, others
        )
        return carry

    lax.fori_loop(0, ROWS // 2 // CHUNK, step, 0)


HALF_SHAPE = jax.ShapeDtypeStruct((ROWS // 2, ZS), F32)
WEIGHT_SHAPE = (BASIS + 8, ZS)


def far_kernel(count, cells, *refs):
    recv_ref, w_ref, v_ref, *others = refs[: 3 + count]
    *states, far_ref, weight_ref, state_ref, pack_ref = refs[3 + count :]
    state_in = states[0] if states else None
    solve_weights(count, cells, recv_ref, state_in, state_ref, weight_ref, pack_ref)
    odd = lax.axis_index("gx") % 2 == 1
    combine_half(far_ref, odd, weight_ref, w_ref, v_ref, others)


def far_call(recv, w, v, created, state, cells):
    count = len(created)
    states = [state] if created else []
    return pl.pallas_call(
        functools.partial(far_kernel, count, cells),
        in_specs=[VMEM_SPEC] * (3 + count + len(states)),
        out_specs=(VMEM_SPEC,) * 3,
        out_shape=(
            HALF_SHAPE,
            pltpu.VMEM(WEIGHT_SHAPE, F32),
            jax.ShapeDtypeStruct((STATE_ROWS, 128), F32),
        ),
        scratch_shapes=[pltpu.VMEM((128, 128), F32)],
        compiler_params=PARAMS,
    )(recv, w, v, *created, *states)


def near_kernel(count, *refs):
    weight_ref, far_ref, w_ref, v_ref, *others = refs[: 4 + count]
    near_ref, swap_ref = refs[4 + count :]
    odd = lax.axis_index("gx") % 2 == 1
    upper = lax.axis_index("gy") == 1
    combine_half(near_ref, jnp.logical_not(odd), weight_ref, w_ref, v_ref, others)
    for x in range(XS):
        sides = []
        for y in (0, YS - 2):
            rows = pl.ds((x % 2) * YS + y, 2)
            low, high = (near_ref, far_ref) if x < 2 else (far_ref, near_ref)
            sides.append(jnp.where(odd, low[rows, :], high[rows, :]))
        swap_ref[pl.ds(2 * x, 2), :] = jnp.where(upper, *sides)


def near_call(weight, far, w, v, created):
    count = len(created)
    return pl.pallas_call(
        functools.partial(near_kernel, count),
        in_specs=[VMEM_SPEC] * (4 + count),
        out_specs=(VMEM_SPEC,) * 2,
        out_shape=(HALF_SHAPE, jax.ShapeDtypeStruct((2 * XS, ZS), F32)),
        compiler_params=PARAMS,
    )(weight, far, w, v, *created)


def last_kernel(cells, *refs):
    count = STEPS - 1
    recv_ref, w_ref, v_ref, *others = refs[: 3 + count]
    state_in, u_ref, state_ref, square_ref, guess_ref, sound_ref, new_ref = refs[3 + count : 10 + count]
    weight_ref, scaled_ref, sems = refs[10 + count :]
    weights, first, gram, image_square = solve_weights(
        count, cells, recv_ref, state_in, state_ref, weight_ref, None
    )
    again = jnp.sum(gram * to_row(weights), axis=1, keepdims=True)
    guess = image_square - jnp.sum(weights * (2.0 * first - again), axis=0, keepdims=True)
    guess_ref[...] = jnp.where(iota((1, 128), 1) == 0, guess, 0.0)
    sound = jnp.where(guess > SOUND_SHARE * image_square, 1, 0)
    sound_ref[0] = sound[0, 0]
    lane = iota((1, 128), 1)
    inverse_row = state_ref[pl.ds(STATE_D, 1), :]
    copies = []
    for j, other in enumerate(others):
        inverse = jnp.sum(jnp.where(lane == KEEP + j, inverse_row, 0.0), axis=1, keepdims=True)
        for c in range(ROWS // CHUNK):
            rows = pl.ds(c * CHUNK, CHUNK)
            scaled_ref[j, rows, :] = other[rows, :] * inverse
        copies.append(pltpu.make_async_copy(scaled_ref.at[j], new_ref.at[j], sems.at[j]))
        copies[-1].start()

    def step(c, acc):
        rows = pl.ds(pl.multiple_of(c * BLOCK, BLOCK), BLOCK)
        value = combined(rows, weight_ref, w_ref, v_ref, others)
        u_ref[rows, :] = value
        return acc + fold_tiles(value * value)

    acc = lax.fori_loop(0, ROWS // BLOCK, step, jnp.zeros((8, ZS), F32))
    square_ref[...] = fold_row(acc)
    for copy in copies:
        copy.wait()


def last_call(recv, w, v, created, state, cells):
    return pl.pallas_call(
        functools.partial(last_kernel, cells),
        in_specs=[VMEM_SPEC] * (4 + len(created)),
        out_specs=(VMEM_SPEC,) * 4 + (SMEM_SPEC, HBM_SPEC),
        out_shape=(
            pltpu.VMEM((ROWS, ZS), F32),
            jax.ShapeDtypeStruct((STATE_ROWS, 128), F32),
            *LAST_SHAPES,
            pltpu.HBM((STEPS, ROWS, ZS), F32),
        ),
        scratch_shapes=[
            pltpu.VMEM(WEIGHT_SHAPE, F32),
            pltpu.VMEM((STEPS - 1, ROWS, ZS), F32),
            pltpu.SemaphoreType.DMA((STEPS - 1,)),
        ],
        compiler_params=PARAMS,
        name="last",
    )(recv, w, v, *created, state)


def finish_kernel(square_ref, state_ref, u_ref, new_in, new_ref, hess_ref, scaled_ref, sem):
    norm = jnp.sqrt(jnp.sum(square_ref[...], axis=1, keepdims=True) + EPSILON)
    inverse = 1.0 / norm
    for c in range(ROWS // CHUNK):
        rows = pl.ds(c * CHUNK, CHUNK)
        scaled_ref[rows, :] = u_ref[rows, :] * inverse
    copy = pltpu.make_async_copy(scaled_ref, new_ref.at[STEPS - 1], sem)
    copy.start()
    lanes = iota((BASIS, 128), 1)
    subs = iota((BASIS, 128), 0)
    hess = state_ref[pl.ds(STATE_H, BASIS), :]
    hess = jnp.where((subs == BASIS - 1) & (lanes == STEPS - 1), norm, hess)
    hess = jnp.concatenate([hess, jnp.zeros((128 - BASIS, 128), F32)], axis=0)
    hess_ref[...] = jnp.transpose(hess)[:STEPS, :BASIS]
    copy.wait()


def finish_call(square, state, u, new):
    return pl.pallas_call(
        finish_kernel,
        in_specs=[VMEM_SPEC] * 3 + [HBM_SPEC],
        out_specs=(HBM_SPEC, VMEM_SPEC),
        out_shape=(
            pltpu.HBM((STEPS, ROWS, ZS), F32),
            jax.ShapeDtypeStruct((STEPS, BASIS), F32),
        ),
        scratch_shapes=[pltpu.VMEM((ROWS, ZS), F32), pltpu.SemaphoreType.DMA],
        input_output_aliases={3: 0},
        compiler_params=PARAMS,
        name="finish",
    )(square, state, u, new)


def paired(half, start):
    lower = range(start, lax.axis_size("gx") - 1, 2)
    return lax.ppermute(half, "gx", [(i, i + 1) for i in lower] + [(i + 1, i) for i in lower])


def across(edge):
    return lax.ppermute(edge, "gy", [(0, 1), (1, 0)])


def from_all(payload):
    axes = ("gy", "gx")
    devices = lax.axis_size(axes)
    copies = payload.reshape(devices, 1, -1)
    got = lax.all_to_all(copies, axes, split_axis=0, concat_axis=0, tiled=True)
    return got.reshape(-1, 128)


def body(basis_vectors, reaction):
    devices = lax.axis_size(("gy", "gx"))
    cells = float(ROWS * ZS * devices)
    basis = basis_vectors.reshape(KEEP, ROWS, ZS)
    v, near, far, swap, early = start_call(basis)
    second = paired(far, 1)
    first = paired(near, 0)
    swap = across(swap)
    reaction = reaction.reshape(ROWS, ZS)
    keep, give = gram_call(v, early)
    got = across(give)
    w, row = first_image_call(v, (first, second, swap), reaction)
    payload = first_payload_call(row, keep, got, devices)
    created = []
    state = None
    for _ in range(1, STEPS):
        recv = from_all(payload)
        far, weight, state = far_call(recv, w, v, created, state, cells)
        second = paired(far, 1)
        near, swap = near_call(weight, far, w, v, created)
        first = paired(near, 0)
        swap = across(swap)
        u, own = own_call(v, near, far, created)
        created.append(u)
        inner, extra = inner_call(v, created, swap, reaction, own)
        w, payload = outer_call(v, created, first, second, inner, extra, devices)
    recv = from_all(payload)
    u, state, square, guess, sound, new = last_call(recv, w, v, created, state, cells)
    square = lax.cond(
        sound[0] == 1,
        lambda guess, square: guess,
        lambda guess, square: jnp.sum(from_all(square), axis=0, keepdims=True) * (1.0 / cells),
        guess,
        jnp.broadcast_to(square, (devices, 128)),
    )
    new, hessenberg = finish_call(square, state, u, new)
    return new.reshape(STEPS, XS, YS, ZS), hessenberg.T


def solution(mesh):
    return jax.shard_map(
        body,
        mesh=mesh,
        in_specs=(P(None, "gx", "gy", None), P("gx", "gy", None)),
        out_specs=(P(None, "gx", "gy", None), P()),
        check_vma=False,
    )
```
